32 devices in a mesh: batch: 1 (over z), g: 32 (over y, x, core).
Axes of the slice: x: 4, y: 4, z: 1, core: 2. Of those that a mesh axis runs over, the one named last changes fastest.
The devices are a block of a 4x4x8 slice.
Arguments:
- keys: float32 [65536], P(('batch', 'g'))
- payload: bfloat16 [65536, 1536], P(('batch', 'g'))
Outputs:
- output 1: float32 [131072], P(('batch', 'g'))
- output 2: bfloat16 [131072, 1536], P(('batch', 'g'))
- output 3: int32 [32], P(('batch', 'g'))
All inputs are finite; a program needn't handle non-finite values.
Results may differ from the reference program's by a relative error of at most 0.001.
Values are sent between devices in bfloat16 or wider.
A program may use at most 768 MiB of HBM per device.

```python
import math
import functools
import jax
import jax.numpy as jnp
from jax import lax

GROUP = 32
N_DEV = 2048
WIDTH = 1536
SEGMENTS = 16
PART_ROWS = GROUP * N_DEV
OUT_ROWS = 2 * N_DEV
PAD_KEY = 128.0


def swap_into(perm_row, dev_id, target):
    cur_pos = jnp.argmax(perm_row == dev_id)
    displaced = perm_row[target]
    slot_ids = jnp.arange(perm_row.shape[0])
    return jnp.where(slot_ids == target, dev_id, jnp.where(slot_ids == cur_pos, displaced, perm_row))


def draw_keys(base):
    k_gap, k_exp, k_pick, k_block, k_heads, k_rest, k_local = jax.random.split(base, 7)
    seg_exp = jax.random.randint(k_exp, (SEGMENTS, 1), 0, 8)
    raw_bits = jax.random.randint(k_gap, (SEGMENTS, PART_ROWS // SEGMENTS), 0, 128)
    levels = jnp.cumsum((1 + jnp.right_shift(raw_bits, 7 - seg_exp)).reshape(-1))
    centered = levels - levels[PART_ROWS // 2]
    key_scale = 2.0 ** -(int(math.log2(PART_ROWS)) + 2)
    ranked_keys = centered.astype(jnp.float32) * key_scale
    picked = jax.random.permutation(k_pick, GROUP)
    hot_dev = picked[0]
    cold_dev = picked[1]
    hot_block = jax.random.randint(k_block, (), 0, GROUP - 1)
    block_ids = jnp.arange(GROUP)[:, None]
    head_owner = jax.vmap(functools.partial(jax.random.permutation, x=GROUP))(jax.random.split(k_heads, GROUP))
    hot_row = head_owner[hot_block]
    hot_pos = jnp.argmax(hot_row == hot_dev)
    hot_row = swap_into(hot_row, hot_dev, jnp.where(hot_pos >= GROUP // 2, hot_pos, GROUP - 1))
    head_owner = jnp.where(block_ids == hot_block, hot_row[None, :], head_owner)
    next_row = swap_into(head_owner[hot_block + 1], hot_dev, 0)
    head_owner = jnp.where(block_ids == hot_block + 1, next_row[None, :], head_owner)
    tail_owner = jnp.broadcast_to(jnp.repeat(jnp.arange(GROUP), N_DEV // GROUP - 1)[None, :], (GROUP, N_DEV - GROUP))
    tail_owner = jnp.where((block_ids == hot_block) & (tail_owner == cold_dev), hot_dev, tail_owner)
    tail_owner = jnp.where((block_ids == hot_block + 1) & (tail_owner == hot_dev), cold_dev, tail_owner)
    tail_owner = jax.vmap(jax.random.permutation)(jax.random.split(k_rest, GROUP), tail_owner)
    owners = jnp.concatenate([head_owner, tail_owner], axis=1).reshape(-1)
    rank_grid = jnp.argsort(owners, stable=True).reshape(GROUP, N_DEV)
    rank_grid = jax.vmap(jax.random.permutation)(jax.random.split(k_local, GROUP), rank_grid)
    return ranked_keys[rank_grid.reshape(-1)]


def setup_inputs(seed: int = 0, part: int = 0) -> dict:
    base = jax.random.fold_in(jax.random.key(seed), part)
    k_keys, k_rows = jax.random.split(base)
    keys = draw_keys(k_keys)
    payload = jax.random.normal(k_rows, (PART_ROWS, WIDTH), jnp.float32).astype(jnp.bfloat16)
    return {"keys": keys, "payload": payload}


def reference(keys, payload):
    local_sorted = jnp.sort(keys.reshape(GROUP, N_DEV), axis=1)
    samples = local_sorted[:, :: N_DEV // GROUP].reshape(-1)
    splitters = jnp.sort(samples)[GROUP + GROUP // 2 :: GROUP]
    sorted_all, sort_order = lax.sort((keys, jnp.arange(PART_ROWS, dtype=jnp.int32)), num_keys=1)
    edges = jnp.searchsorted(sorted_all, splitters, side="left").astype(jnp.int32)
    starts = jnp.concatenate([jnp.zeros((1,), jnp.int32), edges])
    stops = jnp.concatenate([edges, jnp.full((1,), PART_ROWS, jnp.int32)])
    counts = stops - starts
    slot_ids = jnp.arange(OUT_ROWS, dtype=jnp.int32)
    src_pos = jnp.minimum(starts[:, None] + slot_ids[None, :], PART_ROWS - 1)
    is_valid = slot_ids[None, :] < counts[:, None]
    out_keys = jnp.where(is_valid, sorted_all[src_pos], PAD_KEY)
    out_payload = jnp.where(is_valid[:, :, None], payload[sort_order[src_pos]], 0.0)
    return out_keys.reshape(-1), out_payload.reshape(-1, WIDTH), counts
```

```python
import functools

import jax
import jax.numpy as jnp
from jax import lax
from jax.experimental import pallas as pl
from jax.experimental.pallas import tpu as pltpu
from jax.sharding import PartitionSpec as P

PAD_KEY = 128.0
LANES = 128
SUB = 4
BASE = 65
RELAY = 2

VMEM = pl.BlockSpec(memory_space=pltpu.VMEM)
SMEM = pl.BlockSpec(memory_space=pltpu.SMEM)
ANY = pl.BlockSpec(memory_space=pl.ANY)


def share_keys_kernel(group_size, keys_ref, all_ref, send_sem, recv_sem):
    me = lax.axis_index("g")
    barrier = pltpu.get_barrier_semaphore()
    for d in range(1, group_size):
        pl.semaphore_signal(barrier, inc=1, device_id={"g": lax.rem(me + d, group_size)}, device_id_type=pl.DeviceIdType.MESH)
    pl.semaphore_wait(barrier, group_size - 1)
    copies = []
    for d in range(1, group_size):
        copies.append(
            pltpu.make_async_remote_copy(
                src_ref=keys_ref,
                dst_ref=all_ref.at[me],
                send_sem=send_sem.at[d],
                recv_sem=recv_sem.at[d],
                device_id={"g": lax.rem(me + d, group_size)},
                device_id_type=pl.DeviceIdType.MESH,
            )
        )
        copies[-1].start()
    all_ref[pl.ds(me, 1)] = keys_ref[...][None]
    for c in copies:
        c.wait()


def share_keys(keys, group_size):
    return pl.pallas_call(
        functools.partial(share_keys_kernel, group_size),
        out_shape=jax.ShapeDtypeStruct((group_size, *keys.shape), keys.dtype),
        in_specs=[VMEM],
        out_specs=VMEM,
        scratch_shapes=[pltpu.SemaphoreType.DMA((group_size,)), pltpu.SemaphoreType.DMA((group_size,))],
        compiler_params=pltpu.CompilerParams(collective_id=0, has_side_effects=True),
        name="share_keys",
    )(keys)


def split_rows_kernel(rows_ref, out_ref):
    tiles = rows_ref.shape[1] // LANES
    parts = tiles // SUB

    def body(g, carry):
        r = pl.multiple_of(g * 16, 16)
        v = rows_ref[pl.ds(r, 16), :].reshape(16, tiles, LANES)
        for q in range(parts):
            out_ref[pl.ds(r, 16), q] = v[:, SUB * q : SUB * (q + 1)]
        return carry

    lax.fori_loop(0, rows_ref.shape[0] // 16, body, 0)


def split_rows(rows):
    n, width = rows.shape
    block = 256
    shape = (n, width // (SUB * LANES), SUB, LANES)
    return pl.pallas_call(
        split_rows_kernel,
        grid=(n // block,),
        out_shape=jax.ShapeDtypeStruct(shape, rows.dtype),
        in_specs=[pl.BlockSpec((block, width), lambda i: (i, 0))],
        out_specs=pl.BlockSpec((block, *shape[1:]), lambda i: (i, 0, 0, 0)),
        name="split_rows",
    )(rows)


def pick_kernel(cap, relay, group_size, order_ref, start_ref, extra_ref, rows_ref, out_ref, *relay_out):
    last = rows_ref.shape[0] - 1
    unroll = next(u for u in (8, 5, 4, 2, 1) if cap % u == 0)

    def per_dst(j, carry):
        first = start_ref[j]

        def body(b, c):
            for u in range(unroll):
                k = b * unroll + u
                out_ref[j, k] = rows_ref[order_ref[jnp.minimum(first + k, last)]]
            return c

        return lax.fori_loop(0, cap // unroll, body, carry)

    lax.fori_loop(0, group_size, per_dst, 0)
    if relay:

        def per_mid(m, carry):
            for r in range(relay):
                src = jnp.minimum(extra_ref[0] + r * group_size + m, last)
                relay_out[0][m, r] = rows_ref[order_ref[src]]
            return carry

        lax.fori_loop(0, group_size, per_mid, 0)


def pick(order, starts, extra, rows, cap, relay, group_size):
    row = rows.shape[1:]
    outs = [jax.ShapeDtypeStruct((group_size, cap, *row), rows.dtype)]
    if relay:
        outs.append(jax.ShapeDtypeStruct((group_size, relay, *row), rows.dtype))
    return pl.pallas_call(
        functools.partial(pick_kernel, cap, relay, group_size),
        out_shape=outs,
        in_specs=[SMEM, SMEM, SMEM, VMEM],
        out_specs=[VMEM] * len(outs),
        name="pick_rows",
    )(order, starts, extra, rows)


def segment_kernel(start_ref, count_ref, all_ref, out_ref):
    group_size, tiles, _ = all_ref.shape
    lane = lax.broadcasted_iota(jnp.int32, (1, LANES), 1)
    for i in range(group_size):
        s = start_ref[i]
        t = s // LANES
        off = s - t * LANES
        t = jnp.minimum(t, tiles - 1)
        a = all_ref[i, pl.ds(t, 1), :]
        b = all_ref[i, pl.ds(jnp.minimum(t + 1, tiles - 1), 1), :]
        shift = lax.rem(LANES - off, LANES)
        a = pltpu.roll(a, shift, 1)
        b = pltpu.roll(b, shift, 1)
        v = jnp.where(lane < LANES - off, a, b)
        out_ref[pl.ds(i, 1), :] = jnp.where(lane < count_ref[i], v, PAD_KEY)


def segments(starts, counts, all_keys):
    group_size = all_keys.shape[0]
    return pl.pallas_call(
        segment_kernel,
        out_shape=jax.ShapeDtypeStruct((group_size, LANES), all_keys.dtype),
        in_specs=[SMEM, SMEM, VMEM],
        out_specs=VMEM,
        name="segments",
    )(starts, counts, all_keys)


def swap_kernel(src_ref, in_ref, out_ref):
    for j in range(out_ref.shape[0]):
        out_ref[j] = in_ref[src_ref[j]]


def swap(src, blocks):
    return pl.pallas_call(
        swap_kernel,
        out_shape=jax.ShapeDtypeStruct(blocks.shape, blocks.dtype),
        in_specs=[SMEM, VMEM],
        out_specs=VMEM,
        name="swap",
    )(src, blocks)


def place_kernel(n_in, idx_ref, count_ref, *refs):
    ins, (out_ref, held, sem) = refs[:n_in], refs[n_in:]
    step = pl.program_id(0)
    block, width = out_ref.shape
    parts, sub, lanes = held.shape[1:]

    @pl.when(step == 0)
    def _():
        copies = []
        first = 0
        for i, ref in enumerate(ins):
            copies.append(pltpu.make_async_copy(ref, held.at[pl.ds(first, ref.shape[0])], sem.at[i]))
            copies[-1].start()
            first += ref.shape[0]
        held[first] = jnp.zeros(held.shape[1:], held.dtype)
        for c in copies:
            c.wait()

    live = step * block < count_ref[0]

    @pl.when(live)
    def _():
        def body(g, carry):
            r = pl.multiple_of(g * 16, 16)
            rows = []
            for u in range(16):
                k = idx_ref[step * block + r + u]
                rows.append(jnp.concatenate([held[k, q] for q in range(parts)], 0))
            out_ref[pl.ds(r, 16), :] = jnp.stack(rows, 0).reshape(16, width)
            return carry

        lax.fori_loop(0, block // 16, body, 0)

    @pl.when(jnp.logical_not(live))
    def _():
        out_ref[...] = jnp.zeros(out_ref.shape, out_ref.dtype)


def place(idx, count, ins, width):
    n_out = idx.shape[0]
    block = 256
    total = sum(x.shape[0] for x in ins)
    return pl.pallas_call(
        functools.partial(place_kernel, len(ins)),
        grid_spec=pltpu.PrefetchScalarGridSpec(
            num_scalar_prefetch=2,
            grid=(n_out // block,),
            in_specs=[ANY] * len(ins),
            out_specs=pl.BlockSpec((block, width), lambda i, *_: (i, 0)),
            scratch_shapes=[pltpu.VMEM((total + 1, *ins[0].shape[1:]), ins[0].dtype), pltpu.SemaphoreType.DMA((len(ins),))],
        ),
        out_shape=jax.ShapeDtypeStruct((n_out, width), ins[0].dtype),
        name="place_rows",
    )(idx, count, *ins)


def solution(mesh):
    group_size = mesh.shape["g"]

    def local_part(keys_loc, rows_loc):
        n_dev = keys_loc.shape[0]
        width = rows_loc.shape[1]
        cap_rows = 2 * n_dev // group_size
        me = lax.axis_index("g")
        sorted_keys, order = lax.sort((keys_loc, lax.iota(jnp.int32, n_dev)), num_keys=1)
        all_keys = share_keys(sorted_keys.reshape(n_dev // LANES, LANES), group_size)
        rows = split_rows(rows_loc)
        per_sample = n_dev // group_size
        flat_keys = all_keys.reshape(group_size, n_dev)
        all_samples = jnp.sort(flat_keys[:, ::per_sample].reshape(-1))
        splitters = all_samples[group_size + group_size // 2 :: group_size]
        below = (all_keys[:, None] < splitters[None, :, None, None]).astype(jnp.int32)
        edges = jnp.sum(below, axis=(2, 3))
        edges = jnp.concatenate([jnp.zeros((group_size, 1), jnp.int32), edges, jnp.full((group_size, 1), n_dev, jnp.int32)], axis=1)
        counts = edges[:, 1:] - edges[:, :-1]
        over = jnp.maximum(counts - BASE, 0)
        has = (over > 0).astype(jnp.int32)
        short = (jnp.max(jnp.sum(has, 0)) <= 1) & (jnp.max(jnp.sum(has, 1)) <= 1) & (jnp.max(over) <= RELAY * group_size)

        starts = edges[me, :group_size]
        col = lambda m: lax.dynamic_slice_in_dim(m, me, 1, axis=1)[:, 0]
        my_counts = col(counts)
        segs = segments(col(edges), my_counts, all_keys)
        own_count = jnp.sum(my_counts).reshape(1)
        src = lax.broadcasted_iota(jnp.int32, segs.shape, 0)
        pos = lax.broadcasted_iota(jnp.int32, segs.shape, 1)

        def merge(slot, n_slots):
            slot = jnp.where(pos < my_counts[:, None], slot, n_slots)
            return lax.sort((segs.reshape(-1), slot.reshape(-1)), num_keys=1)

        def send(blocks):
            return lax.all_to_all(blocks, "g", 0, 0, tiled=True)

        def flat(blocks):
            return blocks.reshape(-1, *blocks.shape[2:])

        def with_relay():
            dst = jnp.argmax(over[me]).astype(jnp.int32)
            extra = (starts[dst] + BASE).reshape(1)
            base, first = pick(order, starts, extra, rows, BASE, RELAY, group_size)
            first = send(first)
            second = send(swap(jnp.argmax(over, axis=0).astype(jnp.int32), first))
            base = send(base)
            past = pos - BASE
            slot = jnp.where(past < 0, src * BASE + pos, group_size * BASE + lax.rem(past, group_size) * RELAY + past // group_size)
            merged, idx = merge(slot, group_size * (BASE + RELAY))
            return merged, place(idx, own_count, [flat(base), flat(second)], width)

        def direct():
            (base,) = pick(order, starts, jnp.zeros((1,), jnp.int32), rows, cap_rows, 0, group_size)
            base = send(base)
            merged, idx = merge(src * cap_rows + pos, group_size * cap_rows)
            return merged, place(idx, own_count, [flat(base)], width)

        merged, merged_rows = lax.cond(short, with_relay, direct)
        return merged, merged_rows, own_count

    row_spec = P(("batch", "g"))
    mat_spec = P(("batch", "g"), None)
    return jax.shard_map(local_part, mesh=mesh, in_specs=(row_spec, mat_spec), out_specs=(row_spec, mat_spec, row_spec), check_vma=False)
```

```python
import functools

import jax
import jax.numpy as jnp
from jax import lax
from jax.experimental import pallas as pl
from jax.experimental.pallas import tpu as pltpu
from jax.sharding import PartitionSpec as P

PAD_KEY = 128.0
LANES = 128
SUB = 4
BASE = 65
RELAY = 2

VMEM = pl.BlockSpec(memory_space=pltpu.VMEM)
SMEM = pl.BlockSpec(memory_space=pltpu.SMEM)
ANY = pl.BlockSpec(memory_space=pl.ANY)
MESH = pl.DeviceIdType.MESH
STARTS, COL_STARTS, COL_COUNTS, FROM_SRC, EXTRA, SHORT, OWN = range(7)


def share_keys_kernel(group_size, block, keys_ref, rows_ref, all_ref, split_ref, fetched, held, send_sem, recv_sem, in_sem, out_sem):
    me = lax.axis_index("g")
    barrier = pltpu.get_barrier_semaphore()
    for d in range(1, group_size):
        pl.semaphore_signal(barrier, inc=1, device_id={"g": lax.rem(me + d, group_size)}, device_id_type=MESH)
    n, width = rows_ref.shape
    steps = n // block
    tiles = width // LANES

    def fetch(s):
        return pltpu.make_async_copy(rows_ref.at[pl.ds(s * block, block)], fetched.at[s], in_sem.at[s])

    def keep(s):
        return pltpu.make_async_copy(held.at[s], split_ref.at[pl.ds(s * block, block)], out_sem.at[s])

    for s in range(steps):
        fetch(s).start()
    pl.semaphore_wait(barrier, group_size - 1)
    copies = []
    for d in range(1, group_size):
        copies.append(
            pltpu.make_async_remote_copy(
                src_ref=keys_ref,
                dst_ref=all_ref.at[me],
                send_sem=send_sem.at[d],
                recv_sem=recv_sem.at[d],
                device_id={"g": lax.rem(me + d, group_size)},
                device_id_type=MESH,
            )
        )
        copies[-1].start()
    all_ref[pl.ds(me, 1)] = keys_ref[...][None]
    for s in range(steps):
        fetch(s).wait()

        def body(g, carry):
            r = pl.multiple_of(g * 16, 16)
            v = fetched[s, pl.ds(r, 16), :].reshape(16, tiles, LANES)
            for q in range(tiles // SUB):
                held[s, pl.ds(r, 16), q] = v[:, SUB * q : SUB * (q + 1)]
            return carry

        lax.fori_loop(0, block // 16, body, 0)
        if s:
            keep(s - 1).start()
    for c in copies:
        c.wait()
    keep(steps - 1).start()
    for s in range(steps):
        keep(s).wait()


def share_keys(keys, rows, group_size):
    n, width = rows.shape
    block = 512
    row = (width // (SUB * LANES), SUB, LANES)
    return pl.pallas_call(
        functools.partial(share_keys_kernel, group_size, block),
        out_shape=[
            jax.ShapeDtypeStruct((group_size, *keys.shape), keys.dtype),
            jax.ShapeDtypeStruct((n, *row), rows.dtype),
        ],
        in_specs=[VMEM, ANY],
        out_specs=[VMEM, ANY],
        scratch_shapes=[
            pltpu.VMEM((n // block, block, width), rows.dtype),
            pltpu.VMEM((n // block, block, *row), rows.dtype),
            pltpu.SemaphoreType.DMA((group_size,)),
            pltpu.SemaphoreType.DMA((group_size,)),
            pltpu.SemaphoreType.DMA((n // block,)),
            pltpu.SemaphoreType.DMA((n // block,)),
        ],
        compiler_params=pltpu.CompilerParams(collective_id=0, has_side_effects=True),
        name="share_keys",
    )(keys, rows)


def plan_kernel(cap, most, all_ref, table_ref, edge_ref):
    group_size, tiles, _ = all_ref.shape
    n_dev = tiles * LANES
    per = n_dev // group_size
    each = LANES // per
    me = lax.axis_index("g")
    f32 = jnp.float32
    lane = lax.broadcasted_iota(jnp.int32, (tiles, LANES), 1)
    sub = lax.broadcasted_iota(jnp.int32, (tiles, LANES), 0)
    group_lane = lax.broadcasted_iota(jnp.int32, (group_size, LANES), 1)
    group_sub = lax.broadcasted_iota(jnp.int32, (group_size, LANES), 0)

    def samples(i):
        return [jnp.broadcast_to(all_ref[i, :, l * per : l * per + 1], (tiles, LANES)) for l in range(each)]

    fit = LANES // group_size
    packed = []
    for c in range(group_size // fit):
        acc = jnp.zeros((tiles, LANES), f32)
        for i in range(c * fit, (c + 1) * fit):
            for l, a in enumerate(samples(i)):
                acc = jnp.where(lane == (i % fit) * group_size + each * sub + l, a, acc)
        packed.append(jnp.sum(acc, axis=0, keepdims=True))
    target = lax.broadcasted_iota(jnp.int32, (1, LANES), 1) * group_size + group_size // 2
    target = jnp.where((target > group_size) & (target < group_size * group_size), target, -1).astype(f32)
    found = jnp.zeros((tiles, LANES), f32)
    for i in range(group_size):
        for a in samples(i):
            less = jnp.zeros((tiles, LANES), f32)
            for b in packed:
                less += (b < a).astype(f32)
            rank = jnp.sum(less, axis=1, keepdims=True)
            found += jnp.where(rank == target, a, 0.0)
    splitters = jnp.sum(found, axis=0, keepdims=True)
    splitters = jnp.sum(jnp.where(group_lane == group_sub, splitters, 0.0), axis=1, keepdims=True)
    splitters = jnp.where(group_sub == 0, -PAD_KEY, splitters)

    edge_ref[...] = jnp.zeros(edge_ref.shape, f32)

    def count(b, carry):
        edges = edge_ref[...]
        for u in range(4):
            i = b * 4 + u
            less = jnp.zeros((group_size, LANES), f32)
            for r in range(tiles):
                less += (all_ref[i, r : r + 1, :] < splitters).astype(f32)
            edges = jnp.where(group_lane == i, jnp.sum(less, axis=1, keepdims=True), edges)
        edge_ref[...] = edges
        return carry

    lax.fori_loop(0, group_size // 4, count, 0)
    edges = edge_ref[...]
    after = jnp.concatenate([edges[1:], jnp.full((1, LANES), n_dev, f32)], 0)
    counts = jnp.where(group_lane < group_size, after - edges, 0.0)
    over = jnp.maximum(counts - cap, 0.0)
    has = (over > 0).astype(f32)
    worst = jnp.maximum(jnp.max(jnp.sum(has, axis=0, keepdims=True), axis=1, keepdims=True), jnp.max(jnp.sum(has, axis=1, keepdims=True), axis=0, keepdims=True))
    most_over = jnp.max(jnp.max(over, axis=0, keepdims=True), axis=1, keepdims=True)
    short = ((worst <= 1) & (most_over <= most)).astype(f32)

    def to_row(column):
        return jnp.sum(jnp.where(group_lane == group_sub, column, 0.0), axis=0, keepdims=True)

    mine = group_lane == me
    starts = to_row(jnp.sum(jnp.where(mine, edges, 0.0), axis=1, keepdims=True))
    col_starts = jnp.sum(jnp.where(group_sub == me, edges, 0.0), axis=0, keepdims=True)
    col_counts = jnp.sum(jnp.where(group_sub == me, counts, 0.0), axis=0, keepdims=True)
    from_src = to_row(jnp.sum(has * group_lane.astype(f32), axis=1, keepdims=True))
    extra = jnp.sum(jnp.sum(jnp.where(mine, has * (edges + cap), 0.0), axis=0, keepdims=True), axis=1, keepdims=True)
    own = jnp.sum(col_counts, axis=1, keepdims=True)
    rows = [starts, col_starts, col_counts, from_src, extra, short, own, own]
    table_ref[...] = jnp.concatenate([jnp.broadcast_to(r, (1, LANES)) for r in rows], 0).astype(jnp.int32)


def plan(all_keys, cap, most):
    return pl.pallas_call(
        functools.partial(plan_kernel, cap, most),
        out_shape=jax.ShapeDtypeStruct((8, LANES), jnp.int32),
        in_specs=[VMEM],
        out_specs=VMEM,
        scratch_shapes=[pltpu.VMEM((all_keys.shape[0], LANES), jnp.float32)],
        name="plan",
    )(all_keys)


def segment_kernel(cap, relay, table_ref, all_ref, out_ref, slot_ref):
    group_size, tiles, _ = all_ref.shape
    lane = lax.broadcasted_iota(jnp.int32, (1, LANES), 1)
    short = table_ref[SHORT, 0] > 0
    past = lane - cap
    relayed = group_size * cap + lax.rem(past, group_size) * relay + past // group_size
    unused = jnp.where(short, group_size * (cap + relay), group_size * LANES)
    for i in range(group_size):
        s = table_ref[COL_STARTS, i]
        t = s // LANES
        off = s - t * LANES
        t = jnp.minimum(t, tiles - 1)
        a = all_ref[i, pl.ds(t, 1), :]
        b = all_ref[i, pl.ds(jnp.minimum(t + 1, tiles - 1), 1), :]
        shift = lax.rem(LANES - off, LANES)
        a = pltpu.roll(a, shift, 1)
        b = pltpu.roll(b, shift, 1)
        v = jnp.where(lane < LANES - off, a, b)
        live = lane < table_ref[COL_COUNTS, i]
        out_ref[pl.ds(i, 1), :] = jnp.where(live, v, PAD_KEY)
        slot = jnp.where(short, jnp.where(past < 0, i * cap + lane, relayed), i * LANES + lane)
        slot_ref[pl.ds(i, 1), :] = jnp.where(live, slot, unused)


def segments(table, all_keys, cap, relay):
    shape = (all_keys.shape[0], LANES)
    return pl.pallas_call(
        functools.partial(segment_kernel, cap, relay),
        out_shape=[jax.ShapeDtypeStruct(shape, all_keys.dtype), jax.ShapeDtypeStruct(shape, jnp.int32)],
        in_specs=[SMEM, VMEM],
        out_specs=[VMEM, VMEM],
        name="segments",
    )(table, all_keys)


def exchange_kernel(group_size, cap, relay, early, order_ref, table_ref, rows_ref, out_ref, held, outgoing, first, arrived, second, load_sem, own_sem, send_sem, recv_sem):
    me = lax.axis_index("g")
    last = rows_ref.shape[0] - 1
    load = pltpu.make_async_copy(rows_ref, held, load_sem)
    load.start()
    barrier = pltpu.get_barrier_semaphore()
    for d in range(1, group_size):
        pl.semaphore_signal(barrier, inc=1, device_id={"g": lax.rem(me + d, group_size)}, device_id_type=MESH)

    def peer(d):
        return lax.rem(me + d, group_size)

    def remote(d, src, dst, kind):
        return pltpu.make_async_remote_copy(
            src_ref=src, dst_ref=dst, send_sem=send_sem.at[kind, d], recv_sem=recv_sem.at[kind, d], device_id={"g": peer(d)}, device_id_type=MESH
        )

    def base(d):
        return remote(d, outgoing.at[peer(d)], out_ref.at[pl.ds(me * cap, cap)], 0)

    def hop_one(d):
        return remote(d, first.at[peer(d)], arrived.at[me], 1)

    def hop_two(d):
        return remote(d, second.at[peer(d)], out_ref.at[pl.ds(group_size * cap + me * relay, relay)], 2)

    own_base = pltpu.make_async_copy(outgoing.at[me], out_ref.at[pl.ds(me * cap, cap)], own_sem.at[0])
    own_two = pltpu.make_async_copy(second.at[me], out_ref.at[pl.ds(group_size * cap + me * relay, relay)], own_sem.at[1])

    def gather(d):
        dst = peer(d)
        begin = table_ref[STARTS, dst]

        def body(b, carry):
            for u in range(5):
                k = b * 5 + u
                outgoing[dst, k] = held[order_ref[jnp.minimum(begin + k, last)]]
            return carry

        lax.fori_loop(0, cap // 5, body, 0)

    load.wait()
    extra = table_ref[EXTRA, 0]

    def gather_extra(m, carry):
        for r in range(relay):
            first[m, r] = held[order_ref[jnp.minimum(extra + r * group_size + m, last)]]
        return carry

    lax.fori_loop(0, group_size, gather_extra, 0)
    arrived[pl.ds(me, 1)] = first[pl.ds(me, 1)]
    gather(1)
    pl.semaphore_wait(barrier, group_size - 1)

    def start_one(d, carry):
        hop_one(d).start()
        return carry

    lax.fori_loop(1, group_size, start_one, 0)

    def step(d, carry):
        gather(d)
        base(d - 1).start()
        return carry

    lax.fori_loop(2, early, step, 0)

    def wait_one(d, carry):
        hop_one(d).wait()
        return carry

    lax.fori_loop(1, group_size, wait_one, 0)
    for j in range(group_size):
        second[j] = arrived[table_ref[FROM_SRC, j]]
    lax.fori_loop(early, early + 1, step, 0)

    def start_two(d, carry):
        hop_two(d).start()
        return carry

    lax.fori_loop(1, group_size, start_two, 0)
    lax.fori_loop(early + 1, group_size, step, 0)
    gather(0)
    base(group_size - 1).start()
    own_two.start()
    own_base.start()

    def wait_rest(d, carry):
        hop_two(d).wait()
        base(d).wait()
        return carry

    lax.fori_loop(1, group_size, wait_rest, 0)
    own_two.wait()
    own_base.wait()


def exchange(order, table, rows, cap, relay, group_size):
    row = rows.shape[1:]
    return pl.pallas_call(
        functools.partial(exchange_kernel, group_size, cap, relay, 9),
        out_shape=jax.ShapeDtypeStruct((group_size * (cap + relay), *row), rows.dtype),
        in_specs=[SMEM, SMEM, ANY],
        out_specs=ANY,
        scratch_shapes=[
            pltpu.VMEM(rows.shape, rows.dtype),
            pltpu.VMEM((group_size, cap, *row), rows.dtype),
            pltpu.VMEM((group_size, relay, *row), rows.dtype),
            pltpu.VMEM((group_size, relay, *row), rows.dtype),
            pltpu.VMEM((group_size, relay, *row), rows.dtype),
            pltpu.SemaphoreType.DMA,
            pltpu.SemaphoreType.DMA((2,)),
            pltpu.SemaphoreType.DMA((3, group_size)),
            pltpu.SemaphoreType.DMA((3, group_size)),
        ],
        compiler_params=pltpu.CompilerParams(collective_id=1, has_side_effects=True),
        name="exchange",
    )(order, table, rows)


def pick_kernel(cap, group_size, order_ref, table_ref, rows_ref, out_ref):
    last = rows_ref.shape[0] - 1

    def per_dst(j, carry):
        first = table_ref[STARTS, j]

        def body(b, c):
            for u in range(8):
                k = b * 8 + u
                out_ref[j, k] = rows_ref[order_ref[jnp.minimum(first + k, last)]]
            return c

        return lax.fori_loop(0, cap // 8, body, carry)

    lax.fori_loop(0, group_size, per_dst, 0)


def pick(order, table, rows, cap, group_size):
    return pl.pallas_call(
        functools.partial(pick_kernel, cap, group_size),
        out_shape=jax.ShapeDtypeStruct((group_size, cap, *rows.shape[1:]), rows.dtype),
        in_specs=[SMEM, SMEM, VMEM],
        out_specs=VMEM,
        name="pick_rows",
    )(order, table, rows)


def place_kernel(idx_ref, count_ref, in_ref, out_ref, held, staged, blank, in_sem, out_sem, blank_sem):
    slots, block, width = staged.shape
    total = in_ref.shape[0]
    parts = held.shape[1]
    load = pltpu.make_async_copy(in_ref, held.at[pl.ds(0, total)], in_sem)
    load.start()
    blank[...] = jnp.zeros(blank.shape, blank.dtype)
    held[total] = jnp.zeros(held.shape[1:], held.dtype)
    steps = out_ref.shape[0] // block
    live = pl.cdiv(count_ref[0], block)

    def clear(s):
        return pltpu.make_async_copy(blank, out_ref.at[pl.ds(s * block, block)], blank_sem)

    def store(s):
        slot = lax.rem(s, slots)
        return pltpu.make_async_copy(staged.at[slot], out_ref.at[pl.ds(s * block, block)], out_sem.at[slot])

    load.wait()

    def start_clear(s, carry):
        clear(s).start()
        return carry

    lax.fori_loop(live, steps, start_clear, 0)

    def step(s, carry):
        @pl.when(s >= slots)
        def _():
            store(s - slots).wait()

        slot = lax.rem(s, slots)

        def body(g, c):
            r = pl.multiple_of(g * 16, 16)
            rows = []
            for u in range(16):
                k = idx_ref[s * block + r + u]
                rows.append(jnp.concatenate([held[k, q] for q in range(parts)], 0))
            staged[slot, pl.ds(r, 16), :] = jnp.stack(rows, 0).reshape(16, width)
            return c

        lax.fori_loop(0, block // 16, body, 0)
        store(s).start()
        return carry

    lax.fori_loop(0, live, step, 0)

    def end_store(s, carry):
        store(s).wait()
        return carry

    lax.fori_loop(jnp.maximum(live - slots, 0), live, end_store, 0)

    def end_clear(s, carry):
        clear(s).wait()
        return carry

    lax.fori_loop(live, steps, end_clear, 0)


def place(idx, count, rows, width):
    n_out = idx.shape[0]
    block, slots = 128, 4
    return pl.pallas_call(
        place_kernel,
        out_shape=jax.ShapeDtypeStruct((n_out, width), rows.dtype),
        in_specs=[SMEM, SMEM, ANY],
        out_specs=ANY,
        scratch_shapes=[
            pltpu.VMEM((rows.shape[0] + 1, *rows.shape[1:]), rows.dtype),
            pltpu.VMEM((slots, block, width), rows.dtype),
            pltpu.VMEM((block, width), rows.dtype),
            pltpu.SemaphoreType.DMA,
            pltpu.SemaphoreType.DMA((slots,)),
            pltpu.SemaphoreType.DMA,
        ],
        name="place_rows",
    )(idx, count, rows)


def solution(mesh):
    group_size = mesh.shape["g"]

    def local_part(keys_loc, rows_loc):
        n_dev = keys_loc.shape[0]
        width = rows_loc.shape[1]
        cap_rows = 2 * n_dev // group_size
        sorted_keys, order = lax.sort((keys_loc, lax.iota(jnp.int32, n_dev)), num_keys=1)
        all_keys, rows = share_keys(sorted_keys.reshape(n_dev // LANES, LANES), rows_loc, group_size)
        table = plan(all_keys, BASE, RELAY * group_size)
        segs, slots = segments(table, all_keys, BASE, RELAY)
        merged, idx = lax.sort((segs.reshape(-1), slots.reshape(-1)), num_keys=1)
        own_count = table[OWN, :1]

        def with_relay():
            return place(idx, own_count, exchange(order, table, rows, BASE, RELAY, group_size), width)

        def direct():
            blocks = lax.all_to_all(pick(order, table, rows, cap_rows, group_size), "g", 0, 0, tiled=True)
            return place(idx, own_count, blocks.reshape(-1, *blocks.shape[2:]), width)

        merged_rows = lax.cond(table[SHORT, 0] > 0, with_relay, direct)
        return merged, merged_rows, own_count

    row_spec = P(("batch", "g"))
    mat_spec = P(("batch", "g"), None)
    return jax.shard_map(local_part, mesh=mesh, in_specs=(row_spec, mat_spec), out_specs=(row_spec, mat_spec, row_spec), check_vma=False)
```

```python
import functools

import jax
import jax.numpy as jnp
from jax import lax
from jax.experimental import pallas as pl
from jax.experimental.pallas import tpu as pltpu
from jax.sharding import PartitionSpec as P

PAD_KEY = 128.0
LANES = 128
SUB = 4
BASE = 65
RELAY = 2
WINDOW = 6
SIDE = 4
CORES = 2
SLOTS = (((0, 2), (2, 0)), ((0, 1), (2, 3)), ((0, 3), (2, 1)), ((1, 0), (3, 2)), ((3, 0), (1, 2)), ((3, 1), (1, 3)), ((3, 3), (1, 1)), ((2, 2),))
STEPS = ((0, 0, 1), *((dx, dy, dc) for slot in SLOTS for dc in (1, 0) for dx, dy in slot))

VMEM = pl.BlockSpec(memory_space=pltpu.VMEM)
SMEM = pl.BlockSpec(memory_space=pltpu.SMEM)
ANY = pl.BlockSpec(memory_space=pl.ANY)
MESH = pl.DeviceIdType.MESH
STARTS, COL_STARTS, COL_COUNTS, FROM_SRC, EXTRA, SHORT, OWN = range(7)


def bitonic_sort(keys, vals):
    rows, lanes = keys.shape
    pos = lax.broadcasted_iota(jnp.int32, keys.shape, 0) * lanes + lax.broadcasted_iota(jnp.int32, keys.shape, 1)

    def partner(x, j, low):
        axis, size, d = (1, lanes, j) if j < lanes else (0, rows, j // lanes)
        return jnp.where(low, pltpu.roll(x, size - d, axis), pltpu.roll(x, d, axis))

    k = 2
    while k <= rows * lanes:
        j = k // 2
        while j:
            low = (pos & j) == 0
            keep_min = jnp.logical_xor(low, (pos & k) != 0)
            other = partner(keys, j, low)
            swap = jnp.logical_or(jnp.logical_and(keep_min, keys > other), jnp.logical_and(jnp.logical_not(keep_min), keys < other))
            vals = jnp.where(swap, partner(vals, j, low), vals)
            keys = jnp.where(swap, other, keys)
            j //= 2
        k *= 2
    return keys, vals


def make_plan(me, cap, most, all_ref, edge_ref):
    group_size, tiles, _ = all_ref.shape
    n_dev = tiles * LANES
    per = n_dev // group_size
    each = LANES // per
    f32 = jnp.float32
    lane = lax.broadcasted_iota(jnp.int32, (tiles, LANES), 1)
    sub = lax.broadcasted_iota(jnp.int32, (tiles, LANES), 0)
    group_lane = lax.broadcasted_iota(jnp.int32, (group_size, LANES), 1)
    group_sub = lax.broadcasted_iota(jnp.int32, (group_size, LANES), 0)

    def samples(i):
        return [jnp.broadcast_to(all_ref[i, :, l * per : l * per + 1], (tiles, LANES)) for l in range(each)]

    fit = LANES // group_size
    packed = []
    for c in range(group_size // fit):
        acc = jnp.zeros((tiles, LANES), f32)
        for i in range(c * fit, (c + 1) * fit):
            for l, a in enumerate(samples(i)):
                acc = jnp.where(lane == (i % fit) * group_size + each * sub + l, a, acc)
        packed.append(jnp.sum(acc, axis=0, keepdims=True))
    target = lax.broadcasted_iota(jnp.int32, (1, LANES), 1) * group_size + group_size // 2
    target = jnp.where((target > group_size) & (target < group_size * group_size), target, -1).astype(f32)
    found = jnp.zeros((tiles, LANES), f32)
    for i in range(group_size):
        for a in samples(i):
            less = jnp.zeros((tiles, LANES), f32)
            for b in packed:
                less += (b < a).astype(f32)
            rank = jnp.sum(less, axis=1, keepdims=True)
            found += jnp.where(rank == target, a, 0.0)
    splitters = jnp.sum(found, axis=0, keepdims=True)
    splitters = jnp.sum(jnp.where(group_lane == group_sub, splitters, 0.0), axis=1, keepdims=True)
    splitters = jnp.where(group_sub == 0, -PAD_KEY, splitters)

    edge_ref[...] = jnp.zeros(edge_ref.shape, f32)

    def count(b, carry):
        edges = edge_ref[...]
        for u in range(4):
            i = b * 4 + u
            less = jnp.zeros((group_size, LANES), f32)
            for r in range(tiles):
                less += (all_ref[i, r : r + 1, :] < splitters).astype(f32)
            edges = jnp.where(group_lane == i, jnp.sum(less, axis=1, keepdims=True), edges)
        edge_ref[...] = edges
        return carry

    lax.fori_loop(0, group_size // 4, count, 0)
    edges = edge_ref[...]
    after = jnp.concatenate([edges[1:], jnp.full((1, LANES), n_dev, f32)], 0)
    counts = jnp.where(group_lane < group_size, after - edges, 0.0)
    over = jnp.maximum(counts - cap, 0.0)
    has = (over > 0).astype(f32)
    worst = jnp.maximum(jnp.max(jnp.sum(has, axis=0, keepdims=True), axis=1, keepdims=True), jnp.max(jnp.sum(has, axis=1, keepdims=True), axis=0, keepdims=True))
    most_over = jnp.max(jnp.max(over, axis=0, keepdims=True), axis=1, keepdims=True)
    short = ((worst <= 1) & (most_over <= most)).astype(f32)

    def to_row(column):
        return jnp.sum(jnp.where(group_lane == group_sub, column, 0.0), axis=0, keepdims=True)

    mine = group_lane == me
    starts = to_row(jnp.sum(jnp.where(mine, edges, 0.0), axis=1, keepdims=True))
    col_starts = jnp.sum(jnp.where(group_sub == me, edges, 0.0), axis=0, keepdims=True)
    col_counts = jnp.sum(jnp.where(group_sub == me, counts, 0.0), axis=0, keepdims=True)
    from_src = to_row(jnp.sum(has * group_lane.astype(f32), axis=1, keepdims=True))
    extra = jnp.sum(jnp.sum(jnp.where(mine, has * (edges + cap), 0.0), axis=0, keepdims=True), axis=1, keepdims=True)
    own = jnp.sum(col_counts, axis=1, keepdims=True)
    rows = [starts, col_starts, col_counts, from_src, extra, short, own, own]
    return jnp.concatenate([jnp.broadcast_to(r, (1, LANES)) for r in rows], 0).astype(jnp.int32)


def take_segments(cap, relay, table_ref, all_ref, out_ref, slot_ref):
    group_size, tiles, _ = all_ref.shape
    lane = lax.broadcasted_iota(jnp.int32, (1, LANES), 1)
    short = table_ref[SHORT, 0] > 0
    past = lane - cap
    relayed = group_size * cap + lax.rem(past, group_size) * relay + past // group_size
    unused = jnp.where(short, group_size * (cap + relay), group_size * LANES)
    for i in range(group_size):
        s = jnp.clip(table_ref[COL_STARTS, i], 0, tiles * LANES - 1)
        t = s // LANES
        off = s - t * LANES
        a = all_ref[i, pl.ds(t, 1), :]
        b = all_ref[i, pl.ds(jnp.minimum(t + 1, tiles - 1), 1), :]
        shift = lax.rem(LANES - off, LANES)
        a = pltpu.roll(a, shift, 1)
        b = pltpu.roll(b, shift, 1)
        v = jnp.where(lane < LANES - off, a, b)
        live = lane < table_ref[COL_COUNTS, i]
        out_ref[pl.ds(i, 1), :] = jnp.where(live, v, PAD_KEY)
        slot = jnp.where(short, jnp.where(past < 0, i * cap + lane, relayed), i * LANES + lane)
        slot_ref[pl.ds(i, 1), :] = jnp.where(live, slot, unused)


def sort_exchange_kernel(
    group_size, cap, relay, block,
    keys_ref, rows_ref,
    out_ref, merged_ref, idx_ref, order_ref, split_ref, table_ref,
    fetched, held, outgoing, first, arrived, second, mine, all_ref, edge_ref, seg_ref, slot_ref, order, table,
    in_sem, own_sem, send_sem, recv_sem,
):
    me = lax.axis_index("g")
    core, x, y = lax.rem(me, CORES), lax.rem(me // CORES, SIDE), me // (CORES * SIDE)
    n, width = rows_ref.shape
    tiles = width // LANES

    def peer(d):
        return lax.rem(me + d, group_size)

    barrier = pltpu.get_barrier_semaphore()
    for d in range(1, group_size):
        pl.semaphore_signal(barrier, inc=1, device_id={"g": peer(d)}, device_id_type=MESH)

    def fetch(s):
        return pltpu.make_async_copy(rows_ref.at[pl.ds(s * block, block)], fetched.at[s], in_sem.at[s])

    def split(s):
        fetch(s).wait()

        def body(g, carry):
            r = pl.multiple_of(g * 16, 16)
            v = fetched[s, pl.ds(r, 16), :].reshape(16, tiles, LANES)
            for q in range(tiles // SUB):
                held[pl.ds(s * block + r, 16), q] = v[:, SUB * q : SUB * (q + 1)]
            return carry

        lax.fori_loop(0, block // 16, body, 0)

    for s in range(n // block):
        fetch(s).start()
    shape = keys_ref.shape
    places = lax.broadcasted_iota(jnp.int32, shape, 0) * LANES + lax.broadcasted_iota(jnp.int32, shape, 1)
    sorted_keys, sorted_places = bitonic_sort(keys_ref[...], places)
    mine[...] = sorted_keys
    order_ref[...] = sorted_places
    all_ref[pl.ds(me, 1)] = sorted_keys[None]
    split(0)
    pl.semaphore_wait(barrier, group_size - 1)

    def remote(d, dst, src_ref, dst_ref, kind):
        return pltpu.make_async_remote_copy(
            src_ref=src_ref, dst_ref=dst_ref, send_sem=send_sem.at[kind, d], recv_sem=recv_sem.at[kind, d], device_id={"g": dst}, device_id_type=MESH
        )

    def share(d):
        return remote(d, peer(d), mine, all_ref.at[me], 3)

    def hop_one(d):
        return remote(d, peer(d), first.at[peer(d)], arrived.at[me], 1)

    def hop_two(d):
        return remote(d, peer(d), second.at[peer(d)], out_ref.at[pl.ds(group_size * cap + me * relay, relay)], 2)

    def far(s):
        dx, dy, dc = STEPS[s]
        return (lax.rem(y + dy, SIDE) * SIDE + lax.rem(x + dx, SIDE)) * CORES + lax.rem(core + dc, CORES)

    def base(s):
        return remote(s, far(s), outgoing.at[far(s)], out_ref.at[pl.ds(me * cap, cap)], 0)

    def each(act):
        def body(d, carry):
            act(d)
            return carry

        lax.fori_loop(1, group_size, body, 0)

    each(lambda d: share(d).start())
    for s in range(1, n // block):
        split(s)
    to_order = pltpu.make_async_copy(order_ref, order, own_sem.at[2])
    to_order.start()
    each(lambda d: share(d).wait())
    table_ref[...] = make_plan(me, cap, relay * group_size, all_ref, edge_ref)
    to_table = pltpu.make_async_copy(table_ref, table, own_sem.at[3])
    to_table.start()
    to_order.wait()
    to_table.wait()

    last = n - 1

    def row(k):
        k = jnp.minimum(k, last)
        return held[jnp.clip(order[k // LANES, lax.rem(k, LANES)], 0, last)]

    def gather(dst):
        begin = jnp.clip(table[STARTS, dst], 0, last)

        def body(b, carry):
            for u in range(5):
                k = b * 5 + u
                outgoing[dst, k] = row(begin + k)
            return carry

        lax.fori_loop(0, cap // 5, body, 0)

    extra = jnp.clip(table[EXTRA, 0], 0, last)

    def gather_extra(m, carry):
        for r in range(relay):
            first[m, r] = row(extra + r * group_size + m)
        return carry

    lax.fori_loop(0, group_size, gather_extra, 0)
    arrived[pl.ds(me, 1)] = first[pl.ds(me, 1)]
    gather(far(0))
    each(lambda d: hop_one(d).start())
    for s in range(group_size - 1):
        if s >= WINDOW:
            base(s - WINDOW).wait_send()
        if s + 1 < group_size - 1:
            gather(far(s + 1))
        base(s).start()
        if s == WINDOW:
            each(lambda d: hop_one(d).wait())
            for j in range(group_size):
                second[j] = arrived[jnp.clip(table[FROM_SRC, j], 0, group_size - 1)]
            gather(me)
        if s == WINDOW + 1:
            each(lambda d: hop_two(d).start())
            own_two = pltpu.make_async_copy(second.at[me], out_ref.at[pl.ds(group_size * cap + me * relay, relay)], own_sem.at[1])
            own_base = pltpu.make_async_copy(outgoing.at[me], out_ref.at[pl.ds(me * cap, cap)], own_sem.at[0])
            own_two.start()
            own_base.start()
        if s == WINDOW + 4:
            take_segments(cap, relay, table, all_ref, seg_ref, slot_ref)
            merged_ref[...], idx_ref[...] = bitonic_sort(seg_ref[...], slot_ref[...])
    keep = pltpu.make_async_copy(held, split_ref, own_sem.at[4])
    keep.start()
    for s in range(group_size - 1):
        if s >= group_size - 1 - WINDOW:
            base(s).wait_send()
        base(s).wait_recv()
    each(lambda d: hop_two(d).wait())
    own_two.wait()
    own_base.wait()
    keep.wait()


def sort_exchange(keys, rows, cap, relay, group_size):
    n, width = rows.shape
    block = 512
    row = (width // (SUB * LANES), SUB, LANES)
    segs = (group_size, LANES)
    sems = pltpu.SemaphoreType.DMA
    return pl.pallas_call(
        functools.partial(sort_exchange_kernel, group_size, cap, relay, block),
        out_shape=[
            jax.ShapeDtypeStruct((group_size * (cap + relay), *row), rows.dtype),
            jax.ShapeDtypeStruct(segs, keys.dtype),
            jax.ShapeDtypeStruct(segs, jnp.int32),
            jax.ShapeDtypeStruct(keys.shape, jnp.int32),
            jax.ShapeDtypeStruct((n, *row), rows.dtype),
            jax.ShapeDtypeStruct((8, LANES), jnp.int32),
        ],
        in_specs=[VMEM, ANY],
        out_specs=[ANY, VMEM, VMEM, VMEM, ANY, VMEM],
        scratch_shapes=[
            pltpu.VMEM((n // block, block, width), rows.dtype),
            pltpu.VMEM((n, *row), rows.dtype),
            pltpu.VMEM((group_size, cap, *row), rows.dtype),
            pltpu.VMEM((group_size, relay, *row), rows.dtype),
            pltpu.VMEM((group_size, relay, *row), rows.dtype),
            pltpu.VMEM((group_size, relay, *row), rows.dtype),
            pltpu.VMEM(keys.shape, keys.dtype),
            pltpu.VMEM((group_size, *keys.shape), keys.dtype),
            pltpu.VMEM(segs, jnp.float32),
            pltpu.VMEM(segs, keys.dtype),
            pltpu.VMEM(segs, jnp.int32),
            pltpu.SMEM(keys.shape, jnp.int32),
            pltpu.SMEM((8, LANES), jnp.int32),
            sems((n // block,)),
            sems((5,)),
            sems((4, group_size)),
            sems((4, group_size)),
        ],
        compiler_params=pltpu.CompilerParams(collective_id=0, has_side_effects=True),
        name="sort_exchange",
    )(keys, rows)


def pick_kernel(cap, group_size, order_ref, table_ref, rows_ref, out_ref):
    last = rows_ref.shape[0] - 1

    def per_dst(j, carry):
        first = table_ref[STARTS, j]

        def body(b, c):
            for u in range(8):
                k = b * 8 + u
                out_ref[j, k] = rows_ref[order_ref[jnp.minimum(first + k, last)]]
            return c

        return lax.fori_loop(0, cap // 8, body, carry)

    lax.fori_loop(0, group_size, per_dst, 0)


def pick(order, table, rows, cap, group_size):
    return pl.pallas_call(
        functools.partial(pick_kernel, cap, group_size),
        out_shape=jax.ShapeDtypeStruct((group_size, cap, *rows.shape[1:]), rows.dtype),
        in_specs=[SMEM, SMEM, VMEM],
        out_specs=VMEM,
        name="pick_rows",
    )(order, table, rows)


def place_kernel(idx_ref, count_ref, in_ref, out_ref, held, staged, blank, in_sem, out_sem, blank_sem):
    slots, block, width = staged.shape
    total = in_ref.shape[0]
    parts = held.shape[1]
    load = pltpu.make_async_copy(in_ref, held.at[pl.ds(0, total)], in_sem)
    load.start()
    blank[...] = jnp.zeros(blank.shape, blank.dtype)
    held[total] = jnp.zeros(held.shape[1:], held.dtype)
    steps = out_ref.shape[0] // block
    live = pl.cdiv(count_ref[0], block)

    def clear(s):
        return pltpu.make_async_copy(blank, out_ref.at[pl.ds(s * block, block)], blank_sem)

    def store(s):
        slot = lax.rem(s, slots)
        return pltpu.make_async_copy(staged.at[slot], out_ref.at[pl.ds(s * block, block)], out_sem.at[slot])

    load.wait()

    def start_clear(s, carry):
        clear(s).start()
        return carry

    lax.fori_loop(live, steps, start_clear, 0)

    def step(s, carry):
        @pl.when(s >= slots)
        def _():
            store(s - slots).wait()

        slot = lax.rem(s, slots)

        def body(g, c):
            r = pl.multiple_of(g * 16, 16)
            rows = []
            for u in range(16):
                k = idx_ref[s * block + r + u]
                rows.append(jnp.concatenate([held[k, q] for q in range(parts)], 0))
            staged[slot, pl.ds(r, 16), :] = jnp.stack(rows, 0).reshape(16, width)
            return c

        lax.fori_loop(0, block // 16, body, 0)
        store(s).start()
        return carry

    lax.fori_loop(0, live, step, 0)

    def end_store(s, carry):
        store(s).wait()
        return carry

    lax.fori_loop(jnp.maximum(live - slots, 0), live, end_store, 0)

    def end_clear(s, carry):
        clear(s).wait()
        return carry

    lax.fori_loop(live, steps, end_clear, 0)


def place(idx, count, rows, width):
    n_out = idx.shape[0]
    block, slots = 128, 4
    return pl.pallas_call(
        place_kernel,
        out_shape=jax.ShapeDtypeStruct((n_out, width), rows.dtype),
        in_specs=[SMEM, SMEM, ANY],
        out_specs=ANY,
        scratch_shapes=[
            pltpu.VMEM((rows.shape[0] + 1, *rows.shape[1:]), rows.dtype),
            pltpu.VMEM((slots, block, width), rows.dtype),
            pltpu.VMEM((block, width), rows.dtype),
            pltpu.SemaphoreType.DMA,
            pltpu.SemaphoreType.DMA((slots,)),
            pltpu.SemaphoreType.DMA,
        ],
        name="place_rows",
    )(idx, count, rows)


def solution(mesh):
    group_size = mesh.shape["g"]

    def local_part(keys_loc, rows_loc):
        n_dev = keys_loc.shape[0]
        width = rows_loc.shape[1]
        cap_rows = 2 * n_dev // group_size
        blocks, merged, idx, order, rows, table = sort_exchange(keys_loc.reshape(n_dev // LANES, LANES), rows_loc, BASE, RELAY, group_size)
        own_count = table[OWN, :1]
        idx = idx.reshape(-1)

        def arrived():
            return place(idx, own_count, blocks, width)

        def direct():
            wide = lax.all_to_all(pick(order.reshape(-1), table, rows, cap_rows, group_size), "g", 0, 0, tiled=True)
            return place(idx, own_count, wide.reshape(-1, *wide.shape[2:]), width)

        merged_rows = lax.cond(table[SHORT, 0] > 0, arrived, direct)
        return merged.reshape(-1), merged_rows, own_count

    row_spec = P(("batch", "g"))
    mat_spec = P(("batch", "g"), None)
    return jax.shard_map(local_part, mesh=mesh, in_specs=(row_spec, mat_spec), out_specs=(row_spec, mat_spec, row_spec), check_vma=False)
```

```python
import functools

import jax
import jax.numpy as jnp
from jax import lax
from jax.experimental import pallas as pl
from jax.experimental.pallas import tpu as pltpu
from jax.sharding import PartitionSpec as P

PAD_KEY = 128.0
LANES = 128
SUB = 4
BASE = 65
RELAY = 2
WINDOW = 6
SIDE = 4
CORES = 2
SLOTS = (((0, 2), (2, 0)), ((0, 1), (2, 3)), ((0, 3), (2, 1)), ((1, 0), (3, 2)), ((3, 0), (1, 2)), ((3, 1), (1, 3)), ((3, 3), (1, 1)), ((2, 2),))
STEPS = ((0, 0, 1), *((dx, dy, dc) for slot in SLOTS for dc in (1, 0) for dx, dy in slot))

VMEM = pl.BlockSpec(memory_space=pltpu.VMEM)
SMEM = pl.BlockSpec(memory_space=pltpu.SMEM)
ANY = pl.BlockSpec(memory_space=pl.ANY)
MESH = pl.DeviceIdType.MESH
STARTS, COL_STARTS, COL_COUNTS, FROM_SRC, EXTRA, SHORT, OWN = range(7)


def bitonic_sort(keys, vals):
    rows, lanes = keys.shape
    pos = lax.broadcasted_iota(jnp.int32, keys.shape, 0) * lanes + lax.broadcasted_iota(jnp.int32, keys.shape, 1)

    def partner(x, j, low):
        axis, size, d = (1, lanes, j) if j < lanes else (0, rows, j // lanes)
        return jnp.where(low, pltpu.roll(x, size - d, axis), pltpu.roll(x, d, axis))

    k = 2
    while k <= rows * lanes:
        j = k // 2
        while j:
            low = (pos & j) == 0
            keep_min = jnp.logical_xor(low, (pos & k) != 0)
            other = partner(keys, j, low)
            swap = jnp.logical_or(jnp.logical_and(keep_min, keys > other), jnp.logical_and(jnp.logical_not(keep_min), keys < other))
            vals = jnp.where(swap, partner(vals, j, low), vals)
            keys = jnp.where(swap, other, keys)
            j //= 2
        k *= 2
    return keys, vals


def sample_row(keys, group_size):
    rows, lanes = keys.shape
    per = rows * lanes // group_size
    each = lanes // per
    lane = lax.broadcasted_iota(jnp.int32, keys.shape, 1)
    sub = lax.broadcasted_iota(jnp.int32, keys.shape, 0)
    acc = jnp.zeros(keys.shape, keys.dtype)
    for l in range(each):
        acc = jnp.where(lane == each * sub + l, keys[:, l * per : l * per + 1], acc)
    return jnp.sum(acc, axis=0, keepdims=True)


def pick_splitters(samples):
    group_size = samples.shape[0]
    lane = lax.broadcasted_iota(jnp.int32, samples.shape, 1)
    sub = lax.broadcasted_iota(jnp.int32, samples.shape, 0)
    fit = LANES // group_size
    merged = samples
    for f in range(1, fit):
        merged = jnp.where(lax.rem(sub, fit) == f, pltpu.roll(samples, f * group_size, 1), merged)
    packed = [jnp.sum(merged[c * fit : (c + 1) * fit], axis=0, keepdims=True) for c in range(group_size // fit)]
    less = [jnp.zeros(samples.shape, jnp.float32) for _ in packed]
    for q in range(group_size):
        a = jnp.broadcast_to(samples[:, q : q + 1], samples.shape)
        less = [n + (a < b).astype(jnp.float32) for n, b in zip(less, packed)]
    target = (sub * group_size + group_size // 2).astype(jnp.float32)
    found = jnp.zeros(samples.shape, jnp.float32)
    for n, b in zip(less, packed):
        found += jnp.where(jnp.sum(n, axis=0, keepdims=True) == target, b, 0.0)
    return jnp.where(sub == 0, -PAD_KEY, jnp.sum(found, axis=1, keepdims=True))


def count_below(keys, splitters):
    less = jnp.zeros(splitters.shape, jnp.float32)
    for r in range(keys.shape[0]):
        less += (keys[r : r + 1] < splitters).astype(jnp.float32)
    return jnp.sum(less, axis=1, keepdims=True)


def to_row(column, shape):
    lane = lax.broadcasted_iota(jnp.int32, shape, 1)
    sub = lax.broadcasted_iota(jnp.int32, shape, 0)
    return jnp.sum(jnp.where(lane == sub, column, 0.0), axis=0, keepdims=True)


def to_table(rows):
    rows = rows + [rows[-1]] * (8 - len(rows))
    return jnp.concatenate([jnp.broadcast_to(r, (1, LANES)) for r in rows], 0).astype(jnp.int32)


def make_plan(me, cap, most, all_ref, split_ref, edge_ref):
    group_size, tiles, _ = all_ref.shape
    n_dev = tiles * LANES
    shape = edge_ref.shape
    lane = lax.broadcasted_iota(jnp.int32, shape, 1)
    sub = lax.broadcasted_iota(jnp.int32, shape, 0)
    splitters = split_ref[...]
    edge_ref[...] = jnp.zeros(shape, jnp.float32)

    def count(b, carry):
        edges = edge_ref[...]
        for u in range(4):
            i = b * 4 + u
            edges = jnp.where(lane == i, count_below(all_ref[i], splitters), edges)
        edge_ref[...] = edges
        return carry

    lax.fori_loop(0, group_size // 4, count, 0)
    edges = edge_ref[...]
    after = jnp.concatenate([edges[1:], jnp.full((1, LANES), n_dev, jnp.float32)], 0)
    counts = jnp.where(lane < group_size, after - edges, 0.0)
    over = jnp.maximum(counts - cap, 0.0)
    has = (over > 0).astype(jnp.float32)
    worst = jnp.maximum(jnp.max(jnp.sum(has, axis=0, keepdims=True), axis=1, keepdims=True), jnp.max(jnp.sum(has, axis=1, keepdims=True), axis=0, keepdims=True))
    most_over = jnp.max(jnp.max(over, axis=0, keepdims=True), axis=1, keepdims=True)
    short = ((worst <= 1) & (most_over <= most)).astype(jnp.float32)
    mine = lane == me
    starts = to_row(jnp.sum(jnp.where(mine, edges, 0.0), axis=1, keepdims=True), shape)
    col_starts = jnp.sum(jnp.where(sub == me, edges, 0.0), axis=0, keepdims=True)
    col_counts = jnp.sum(jnp.where(sub == me, counts, 0.0), axis=0, keepdims=True)
    from_src = to_row(jnp.sum(has * lane.astype(jnp.float32), axis=1, keepdims=True), shape)
    extra = jnp.sum(jnp.sum(jnp.where(mine, has * (edges + cap), 0.0), axis=0, keepdims=True), axis=1, keepdims=True)
    own = jnp.sum(col_counts, axis=1, keepdims=True)
    return to_table([starts, col_starts, col_counts, from_src, extra, short, own])


def take_segments(cap, relay, table_ref, all_ref, out_ref, slot_ref):
    group_size, tiles, _ = all_ref.shape
    lane = lax.broadcasted_iota(jnp.int32, (1, LANES), 1)
    short = table_ref[SHORT, 0] > 0
    past = lane - cap
    relayed = group_size * cap + lax.rem(past, group_size) * relay + past // group_size
    unused = jnp.where(short, group_size * (cap + relay), group_size * LANES)
    for i in range(group_size):
        s = jnp.clip(table_ref[COL_STARTS, i], 0, tiles * LANES - 1)
        t = s // LANES
        off = s - t * LANES
        a = all_ref[i, pl.ds(t, 1), :]
        b = all_ref[i, pl.ds(jnp.minimum(t + 1, tiles - 1), 1), :]
        shift = lax.rem(LANES - off, LANES)
        a = pltpu.roll(a, shift, 1)
        b = pltpu.roll(b, shift, 1)
        v = jnp.where(lane < LANES - off, a, b)
        live = lane < table_ref[COL_COUNTS, i]
        out_ref[pl.ds(i, 1), :] = jnp.where(live, v, PAD_KEY)
        slot = jnp.where(short, jnp.where(past < 0, i * cap + lane, relayed), i * LANES + lane)
        slot_ref[pl.ds(i, 1), :] = jnp.where(live, slot, unused)


def sort_exchange_kernel(
    group_size, cap, relay, block,
    keys_ref, rows_ref,
    out_ref, merged_ref, idx_ref, order_ref, split_ref, table_ref, own_ref, short_ref,
    fetched, held, outgoing, first, arrived, second, mine, all_ref, my_samples, samples, start_ref, splitters, edge_ref, seg_ref, slot_ref, order, starts, table,
    in_sem, own_sem, send_sem, recv_sem,
):
    me = lax.axis_index("g")
    core, x, y = lax.rem(me, CORES), lax.rem(me // CORES, SIDE), me // (CORES * SIDE)
    n, width = rows_ref.shape
    tiles = width // LANES

    def peer(d):
        return lax.rem(me + d, group_size)

    barrier = pltpu.get_barrier_semaphore()
    for d in range(1, group_size):
        pl.semaphore_signal(barrier, inc=1, device_id={"g": peer(d)}, device_id_type=MESH)

    def fetch(s):
        return pltpu.make_async_copy(rows_ref.at[pl.ds(s * block, block)], fetched.at[s], in_sem.at[s])

    def split(s):
        fetch(s).wait()

        def body(g, carry):
            r = pl.multiple_of(g * 16, 16)
            v = fetched[s, pl.ds(r, 16), :].reshape(16, tiles, LANES)
            for q in range(tiles // SUB):
                held[pl.ds(s * block + r, 16), q] = v[:, SUB * q : SUB * (q + 1)]
            return carry

        lax.fori_loop(0, block // 16, body, 0)

    for s in range(n // block):
        fetch(s).start()
    shape = keys_ref.shape
    places = lax.broadcasted_iota(jnp.int32, shape, 0) * LANES + lax.broadcasted_iota(jnp.int32, shape, 1)
    sorted_keys, sorted_places = bitonic_sort(keys_ref[...], places)
    mine[...] = sorted_keys
    order_ref[...] = sorted_places
    all_ref[pl.ds(me, 1)] = sorted_keys[None]
    my_samples[...] = sample_row(sorted_keys, group_size)
    samples[pl.ds(me, 1)] = my_samples[...][None]
    split(0)
    pl.semaphore_wait(barrier, group_size - 1)

    def remote(d, dst, src_ref, dst_ref, kind):
        return pltpu.make_async_remote_copy(
            src_ref=src_ref, dst_ref=dst_ref, send_sem=send_sem.at[kind, d], recv_sem=recv_sem.at[kind, d], device_id={"g": dst}, device_id_type=MESH
        )

    def share(d):
        return remote(d, peer(d), mine, all_ref.at[me], 3)

    def share_samples(d):
        return remote(d, peer(d), my_samples, samples.at[me], 4)

    def hop_one(d):
        return remote(d, peer(d), first.at[peer(d)], arrived.at[me], 1)

    def hop_two(d):
        return remote(d, peer(d), second.at[peer(d)], out_ref.at[pl.ds(group_size * cap + me * relay, relay)], 2)

    def far(s):
        dx, dy, dc = STEPS[s]
        return (lax.rem(y + dy, SIDE) * SIDE + lax.rem(x + dx, SIDE)) * CORES + lax.rem(core + dc, CORES)

    def base(s):
        return remote(s, far(s), outgoing.at[far(s)], out_ref.at[pl.ds(me * cap, cap)], 0)

    def each(act):
        def body(d, carry):
            act(d)
            return carry

        lax.fori_loop(1, group_size, body, 0)

    each(lambda d: share_samples(d).start())
    each(lambda d: share(d).start())
    to_order = pltpu.make_async_copy(order_ref, order, own_sem.at[2])
    to_order.start()
    for s in range(1, n // block):
        split(s)
    each(lambda d: share_samples(d).wait())
    splitters[...] = pick_splitters(samples[:, 0, :])
    start_ref[...] = to_table([to_row(count_below(mine[...], splitters[...]), edge_ref.shape)])
    to_starts = pltpu.make_async_copy(start_ref, starts, own_sem.at[3])
    to_starts.start()
    to_order.wait()
    to_starts.wait()

    last = n - 1

    def row(k):
        k = k & last
        return held[order[k >> 7, k & (LANES - 1)] & last]

    def gather(dst):
        begin = starts[STARTS, dst]

        def body(b, carry):
            for u in range(13):
                k = b * 13 + u
                outgoing[dst, k] = row(begin + k)
            return carry

        lax.fori_loop(0, cap // 13, body, 0)

    own_two = pltpu.make_async_copy(second.at[me], out_ref.at[pl.ds(group_size * cap + me * relay, relay)], own_sem.at[1])
    own_base = pltpu.make_async_copy(outgoing.at[me], out_ref.at[pl.ds(me * cap, cap)], own_sem.at[0])
    gather(far(0))
    for s in range(group_size - 1):
        if s >= WINDOW:
            base(s - WINDOW).wait_send()
        if s + 1 < group_size - 1:
            gather(far(s + 1))
        base(s).start()
        if s == WINDOW:
            each(lambda d: share(d).wait())
            table_ref[...] = make_plan(me, cap, relay * group_size, all_ref, splitters, edge_ref)
            to_smem = pltpu.make_async_copy(table_ref, table, own_sem.at[5])
            to_smem.start()
            gather(me)
            to_smem.wait()
        if s == WINDOW + 1:
            extra = table[EXTRA, 0]

            def gather_extra(b, carry):
                for u in range(8):
                    m = b * 8 + u
                    for r in range(relay):
                        first[m, r] = row(extra + r * group_size + m)
                return carry

            lax.fori_loop(0, group_size // 8, gather_extra, 0)
            arrived[pl.ds(me, 1)] = first[pl.ds(me, 1)]
            own_base.start()
        if s == WINDOW + 2:
            each(lambda d: hop_one(d).start())
        if s == WINDOW + 4:
            own_ref[0] = table[OWN, 0]
            short_ref[0] = table[SHORT, 0]
            take_segments(cap, relay, table, all_ref, seg_ref, slot_ref)
            merged_ref[...], idx_ref[...] = bitonic_sort(seg_ref[...], slot_ref[...])
        if s == WINDOW + 12:
            each(lambda d: hop_one(d).wait())
            for j in range(group_size):
                second[j] = arrived[table[FROM_SRC, j] & (group_size - 1)]
        if s == WINDOW + 13:
            each(lambda d: hop_two(d).start())
            own_two.start()
    keep = pltpu.make_async_copy(held, split_ref, own_sem.at[4])
    keep.start()
    for s in range(group_size - 1):
        if s >= group_size - 1 - WINDOW:
            base(s).wait_send()
        base(s).wait_recv()
    each(lambda d: hop_two(d).wait())
    own_two.wait()
    own_base.wait()
    keep.wait()


def sort_exchange(keys, rows, cap, relay, group_size):
    n, width = rows.shape
    block = 512
    row = (width // (SUB * LANES), SUB, LANES)
    segs = (group_size, LANES)
    sems = pltpu.SemaphoreType.DMA
    return pl.pallas_call(
        functools.partial(sort_exchange_kernel, group_size, cap, relay, block),
        out_shape=[
            jax.ShapeDtypeStruct((group_size * (cap + relay), *row), rows.dtype),
            jax.ShapeDtypeStruct(segs, keys.dtype),
            jax.ShapeDtypeStruct(segs, jnp.int32),
            jax.ShapeDtypeStruct(keys.shape, jnp.int32),
            jax.ShapeDtypeStruct((n, *row), rows.dtype),
            jax.ShapeDtypeStruct((8, LANES), jnp.int32),
            jax.ShapeDtypeStruct((1,), jnp.int32),
            jax.ShapeDtypeStruct((1,), jnp.int32),
        ],
        in_specs=[VMEM, ANY],
        out_specs=[ANY, VMEM, VMEM, VMEM, ANY, VMEM, SMEM, SMEM],
        scratch_shapes=[
            pltpu.VMEM((n // block, block, width), rows.dtype),
            pltpu.VMEM((n, *row), rows.dtype),
            pltpu.VMEM((group_size, cap, *row), rows.dtype),
            pltpu.VMEM((group_size, relay, *row), rows.dtype),
            pltpu.VMEM((group_size, relay, *row), rows.dtype),
            pltpu.VMEM((group_size, relay, *row), rows.dtype),
            pltpu.VMEM(keys.shape, keys.dtype),
            pltpu.VMEM((group_size, *keys.shape), keys.dtype),
            pltpu.VMEM((1, LANES), keys.dtype),
            pltpu.VMEM((group_size, 1, LANES), keys.dtype),
            pltpu.VMEM((8, LANES), jnp.int32),
            pltpu.VMEM(segs, keys.dtype),
            pltpu.VMEM(segs, jnp.float32),
            pltpu.VMEM(segs, keys.dtype),
            pltpu.VMEM(segs, jnp.int32),
            pltpu.SMEM(keys.shape, jnp.int32),
            pltpu.SMEM((8, LANES), jnp.int32),
            pltpu.SMEM((8, LANES), jnp.int32),
            sems((n // block,)),
            sems((6,)),
            sems((5, group_size)),
            sems((5, group_size)),
        ],
        compiler_params=pltpu.CompilerParams(collective_id=0, has_side_effects=True),
        name="sort_exchange",
    )(keys, rows)


def pick_kernel(cap, group_size, order_ref, table_ref, rows_ref, out_ref):
    last = rows_ref.shape[0] - 1

    def per_dst(j, carry):
        first = table_ref[STARTS, j]

        def body(b, c):
            for u in range(8):
                k = b * 8 + u
                out_ref[j, k] = rows_ref[order_ref[jnp.minimum(first + k, last)]]
            return c

        return lax.fori_loop(0, cap // 8, body, carry)

    lax.fori_loop(0, group_size, per_dst, 0)


def pick(order, table, rows, cap, group_size):
    return pl.pallas_call(
        functools.partial(pick_kernel, cap, group_size),
        out_shape=jax.ShapeDtypeStruct((group_size, cap, *rows.shape[1:]), rows.dtype),
        in_specs=[SMEM, SMEM, VMEM],
        out_specs=VMEM,
        name="pick_rows",
    )(order, table, rows)


def place_kernel(idx_ref, count_ref, in_ref, keys_ref, out_ref, out_keys_ref, held, staged, blank, in_sem, out_sem, blank_sem):
    slots, block, width = staged.shape
    total = in_ref.shape[0]
    parts = held.shape[1]
    load = pltpu.make_async_copy(in_ref, held.at[pl.ds(0, total)], in_sem)
    load.start()
    out_keys_ref[...] = keys_ref[...]
    blank[...] = jnp.zeros(blank.shape, blank.dtype)
    held[total] = jnp.zeros(held.shape[1:], held.dtype)
    steps = out_ref.shape[0] // block
    live = pl.cdiv(count_ref[0], block)

    def clear(s):
        return pltpu.make_async_copy(blank, out_ref.at[pl.ds(s * block, block)], blank_sem)

    def store(s):
        slot = lax.rem(s, slots)
        return pltpu.make_async_copy(staged.at[slot], out_ref.at[pl.ds(s * block, block)], out_sem.at[slot])

    load.wait()

    def start_clear(s, carry):
        clear(s).start()
        return carry

    lax.fori_loop(live, steps, start_clear, 0)

    def step(s, carry):
        @pl.when(s >= slots)
        def _():
            store(s - slots).wait()

        slot = lax.rem(s, slots)

        def body(g, c):
            r = pl.multiple_of(g * 16, 16)
            rows = []
            for u in range(16):
                k = idx_ref[s * block + r + u]
                rows.append(jnp.concatenate([held[k, q] for q in range(parts)], 0))
            staged[slot, pl.ds(r, 16), :] = jnp.stack(rows, 0).reshape(16, width)
            return c

        lax.fori_loop(0, block // 16, body, 0)
        store(s).start()
        return carry

    lax.fori_loop(0, live, step, 0)

    def end_store(s, carry):
        store(s).wait()
        return carry

    lax.fori_loop(jnp.maximum(live - slots, 0), live, end_store, 0)

    def end_clear(s, carry):
        clear(s).wait()
        return carry

    lax.fori_loop(live, steps, end_clear, 0)


def place(idx, count, rows, keys, width):
    n_out = idx.shape[0]
    block, slots = 128, 4
    return pl.pallas_call(
        place_kernel,
        out_shape=[jax.ShapeDtypeStruct((n_out, width), rows.dtype), jax.ShapeDtypeStruct(keys.shape, keys.dtype)],
        in_specs=[SMEM, SMEM, ANY, VMEM],
        out_specs=[ANY, VMEM],
        scratch_shapes=[
            pltpu.VMEM((rows.shape[0] + 1, *rows.shape[1:]), rows.dtype),
            pltpu.VMEM((slots, block, width), rows.dtype),
            pltpu.VMEM((block, width), rows.dtype),
            pltpu.SemaphoreType.DMA,
            pltpu.SemaphoreType.DMA((slots,)),
            pltpu.SemaphoreType.DMA,
        ],
        name="place_rows",
    )(idx, count, rows, keys)


def solution(mesh):
    group_size = mesh.shape["g"]

    def local_part(keys_loc, rows_loc):
        n_dev = keys_loc.shape[0]
        width = rows_loc.shape[1]
        cap_rows = 2 * n_dev // group_size
        blocks, merged, idx, order, rows, table, own_count, short = sort_exchange(keys_loc.reshape(n_dev // LANES, LANES), rows_loc, BASE, RELAY, group_size)
        idx = idx.reshape(-1)

        def arrived():
            return place(idx, own_count, blocks, merged, width)

        def direct():
            wide = lax.all_to_all(pick(order.reshape(-1), table, rows, cap_rows, group_size), "g", 0, 0, tiled=True)
            return place(idx, own_count, wide.reshape(-1, *wide.shape[2:]), merged, width)

        out_rows, out_keys = lax.cond(short[0] > 0, arrived, direct)
        return out_keys.reshape(-1), out_rows, own_count

    row_spec = P(("batch", "g"))
    mat_spec = P(("batch", "g"), None)
    return jax.shard_map(local_part, mesh=mesh, in_specs=(row_spec, mat_spec), out_specs=(row_spec, mat_spec, row_spec), check_vma=False)
```

```python
import functools

import jax
import jax.numpy as jnp
from jax import lax
from jax.experimental import pallas as pl
from jax.experimental.pallas import tpu as pltpu
from jax.sharding import PartitionSpec as P

PAD_KEY = 128.0
LANES = 128
SUB = 4
BASE = 65
RELAY = 2
WINDOW = 6
SIDE = 4
CORES = 2
SLOTS = (((0, 2), (2, 0)), ((0, 1), (2, 3)), ((0, 3), (2, 1)), ((1, 0), (3, 2)), ((3, 0), (1, 2)), ((3, 1), (1, 3)), ((3, 3), (1, 1)), ((2, 2),))
STEPS = ((0, 0, 1), *((dx, dy, dc) for slot in SLOTS for dc in (1, 0) for dx, dy in slot))

VMEM = pl.BlockSpec(memory_space=pltpu.VMEM)
SMEM = pl.BlockSpec(memory_space=pltpu.SMEM)
ANY = pl.BlockSpec(memory_space=pl.ANY)
MESH = pl.DeviceIdType.MESH
STARTS, COL_STARTS, COL_COUNTS, FROM_SRC, EXTRA, SHORT, OWN = range(7)


def bitonic_sort(keys, vals):
    rows, lanes = keys.shape
    pos = lax.broadcasted_iota(jnp.int32, keys.shape, 0) * lanes + lax.broadcasted_iota(jnp.int32, keys.shape, 1)

    def partner(x, j, low):
        axis, size, d = (1, lanes, j) if j < lanes else (0, rows, j // lanes)
        return jnp.where(low, pltpu.roll(x, size - d, axis), pltpu.roll(x, d, axis))

    k = 2
    while k <= rows * lanes:
        j = k // 2
        while j:
            low = (pos & j) == 0
            keep_min = jnp.logical_xor(low, (pos & k) != 0)
            other = partner(keys, j, low)
            swap = jnp.logical_or(jnp.logical_and(keep_min, keys > other), jnp.logical_and(jnp.logical_not(keep_min), keys < other))
            vals = jnp.where(swap, partner(vals, j, low), vals)
            keys = jnp.where(swap, other, keys)
            j //= 2
        k *= 2
    return keys, vals


def sample_row(keys, group_size):
    rows, lanes = keys.shape
    per = rows * lanes // group_size
    each = lanes // per
    lane = lax.broadcasted_iota(jnp.int32, keys.shape, 1)
    sub = lax.broadcasted_iota(jnp.int32, keys.shape, 0)
    acc = jnp.zeros(keys.shape, keys.dtype)
    for l in range(each):
        acc = jnp.where(lane == each * sub + l, keys[:, l * per : l * per + 1], acc)
    return jnp.sum(acc, axis=0, keepdims=True)


def pick_splitters(samples):
    group_size = samples.shape[0]
    lane = lax.broadcasted_iota(jnp.int32, samples.shape, 1)
    sub = lax.broadcasted_iota(jnp.int32, samples.shape, 0)
    fit = LANES // group_size
    merged = samples
    for f in range(1, fit):
        merged = jnp.where(lax.rem(sub, fit) == f, pltpu.roll(samples, f * group_size, 1), merged)
    packed = [jnp.sum(merged[c * fit : (c + 1) * fit], axis=0, keepdims=True) for c in range(group_size // fit)]
    less = [jnp.zeros(samples.shape, jnp.float32) for _ in packed]
    for q in range(group_size):
        a = jnp.broadcast_to(samples[:, q : q + 1], samples.shape)
        less = [n + (a < b).astype(jnp.float32) for n, b in zip(less, packed)]
    target = (sub * group_size + group_size // 2).astype(jnp.float32)
    found = jnp.zeros(samples.shape, jnp.float32)
    for n, b in zip(less, packed):
        found += jnp.where(jnp.sum(n, axis=0, keepdims=True) == target, b, 0.0)
    return jnp.where(sub == 0, -PAD_KEY, jnp.sum(found, axis=1, keepdims=True))


def count_below(keys, splitters):
    less = jnp.zeros(splitters.shape, jnp.float32)
    for r in range(keys.shape[0]):
        less += (keys[r : r + 1] < splitters).astype(jnp.float32)
    return jnp.sum(less, axis=1, keepdims=True)


def to_row(column, shape):
    lane = lax.broadcasted_iota(jnp.int32, shape, 1)
    sub = lax.broadcasted_iota(jnp.int32, shape, 0)
    return jnp.sum(jnp.where(lane == sub, column, 0.0), axis=0, keepdims=True)


def to_table(rows):
    rows = rows + [rows[-1]] * (8 - len(rows))
    return jnp.concatenate([jnp.broadcast_to(r, (1, LANES)) for r in rows], 0).astype(jnp.int32)


def make_plan(me, cap, most, all_ref, split_ref, edge_ref):
    group_size, tiles, _ = all_ref.shape
    n_dev = tiles * LANES
    shape = edge_ref.shape
    lane = lax.broadcasted_iota(jnp.int32, shape, 1)
    sub = lax.broadcasted_iota(jnp.int32, shape, 0)
    splitters = split_ref[...]
    edge_ref[...] = jnp.zeros(shape, jnp.float32)

    def count(b, carry):
        edges = edge_ref[...]
        for u in range(4):
            i = b * 4 + u
            edges = jnp.where(lane == i, count_below(all_ref[i], splitters), edges)
        edge_ref[...] = edges
        return carry

    lax.fori_loop(0, group_size // 4, count, 0)
    edges = edge_ref[...]
    after = jnp.concatenate([edges[1:], jnp.full((1, LANES), n_dev, jnp.float32)], 0)
    counts = jnp.where(lane < group_size, after - edges, 0.0)
    over = jnp.maximum(counts - cap, 0.0)
    has = (over > 0).astype(jnp.float32)
    worst = jnp.maximum(jnp.max(jnp.sum(has, axis=0, keepdims=True), axis=1, keepdims=True), jnp.max(jnp.sum(has, axis=1, keepdims=True), axis=0, keepdims=True))
    most_over = jnp.max(jnp.max(over, axis=0, keepdims=True), axis=1, keepdims=True)
    short = ((worst <= 1) & (most_over <= most)).astype(jnp.float32)
    mine = lane == me
    starts = to_row(jnp.sum(jnp.where(mine, edges, 0.0), axis=1, keepdims=True), shape)
    col_starts = jnp.sum(jnp.where(sub == me, edges, 0.0), axis=0, keepdims=True)
    col_counts = jnp.sum(jnp.where(sub == me, counts, 0.0), axis=0, keepdims=True)
    from_src = to_row(jnp.sum(has * lane.astype(jnp.float32), axis=1, keepdims=True), shape)
    extra = jnp.sum(jnp.sum(jnp.where(mine, has * (edges + cap), 0.0), axis=0, keepdims=True), axis=1, keepdims=True)
    own = jnp.sum(col_counts, axis=1, keepdims=True)
    return to_table([starts, col_starts, col_counts, from_src, extra, short, own])


def take_segments(cap, relay, table_ref, all_ref, out_ref, slot_ref):
    group_size, tiles, _ = all_ref.shape
    lane = lax.broadcasted_iota(jnp.int32, (1, LANES), 1)
    short = table_ref[SHORT, 0] > 0
    past = lane - cap
    relayed = group_size * cap + lax.rem(past, group_size) * relay + past // group_size
    unused = jnp.where(short, group_size * (cap + relay), group_size * LANES)
    for i in range(group_size):
        s = jnp.clip(table_ref[COL_STARTS, i], 0, tiles * LANES - 1)
        t = s // LANES
        off = s - t * LANES
        a = all_ref[i, pl.ds(t, 1), :]
        b = all_ref[i, pl.ds(jnp.minimum(t + 1, tiles - 1), 1), :]
        shift = lax.rem(LANES - off, LANES)
        a = pltpu.roll(a, shift, 1)
        b = pltpu.roll(b, shift, 1)
        v = jnp.where(lane < LANES - off, a, b)
        live = lane < table_ref[COL_COUNTS, i]
        out_ref[pl.ds(i, 1), :] = jnp.where(live, v, PAD_KEY)
        slot = jnp.where(short, jnp.where(past < 0, i * cap + lane, relayed), i * LANES + lane)
        slot_ref[pl.ds(i, 1), :] = jnp.where(live, slot, unused)


def sort_exchange_kernel(
    group_size, cap, relay, block,
    keys_ref, rows_ref,
    out_ref, merged_ref, idx_ref, order_ref, split_ref, table_ref, own_ref, short_ref,
    fetched, held, outgoing, first, arrived, second, mine, all_ref, my_samples, samples, start_ref, splitters, edge_ref, seg_ref, slot_ref, order, starts, table,
    in_sem, own_sem, send_sem, recv_sem,
):
    me = lax.axis_index("g")
    core, x, y = lax.rem(me, CORES), lax.rem(me // CORES, SIDE), me // (CORES * SIDE)
    n, width = rows_ref.shape
    tiles = width // LANES

    def peer(d):
        return lax.rem(me + d, group_size)

    barrier = pltpu.get_barrier_semaphore()
    for d in range(1, group_size):
        pl.semaphore_signal(barrier, inc=1, device_id={"g": peer(d)}, device_id_type=MESH)

    def fetch(s):
        return pltpu.make_async_copy(rows_ref.at[pl.ds(s * block, block)], fetched.at[s], in_sem.at[s])

    def split(s):
        fetch(s).wait()

        def body(g, carry):
            r = pl.multiple_of(g * 16, 16)
            v = fetched[s, pl.ds(r, 16), :].reshape(16, tiles, LANES)
            for q in range(tiles // SUB):
                held[pl.ds(s * block + r, 16), q] = v[:, SUB * q : SUB * (q + 1)]
            return carry

        lax.fori_loop(0, block // 16, body, 0)

    for s in range(n // block):
        fetch(s).start()
    shape = keys_ref.shape
    places = lax.broadcasted_iota(jnp.int32, shape, 0) * LANES + lax.broadcasted_iota(jnp.int32, shape, 1)
    sorted_keys, sorted_places = bitonic_sort(keys_ref[...], places)
    mine[...] = sorted_keys
    order_ref[...] = sorted_places
    all_ref[pl.ds(me, 1)] = sorted_keys[None]
    my_samples[...] = sample_row(sorted_keys, group_size)
    samples[pl.ds(me, 1)] = my_samples[...][None]
    split(0)
    pl.semaphore_wait(barrier, group_size - 1)

    def remote(d, dst, src_ref, dst_ref, kind):
        return pltpu.make_async_remote_copy(
            src_ref=src_ref, dst_ref=dst_ref, send_sem=send_sem.at[kind, d], recv_sem=recv_sem.at[kind, d], device_id={"g": dst}, device_id_type=MESH
        )

    def share(d):
        return remote(d, peer(d), mine, all_ref.at[me], 3)

    def share_samples(d):
        return remote(d, peer(d), my_samples, samples.at[me], 4)

    def hop_one(d):
        return remote(d, peer(d), first.at[peer(d)], arrived.at[me], 1)

    def hop_two(d):
        return remote(d, peer(d), second.at[peer(d)], out_ref.at[pl.ds(group_size * cap + me * relay, relay)], 2)

    def far(s):
        dx, dy, dc = STEPS[s]
        return (lax.rem(y + dy, SIDE) * SIDE + lax.rem(x + dx, SIDE)) * CORES + lax.rem(core + dc, CORES)

    def base(s):
        return remote(s, far(s), outgoing.at[far(s)], out_ref.at[pl.ds(me * cap, cap)], 0)

    def each(act):
        def body(d, carry):
            act(d)
            return carry

        lax.fori_loop(1, group_size, body, 0)

    each(lambda d: share_samples(d).start())
    each(lambda d: share(d).start())
    to_order = pltpu.make_async_copy(order_ref, order, own_sem.at[2])
    to_order.start()
    for s in range(1, n // block):
        split(s)
    each(lambda d: share_samples(d).wait())
    for i in range(group_size):
        edge_ref[i : i + 1] = samples[i]
    splitters[...] = pick_splitters(edge_ref[...])
    start_ref[...] = to_table([to_row(count_below(mine[...], splitters[...]), edge_ref.shape)])
    to_starts = pltpu.make_async_copy(start_ref, starts, own_sem.at[3])
    to_starts.start()
    to_order.wait()
    to_starts.wait()

    last = n - 1

    def row(k):
        k = k & last
        return held[order[k >> 7, k & (LANES - 1)] & last]

    def gather(dst):
        begin = starts[STARTS, dst]

        def body(b, carry):
            for u in range(13):
                k = b * 13 + u
                outgoing[dst, k] = row(begin + k)
            return carry

        lax.fori_loop(0, cap // 13, body, 0)

    own_two = pltpu.make_async_copy(second.at[me], out_ref.at[pl.ds(group_size * cap + me * relay, relay)], own_sem.at[1])
    own_base = pltpu.make_async_copy(outgoing.at[me], out_ref.at[pl.ds(me * cap, cap)], own_sem.at[0])
    gather(far(0))
    for s in range(group_size - 1):
        if s >= WINDOW:
            base(s - WINDOW).wait_send()
        if s + 1 < group_size - 1:
            gather(far(s + 1))
        base(s).start()
        if s == WINDOW:
            each(lambda d: share(d).wait())
            table_ref[...] = make_plan(me, cap, relay * group_size, all_ref, splitters, edge_ref)
            to_smem = pltpu.make_async_copy(table_ref, table, own_sem.at[5])
            to_smem.start()
            gather(me)
            to_smem.wait()
        if s == WINDOW + 1:
            extra = table[EXTRA, 0]

            def gather_extra(b, carry):
                for u in range(8):
                    m = b * 8 + u
                    for r in range(relay):
                        first[m, r] = row(extra + r * group_size + m)
                return carry

            lax.fori_loop(0, group_size // 8, gather_extra, 0)
            arrived[pl.ds(me, 1)] = first[pl.ds(me, 1)]
            own_base.start()
        if s == WINDOW + 2:
            each(lambda d: hop_one(d).start())
        if s == WINDOW + 4:
            own_ref[0] = table[OWN, 0]
            short_ref[0] = table[SHORT, 0]
            take_segments(cap, relay, table, all_ref, seg_ref, slot_ref)
            merged_ref[...], idx_ref[...] = bitonic_sort(seg_ref[...], slot_ref[...])
        if s == WINDOW + 12:
            each(lambda d: hop_one(d).wait())
            for j in range(group_size):
                second[j] = arrived[table[FROM_SRC, j] & (group_size - 1)]
        if s == WINDOW + 13:
            each(lambda d: hop_two(d).start())
            own_two.start()
    keep = pltpu.make_async_copy(held, split_ref, own_sem.at[4])
    keep.start()
    for s in range(group_size - 1):
        if s >= group_size - 1 - WINDOW:
            base(s).wait_send()
        base(s).wait_recv()
    each(lambda d: hop_two(d).wait())
    own_two.wait()
    own_base.wait()
    keep.wait()


def sort_exchange(keys, rows, cap, relay, group_size):
    n, width = rows.shape
    block = 512
    row = (width // (SUB * LANES), SUB, LANES)
    segs = (group_size, LANES)
    sems = pltpu.SemaphoreType.DMA
    return pl.pallas_call(
        functools.partial(sort_exchange_kernel, group_size, cap, relay, block),
        out_shape=[
            jax.ShapeDtypeStruct((group_size * (cap + relay), *row), rows.dtype),
            jax.ShapeDtypeStruct(segs, keys.dtype),
            jax.ShapeDtypeStruct(segs, jnp.int32),
            jax.ShapeDtypeStruct(keys.shape, jnp.int32),
            jax.ShapeDtypeStruct((n, *row), rows.dtype),
            jax.ShapeDtypeStruct((8, LANES), jnp.int32),
            jax.ShapeDtypeStruct((1,), jnp.int32),
            jax.ShapeDtypeStruct((1,), jnp.int32),
        ],
        in_specs=[VMEM, ANY],
        out_specs=[ANY, VMEM, VMEM, VMEM, ANY, VMEM, SMEM, SMEM],
        scratch_shapes=[
            pltpu.VMEM((n // block, block, width), rows.dtype),
            pltpu.VMEM((n, *row), rows.dtype),
            pltpu.VMEM((group_size, cap, *row), rows.dtype),
            pltpu.VMEM((group_size, relay, *row), rows.dtype),
            pltpu.VMEM((group_size, relay, *row), rows.dtype),
            pltpu.VMEM((group_size, relay, *row), rows.dtype),
            pltpu.VMEM(keys.shape, keys.dtype),
            pltpu.VMEM((group_size, *keys.shape), keys.dtype),
            pltpu.VMEM((1, LANES), keys.dtype),
            pltpu.VMEM((group_size, 1, LANES), keys.dtype),
            pltpu.VMEM((8, LANES), jnp.int32),
            pltpu.VMEM(segs, keys.dtype),
            pltpu.VMEM(segs, jnp.float32),
            pltpu.VMEM(segs, keys.dtype),
            pltpu.VMEM(segs, jnp.int32),
            pltpu.SMEM(keys.shape, jnp.int32),
            pltpu.SMEM((8, LANES), jnp.int32),
            pltpu.SMEM((8, LANES), jnp.int32),
            sems((n // block,)),
            sems((6,)),
            sems((5, group_size)),
            sems((5, group_size)),
        ],
        compiler_params=pltpu.CompilerParams(collective_id=0, has_side_effects=True),
        name="sort_exchange",
    )(keys, rows)


def pick_kernel(cap, group_size, order_ref, table_ref, rows_ref, out_ref):
    last = rows_ref.shape[0] - 1

    def per_dst(j, carry):
        first = table_ref[STARTS, j]

        def body(b, c):
            for u in range(8):
                k = b * 8 + u
                out_ref[j, k] = rows_ref[order_ref[jnp.minimum(first + k, last)]]
            return c

        return lax.fori_loop(0, cap // 8, body, carry)

    lax.fori_loop(0, group_size, per_dst, 0)


def pick(order, table, rows, cap, group_size):
    return pl.pallas_call(
        functools.partial(pick_kernel, cap, group_size),
        out_shape=jax.ShapeDtypeStruct((group_size, cap, *rows.shape[1:]), rows.dtype),
        in_specs=[SMEM, SMEM, VMEM],
        out_specs=VMEM,
        name="pick_rows",
    )(order, table, rows)


def place_kernel(idx_ref, count_ref, in_ref, keys_ref, out_ref, out_keys_ref, held, staged, blank, in_sem, out_sem, blank_sem):
    slots, block, width = staged.shape
    total = in_ref.shape[0]
    parts = held.shape[1]
    load = pltpu.make_async_copy(in_ref, held.at[pl.ds(0, total)], in_sem)
    load.start()
    out_keys_ref[...] = keys_ref[...]
    blank[...] = jnp.zeros(blank.shape, blank.dtype)
    held[total] = jnp.zeros(held.shape[1:], held.dtype)
    steps = out_ref.shape[0] // block
    live = pl.cdiv(count_ref[0], block)

    def clear(s):
        return pltpu.make_async_copy(blank, out_ref.at[pl.ds(s * block, block)], blank_sem)

    def store(s):
        slot = lax.rem(s, slots)
        return pltpu.make_async_copy(staged.at[slot], out_ref.at[pl.ds(s * block, block)], out_sem.at[slot])

    load.wait()

    def start_clear(s, carry):
        clear(s).start()
        return carry

    lax.fori_loop(live, steps, start_clear, 0)

    def step(s, carry):
        @pl.when(s >= slots)
        def _():
            store(s - slots).wait()

        slot = lax.rem(s, slots)

        def body(g, c):
            r = pl.multiple_of(g * 16, 16)
            rows = []
            for u in range(16):
                k = idx_ref[s * block + r + u]
                rows.append(jnp.concatenate([held[k, q] for q in range(parts)], 0))
            staged[slot, pl.ds(r, 16), :] = jnp.stack(rows, 0).reshape(16, width)
            return c

        lax.fori_loop(0, block // 16, body, 0)
        store(s).start()
        return carry

    lax.fori_loop(0, live, step, 0)

    def end_store(s, carry):
        store(s).wait()
        return carry

    lax.fori_loop(jnp.maximum(live - slots, 0), live, end_store, 0)

    def end_clear(s, carry):
        clear(s).wait()
        return carry

    lax.fori_loop(live, steps, end_clear, 0)


def place(idx, count, rows, keys, width):
    n_out = idx.shape[0]
    block, slots = 128, 4
    return pl.pallas_call(
        place_kernel,
        out_shape=[jax.ShapeDtypeStruct((n_out, width), rows.dtype), jax.ShapeDtypeStruct(keys.shape, keys.dtype)],
        in_specs=[SMEM, SMEM, ANY, VMEM],
        out_specs=[ANY, VMEM],
        scratch_shapes=[
            pltpu.VMEM((rows.shape[0] + 1, *rows.shape[1:]), rows.dtype),
            pltpu.VMEM((slots, block, width), rows.dtype),
            pltpu.VMEM((block, width), rows.dtype),
            pltpu.SemaphoreType.DMA,
            pltpu.SemaphoreType.DMA((slots,)),
            pltpu.SemaphoreType.DMA,
        ],
        name="place_rows",
    )(idx, count, rows, keys)


def solution(mesh):
    group_size = mesh.shape["g"]

    def local_part(keys_loc, rows_loc):
        n_dev = keys_loc.shape[0]
        width = rows_loc.shape[1]
        cap_rows = 2 * n_dev // group_size
        blocks, merged, idx, order, rows, table, own_count, short = sort_exchange(keys_loc.reshape(n_dev // LANES, LANES), rows_loc, BASE, RELAY, group_size)
        idx = idx.reshape(-1)

        def arrived():
            return place(idx, own_count, blocks, merged, width)

        def direct():
            wide = lax.all_to_all(pick(order.reshape(-1), table, rows, cap_rows, group_size), "g", 0, 0, tiled=True)
            return place(idx, own_count, wide.reshape(-1, *wide.shape[2:]), merged, width)

        out_rows, out_keys = lax.cond(short[0] > 0, arrived, direct)
        return out_keys.reshape(-1), out_rows, own_count

    row_spec = P(("batch", "g"))
    mat_spec = P(("batch", "g"), None)
    return jax.shard_map(local_part, mesh=mesh, in_specs=(row_spec, mat_spec), out_specs=(row_spec, mat_spec, row_spec), check_vma=False)
```

```python
import functools

import jax
import jax.numpy as jnp
from jax import lax
from jax.experimental import pallas as pl
from jax.experimental.pallas import tpu as pltpu
from jax.sharding import PartitionSpec as P

PAD_KEY = 128.0
LANES = 128
SUB = 4
BASE = 65
RELAY = 2
FIRST, SECOND = 12, 22
SIDE = 4
CORES = 2
SLOTS = (((0, 2), (2, 0)), ((0, 1), (2, 3)), ((0, 3), (2, 1)), ((1, 0), (3, 2)), ((3, 0), (1, 2)), ((3, 1), (1, 3)), ((3, 3), (1, 1)), ((2, 2),))
STEPS = ((0, 0, 1), *((dx, dy, dc) for slot in SLOTS for dc in (1, 0) for dx, dy in slot))

VMEM = pl.BlockSpec(memory_space=pltpu.VMEM)
SMEM = pl.BlockSpec(memory_space=pltpu.SMEM)
ANY = pl.BlockSpec(memory_space=pl.ANY)
MESH = pl.DeviceIdType.MESH
STARTS, COL_STARTS, COL_COUNTS, FROM_SRC, EXTRA, SHORT, OWN = range(7)


def bitonic_sort(keys, vals):
    rows, lanes = keys.shape
    pos = lax.broadcasted_iota(jnp.int32, keys.shape, 0) * lanes + lax.broadcasted_iota(jnp.int32, keys.shape, 1)

    def partner(x, j, low):
        axis, size, d = (1, lanes, j) if j < lanes else (0, rows, j // lanes)
        return jnp.where(low, pltpu.roll(x, size - d, axis), pltpu.roll(x, d, axis))

    k = 2
    while k <= rows * lanes:
        j = k // 2
        while j:
            low = (pos & j) == 0
            keep_min = jnp.logical_xor(low, (pos & k) != 0)
            other = partner(keys, j, low)
            swap = jnp.logical_or(jnp.logical_and(keep_min, keys > other), jnp.logical_and(jnp.logical_not(keep_min), keys < other))
            vals = jnp.where(swap, partner(vals, j, low), vals)
            keys = jnp.where(swap, other, keys)
            j //= 2
        k *= 2
    return keys, vals


def sample_row(keys, group_size):
    rows, lanes = keys.shape
    per = rows * lanes // group_size
    each = lanes // per
    lane = lax.broadcasted_iota(jnp.int32, keys.shape, 1)
    sub = lax.broadcasted_iota(jnp.int32, keys.shape, 0)
    acc = jnp.zeros(keys.shape, keys.dtype)
    for l in range(each):
        acc = jnp.where(lane == each * sub + l, keys[:, l * per : l * per + 1], acc)
    return jnp.sum(acc, axis=0, keepdims=True)


def pick_splitters(samples):
    group_size = samples.shape[0]
    lane = lax.broadcasted_iota(jnp.int32, samples.shape, 1)
    sub = lax.broadcasted_iota(jnp.int32, samples.shape, 0)
    fit = LANES // group_size
    merged = samples
    for f in range(1, fit):
        merged = jnp.where(lax.rem(sub, fit) == f, pltpu.roll(samples, f * group_size, 1), merged)
    packed = [jnp.sum(merged[c * fit : (c + 1) * fit], axis=0, keepdims=True) for c in range(group_size // fit)]
    less = [jnp.zeros(samples.shape, jnp.float32) for _ in packed]
    for q in range(group_size):
        a = jnp.broadcast_to(samples[:, q : q + 1], samples.shape)
        less = [n + (a < b).astype(jnp.float32) for n, b in zip(less, packed)]
    target = (sub * group_size + group_size // 2).astype(jnp.float32)
    found = jnp.zeros(samples.shape, jnp.float32)
    for n, b in zip(less, packed):
        found += jnp.where(jnp.sum(n, axis=0, keepdims=True) == target, b, 0.0)
    return jnp.where(sub == 0, -PAD_KEY, jnp.sum(found, axis=1, keepdims=True))


def count_below(keys, splitters):
    less = jnp.zeros(splitters.shape, jnp.float32)
    for r in range(keys.shape[0]):
        less += (keys[r : r + 1] < splitters).astype(jnp.float32)
    return jnp.sum(less, axis=1, keepdims=True)


def to_row(column, shape):
    lane = lax.broadcasted_iota(jnp.int32, shape, 1)
    sub = lax.broadcasted_iota(jnp.int32, shape, 0)
    return jnp.sum(jnp.where(lane == sub, column, 0.0), axis=0, keepdims=True)


def to_table(rows):
    rows = rows + [rows[-1]] * (8 - len(rows))
    return jnp.concatenate([jnp.broadcast_to(r, (1, LANES)) for r in rows], 0).astype(jnp.int32)


def make_plan(me, cap, most, all_ref, split_ref, edge_ref):
    group_size, tiles, _ = all_ref.shape
    n_dev = tiles * LANES
    shape = edge_ref.shape
    lane = lax.broadcasted_iota(jnp.int32, shape, 1)
    sub = lax.broadcasted_iota(jnp.int32, shape, 0)
    splitters = split_ref[...]
    edge_ref[...] = jnp.zeros(shape, jnp.float32)

    def count(b, carry):
        edges = edge_ref[...]
        for u in range(4):
            i = b * 4 + u
            edges = jnp.where(lane == i, count_below(all_ref[i], splitters), edges)
        edge_ref[...] = edges
        return carry

    lax.fori_loop(0, group_size // 4, count, 0)
    edges = edge_ref[...]
    after = jnp.concatenate([edges[1:], jnp.full((1, LANES), n_dev, jnp.float32)], 0)
    counts = jnp.where(lane < group_size, after - edges, 0.0)
    over = jnp.maximum(counts - cap, 0.0)
    has = (over > 0).astype(jnp.float32)
    worst = jnp.maximum(jnp.max(jnp.sum(has, axis=0, keepdims=True), axis=1, keepdims=True), jnp.max(jnp.sum(has, axis=1, keepdims=True), axis=0, keepdims=True))
    most_over = jnp.max(jnp.max(over, axis=0, keepdims=True), axis=1, keepdims=True)
    short = ((worst <= 1) & (most_over <= most)).astype(jnp.float32)
    mine = lane == me
    starts = to_row(jnp.sum(jnp.where(mine, edges, 0.0), axis=1, keepdims=True), shape)
    col_starts = jnp.sum(jnp.where(sub == me, edges, 0.0), axis=0, keepdims=True)
    col_counts = jnp.sum(jnp.where(sub == me, counts, 0.0), axis=0, keepdims=True)
    from_src = to_row(jnp.sum(has * lane.astype(jnp.float32), axis=1, keepdims=True), shape)
    extra = jnp.sum(jnp.sum(jnp.where(mine, has * (edges + cap), 0.0), axis=0, keepdims=True), axis=1, keepdims=True)
    own = jnp.sum(col_counts, axis=1, keepdims=True)
    return to_table([starts, col_starts, col_counts, from_src, extra, short, own])


def take_segments(cap, relay, table_ref, all_ref, out_ref, slot_ref):
    group_size, tiles, _ = all_ref.shape
    lane = lax.broadcasted_iota(jnp.int32, (1, LANES), 1)
    short = table_ref[SHORT, 0] > 0
    past = lane - cap
    relayed = group_size * cap + lax.rem(past, group_size) * relay + past // group_size
    unused = jnp.where(short, group_size * (cap + relay), group_size * LANES)
    for i in range(group_size):
        s = jnp.clip(table_ref[COL_STARTS, i], 0, tiles * LANES - 1)
        t = s // LANES
        off = s - t * LANES
        a = all_ref[i, pl.ds(t, 1), :]
        b = all_ref[i, pl.ds(jnp.minimum(t + 1, tiles - 1), 1), :]
        shift = lax.rem(LANES - off, LANES)
        a = pltpu.roll(a, shift, 1)
        b = pltpu.roll(b, shift, 1)
        v = jnp.where(lane < LANES - off, a, b)
        live = lane < table_ref[COL_COUNTS, i]
        out_ref[pl.ds(i, 1), :] = jnp.where(live, v, PAD_KEY)
        slot = jnp.where(short, jnp.where(past < 0, i * cap + lane, relayed), i * LANES + lane)
        slot_ref[pl.ds(i, 1), :] = jnp.where(live, slot, unused)


def sort_exchange_kernel(
    group_size, cap, relay, block,
    keys_ref, rows_ref,
    out_ref, merged_ref, idx_ref, order_ref, split_ref, table_ref, own_ref, short_ref,
    fetched, held, outgoing, first, arrived, second, mine, all_ref, my_samples, samples, start_ref, splitters, edge_ref, seg_ref, slot_ref, order, starts, table,
    in_sem, own_sem, send_sem, recv_sem,
):
    me = lax.axis_index("g")
    core, x, y = lax.rem(me, CORES), lax.rem(me // CORES, SIDE), me // (CORES * SIDE)
    n, width = rows_ref.shape
    tiles = width // LANES

    def peer(d):
        return lax.rem(me + d, group_size)

    barrier = pltpu.get_barrier_semaphore()
    for d in range(1, group_size):
        pl.semaphore_signal(barrier, inc=1, device_id={"g": peer(d)}, device_id_type=MESH)

    def fetch(s):
        return pltpu.make_async_copy(rows_ref.at[pl.ds(s * block, block)], fetched.at[s], in_sem.at[s])

    def split(s):
        fetch(s).wait()

        def body(g, carry):
            r = pl.multiple_of(g * 16, 16)
            v = fetched[s, pl.ds(r, 16), :].reshape(16, tiles, LANES)
            for q in range(tiles // SUB):
                held[pl.ds(s * block + r, 16), q] = v[:, SUB * q : SUB * (q + 1)]
            return carry

        lax.fori_loop(0, block // 16, body, 0)

    for s in range(n // block):
        fetch(s).start()
    shape = keys_ref.shape
    places = lax.broadcasted_iota(jnp.int32, shape, 0) * LANES + lax.broadcasted_iota(jnp.int32, shape, 1)
    sorted_keys, sorted_places = bitonic_sort(keys_ref[...], places)
    mine[...] = sorted_keys
    order_ref[...] = sorted_places
    all_ref[pl.ds(me, 1)] = sorted_keys[None]
    my_samples[...] = sample_row(sorted_keys, group_size)
    samples[pl.ds(me, 1)] = my_samples[...][None]
    split(0)
    pl.semaphore_wait(barrier, group_size - 1)

    def remote(d, dst, src_ref, dst_ref, kind):
        return pltpu.make_async_remote_copy(
            src_ref=src_ref, dst_ref=dst_ref, send_sem=send_sem.at[kind, d], recv_sem=recv_sem.at[kind, d], device_id={"g": dst}, device_id_type=MESH
        )

    def share(d):
        return remote(d, peer(d), mine, all_ref.at[me], 3)

    def share_samples(d):
        return remote(d, peer(d), my_samples, samples.at[me], 4)

    def hop_one(d):
        return remote(d, peer(d), first.at[peer(d)], arrived.at[me], 1)

    def hop_two(d):
        return remote(d, peer(d), second.at[peer(d)], out_ref.at[pl.ds(group_size * cap + me * relay, relay)], 2)

    def far(s):
        dx, dy, dc = STEPS[s]
        return (lax.rem(y + dy, SIDE) * SIDE + lax.rem(x + dx, SIDE)) * CORES + lax.rem(core + dc, CORES)

    def base(s):
        return remote(s, far(s), outgoing.at[far(s)], out_ref.at[pl.ds(me * cap, cap)], 0)

    def each(act):
        def body(d, carry):
            act(d)
            return carry

        lax.fori_loop(1, group_size, body, 0)

    each(lambda d: share_samples(d).start())
    each(lambda d: share(d).start())
    to_order = pltpu.make_async_copy(order_ref, order, own_sem.at[2])
    to_order.start()
    for s in range(1, n // block):
        split(s)
    each(lambda d: share_samples(d).wait())
    for i in range(group_size):
        edge_ref[i : i + 1] = samples[i]
    splitters[...] = pick_splitters(edge_ref[...])
    start_ref[...] = to_table([to_row(count_below(mine[...], splitters[...]), edge_ref.shape)])
    to_starts = pltpu.make_async_copy(start_ref, starts, own_sem.at[3])
    to_starts.start()
    to_order.wait()
    to_starts.wait()

    last = n - 1

    def row(k):
        k = k & last
        return held[order[k >> 7, k & (LANES - 1)] & last]

    def gather(dst):
        begin = starts[STARTS, dst]

        def body(b, carry):
            for u in range(13):
                k = b * 13 + u
                outgoing[dst, k] = row(begin + k)
            return carry

        lax.fori_loop(0, cap // 13, body, 0)

    own_two = pltpu.make_async_copy(second.at[me], out_ref.at[pl.ds(group_size * cap + me * relay, relay)], own_sem.at[1])
    own_base = pltpu.make_async_copy(outgoing.at[me], out_ref.at[pl.ds(me * cap, cap)], own_sem.at[0])

    def send(begin, end):
        for s in range(begin, end):
            gather(far(s))
            if s > begin:
                base(s - 1).start()
        return end - 1

    waiting = send(0, FIRST)
    gather(me)
    base(waiting).start()
    each(lambda d: share(d).wait())
    table_ref[...] = make_plan(me, cap, relay * group_size, all_ref, splitters, edge_ref)
    to_smem = pltpu.make_async_copy(table_ref, table, own_sem.at[5])
    to_smem.start()
    own_base.start()
    to_smem.wait()
    extra = table[EXTRA, 0]

    def gather_extra(b, carry):
        for u in range(8):
            m = b * 8 + u
            for r in range(relay):
                first[m, r] = row(extra + r * group_size + m)
        return carry

    lax.fori_loop(0, group_size // 8, gather_extra, 0)
    arrived[pl.ds(me, 1)] = first[pl.ds(me, 1)]
    gather(far(FIRST))
    each(lambda d: hop_one(d).start())
    base(FIRST).start()
    waiting = send(FIRST + 1, SECOND)
    own_ref[0] = table[OWN, 0]
    short_ref[0] = table[SHORT, 0]
    take_segments(cap, relay, table, all_ref, seg_ref, slot_ref)
    base(waiting).start()
    merged_ref[...], idx_ref[...] = bitonic_sort(seg_ref[...], slot_ref[...])
    each(lambda d: hop_one(d).wait())
    for j in range(group_size):
        second[j] = arrived[table[FROM_SRC, j] & (group_size - 1)]
    gather(far(SECOND))
    each(lambda d: hop_two(d).start())
    own_two.start()
    base(SECOND).start()
    waiting = send(SECOND + 1, group_size - 1)
    keep = pltpu.make_async_copy(held, split_ref, own_sem.at[4])
    keep.start()
    base(waiting).start()
    for s in range(group_size - 1):
        base(s).wait()
    each(lambda d: hop_two(d).wait())
    own_two.wait()
    own_base.wait()
    keep.wait()


def sort_exchange(keys, rows, cap, relay, group_size):
    n, width = rows.shape
    block = 512
    row = (width // (SUB * LANES), SUB, LANES)
    segs = (group_size, LANES)
    sems = pltpu.SemaphoreType.DMA
    return pl.pallas_call(
        functools.partial(sort_exchange_kernel, group_size, cap, relay, block),
        out_shape=[
            jax.ShapeDtypeStruct((group_size * (cap + relay), *row), rows.dtype),
            jax.ShapeDtypeStruct(segs, keys.dtype),
            jax.ShapeDtypeStruct(segs, jnp.int32),
            jax.ShapeDtypeStruct(keys.shape, jnp.int32),
            jax.ShapeDtypeStruct((n, *row), rows.dtype),
            jax.ShapeDtypeStruct((8, LANES), jnp.int32),
            jax.ShapeDtypeStruct((1,), jnp.int32),
            jax.ShapeDtypeStruct((1,), jnp.int32),
        ],
        in_specs=[VMEM, ANY],
        out_specs=[ANY, VMEM, VMEM, VMEM, ANY, VMEM, SMEM, SMEM],
        scratch_shapes=[
            pltpu.VMEM((n // block, block, width), rows.dtype),
            pltpu.VMEM((n, *row), rows.dtype),
            pltpu.VMEM((group_size, cap, *row), rows.dtype),
            pltpu.VMEM((group_size, relay, *row), rows.dtype),
            pltpu.VMEM((group_size, relay, *row), rows.dtype),
            pltpu.VMEM((group_size, relay, *row), rows.dtype),
            pltpu.VMEM(keys.shape, keys.dtype),
            pltpu.VMEM((group_size, *keys.shape), keys.dtype),
            pltpu.VMEM((1, LANES), keys.dtype),
            pltpu.VMEM((group_size, 1, LANES), keys.dtype),
            pltpu.VMEM((8, LANES), jnp.int32),
            pltpu.VMEM(segs, keys.dtype),
            pltpu.VMEM(segs, jnp.float32),
            pltpu.VMEM(segs, keys.dtype),
            pltpu.VMEM(segs, jnp.int32),
            pltpu.SMEM(keys.shape, jnp.int32),
            pltpu.SMEM((8, LANES), jnp.int32),
            pltpu.SMEM((8, LANES), jnp.int32),
            sems((n // block,)),
            sems((6,)),
            sems((5, group_size)),
            sems((5, group_size)),
        ],
        compiler_params=pltpu.CompilerParams(collective_id=0, has_side_effects=True),
        name="sort_exchange",
    )(keys, rows)


def pick_kernel(cap, group_size, order_ref, table_ref, rows_ref, out_ref):
    last = rows_ref.shape[0] - 1

    def per_dst(j, carry):
        first = table_ref[STARTS, j]

        def body(b, c):
            for u in range(8):
                k = b * 8 + u
                out_ref[j, k] = rows_ref[order_ref[jnp.minimum(first + k, last)]]
            return c

        return lax.fori_loop(0, cap // 8, body, carry)

    lax.fori_loop(0, group_size, per_dst, 0)


def pick(order, table, rows, cap, group_size):
    return pl.pallas_call(
        functools.partial(pick_kernel, cap, group_size),
        out_shape=jax.ShapeDtypeStruct((group_size, cap, *rows.shape[1:]), rows.dtype),
        in_specs=[SMEM, SMEM, VMEM],
        out_specs=VMEM,
        name="pick_rows",
    )(order, table, rows)


def place_kernel(idx_ref, count_ref, in_ref, keys_ref, out_ref, out_keys_ref, held, staged, blank, in_sem, out_sem, blank_sem):
    slots, block, width = staged.shape
    total = in_ref.shape[0]
    parts = held.shape[1]
    load = pltpu.make_async_copy(in_ref, held.at[pl.ds(0, total)], in_sem)
    load.start()
    out_keys_ref[...] = keys_ref[...]
    blank[...] = jnp.zeros(blank.shape, blank.dtype)
    held[total] = jnp.zeros(held.shape[1:], held.dtype)
    steps = out_ref.shape[0] // block
    live = pl.cdiv(count_ref[0], block)

    def clear(s):
        return pltpu.make_async_copy(blank, out_ref.at[pl.ds(s * block, block)], blank_sem)

    def store(s):
        slot = lax.rem(s, slots)
        return pltpu.make_async_copy(staged.at[slot], out_ref.at[pl.ds(s * block, block)], out_sem.at[slot])

    load.wait()

    def start_clear(s, carry):
        clear(s).start()
        return carry

    lax.fori_loop(live, steps, start_clear, 0)

    def step(s, carry):
        @pl.when(s >= slots)
        def _():
            store(s - slots).wait()

        slot = lax.rem(s, slots)

        def body(g, c):
            r = pl.multiple_of(g * 16, 16)
            rows = []
            for u in range(16):
                k = idx_ref[s * block + r + u]
                rows.append(jnp.concatenate([held[k, q] for q in range(parts)], 0))
            staged[slot, pl.ds(r, 16), :] = jnp.stack(rows, 0).reshape(16, width)
            return c

        lax.fori_loop(0, block // 16, body, 0)
        store(s).start()
        return carry

    lax.fori_loop(0, live, step, 0)

    def end_store(s, carry):
        store(s).wait()
        return carry

    lax.fori_loop(jnp.maximum(live - slots, 0), live, end_store, 0)

    def end_clear(s, carry):
        clear(s).wait()
        return carry

    lax.fori_loop(live, steps, end_clear, 0)


def place(idx, count, rows, keys, width):
    n_out = idx.shape[0]
    block, slots = 128, 4
    return pl.pallas_call(
        place_kernel,
        out_shape=[jax.ShapeDtypeStruct((n_out, width), rows.dtype), jax.ShapeDtypeStruct(keys.shape, keys.dtype)],
        in_specs=[SMEM, SMEM, ANY, VMEM],
        out_specs=[ANY, VMEM],
        scratch_shapes=[
            pltpu.VMEM((rows.shape[0] + 1, *rows.shape[1:]), rows.dtype),
            pltpu.VMEM((slots, block, width), rows.dtype),
            pltpu.VMEM((block, width), rows.dtype),
            pltpu.SemaphoreType.DMA,
            pltpu.SemaphoreType.DMA((slots,)),
            pltpu.SemaphoreType.DMA,
        ],
        name="place_rows",
    )(idx, count, rows, keys)


def solution(mesh):
    group_size = mesh.shape["g"]

    def local_part(keys_loc, rows_loc):
        n_dev = keys_loc.shape[0]
        width = rows_loc.shape[1]
        cap_rows = 2 * n_dev // group_size
        blocks, merged, idx, order, rows, table, own_count, short = sort_exchange(keys_loc.reshape(n_dev // LANES, LANES), rows_loc, BASE, RELAY, group_size)
        idx = idx.reshape(-1)

        def arrived():
            return place(idx, own_count, blocks, merged, width)

        def direct():
            wide = lax.all_to_all(pick(order.reshape(-1), table, rows, cap_rows, group_size), "g", 0, 0, tiled=True)
            return place(idx, own_count, wide.reshape(-1, *wide.shape[2:]), merged, width)

        out_rows, out_keys = lax.cond(short[0] > 0, arrived, direct)
        return out_keys.reshape(-1), out_rows, own_count

    row_spec = P(("batch", "g"))
    mat_spec = P(("batch", "g"), None)
    return jax.shard_map(local_part, mesh=mesh, in_specs=(row_spec, mat_spec), out_specs=(row_spec, mat_spec, row_spec), check_vma=False)
```

```python
import functools

import jax
import jax.numpy as jnp
from jax import lax
from jax.experimental import pallas as pl
from jax.experimental.pallas import tpu as pltpu
from jax.sharding import PartitionSpec as P

PAD_KEY = 128.0
LANES = 128
SUB = 4
BASE = 65
RELAY = 2
FIRST, SECOND, THIRD = 6, 12, 22
SIDE = 4
CORES = 2
SLOTS = (((0, 2), (2, 0)), ((0, 1), (2, 3)), ((0, 3), (2, 1)), ((1, 0), (3, 2)), ((3, 0), (1, 2)), ((3, 1), (1, 3)), ((3, 3), (1, 1)), ((2, 2),))
STEPS = ((0, 0, 1), *((dx, dy, dc) for slot in SLOTS for dc in (1, 0) for dx, dy in slot))

VMEM = pl.BlockSpec(memory_space=pltpu.VMEM)
SMEM = pl.BlockSpec(memory_space=pltpu.SMEM)
ANY = pl.BlockSpec(memory_space=pl.ANY)
HBM = pl.BlockSpec(memory_space=pltpu.HBM)
MESH = pl.DeviceIdType.MESH
FROM_SRC, EXTRA, SHORT, OWN = range(4)


def bitonic_sort(keys, vals):
    rows, lanes = keys.shape
    pos = lax.broadcasted_iota(jnp.int32, keys.shape, 0) * lanes + lax.broadcasted_iota(jnp.int32, keys.shape, 1)

    def partner(x, j, low):
        axis, size, d = (1, lanes, j) if j < lanes else (0, rows, j // lanes)
        return jnp.where(low, pltpu.roll(x, size - d, axis), pltpu.roll(x, d, axis))

    k = 2
    while k <= rows * lanes:
        j = k // 2
        while j:
            low = (pos & j) == 0
            keep_min = jnp.logical_xor(low, (pos & k) != 0)
            other = partner(keys, j, low)
            swap = jnp.logical_or(jnp.logical_and(keep_min, keys > other), jnp.logical_and(jnp.logical_not(keep_min), keys < other))
            vals = jnp.where(swap, partner(vals, j, low), vals)
            keys = jnp.where(swap, other, keys)
            j //= 2
        k *= 2
    return keys, vals


def sample_row(keys, group_size):
    rows, lanes = keys.shape
    per = rows * lanes // group_size
    each = lanes // per
    lane = lax.broadcasted_iota(jnp.int32, keys.shape, 1)
    sub = lax.broadcasted_iota(jnp.int32, keys.shape, 0)
    acc = jnp.zeros(keys.shape, keys.dtype)
    for l in range(each):
        acc = jnp.where(lane == each * sub + l, keys[:, l * per : l * per + 1], acc)
    return jnp.sum(acc, axis=0, keepdims=True)


def pick_splitters(samples):
    group_size = samples.shape[0]
    lane = lax.broadcasted_iota(jnp.int32, samples.shape, 1)
    sub = lax.broadcasted_iota(jnp.int32, samples.shape, 0)
    fit = LANES // group_size
    merged = samples
    for f in range(1, fit):
        merged = jnp.where(lax.rem(sub, fit) == f, pltpu.roll(samples, f * group_size, 1), merged)
    packed = [jnp.sum(merged[c * fit : (c + 1) * fit], axis=0, keepdims=True) for c in range(group_size // fit)]
    less = [jnp.zeros(samples.shape, jnp.float32) for _ in packed]
    for q in range(group_size):
        a = jnp.broadcast_to(samples[:, q : q + 1], samples.shape)
        less = [n + (a < b).astype(jnp.float32) for n, b in zip(less, packed)]
    target = (sub * group_size + group_size // 2).astype(jnp.float32)
    found = jnp.zeros(samples.shape, jnp.float32)
    for n, b in zip(less, packed):
        found += jnp.where(jnp.sum(n, axis=0, keepdims=True) == target, b, 0.0)
    return jnp.where(sub == 0, -PAD_KEY, jnp.sum(found, axis=1, keepdims=True))


def count_below(keys, splitters):
    less = jnp.zeros(splitters.shape, jnp.float32)
    for r in range(keys.shape[0]):
        less += (keys[r : r + 1] < splitters).astype(jnp.float32)
    return jnp.sum(less, axis=1, keepdims=True)


def to_row(column, shape):
    lane = lax.broadcasted_iota(jnp.int32, shape, 1)
    sub = lax.broadcasted_iota(jnp.int32, shape, 0)
    return jnp.sum(jnp.where(lane == sub, column, 0.0), axis=0, keepdims=True)


def to_table(rows):
    rows = rows + [rows[-1]] * (8 - len(rows))
    return jnp.concatenate([jnp.broadcast_to(r, (1, LANES)) for r in rows], 0).astype(jnp.int32)


def make_plan(me, cap, relay, n_dev, edges):
    group_size = edges.shape[0]
    lane = lax.broadcasted_iota(jnp.int32, edges.shape, 1)
    sub = lax.broadcasted_iota(jnp.int32, edges.shape, 0)
    after = jnp.where(lane == group_size - 1, float(n_dev), pltpu.roll(edges, LANES - 1, 1))
    counts = jnp.where(lane < group_size, after - edges, 0.0)
    over = jnp.maximum(counts - cap, 0.0)
    has = (over > 0).astype(jnp.float32)
    worst = jnp.maximum(jnp.max(jnp.sum(has, axis=0, keepdims=True), axis=1, keepdims=True), jnp.max(jnp.sum(has, axis=1, keepdims=True), axis=0, keepdims=True))
    most_over = jnp.max(jnp.max(over, axis=0, keepdims=True), axis=1, keepdims=True)
    short = ((worst <= 1) & (most_over <= relay * group_size)).astype(jnp.float32)
    my_counts = jnp.sum(jnp.where(lane == me, counts, 0.0), axis=1, keepdims=True)
    own = jnp.sum(my_counts, axis=0, keepdims=True)
    from_src = jnp.sum(has * sub.astype(jnp.float32), axis=0, keepdims=True)
    extra = jnp.sum(jnp.sum(jnp.where(sub == me, has * (edges + cap), 0.0), axis=0, keepdims=True), axis=1, keepdims=True)
    past = lane - cap
    slot = jnp.where(past < 0, sub * cap + lane, group_size * cap + lax.rem(past, group_size) * relay + past // group_size)
    slot = jnp.where(lane.astype(jnp.float32) < my_counts, slot, 0)
    return to_table([from_src, extra, short, own]), slot


def write_messages(start_ref, mine, msg_ref, edges):
    group_size = msg_ref.shape[0]
    tiles = mine.shape[0]
    n_dev = tiles * LANES
    lane = lax.broadcasted_iota(jnp.int32, (1, LANES), 1)

    def one(j):
        s = start_ref[0, j] & (2 * n_dev - 1)
        stop = jnp.where(j == group_size - 1, n_dev, start_ref[0, j + 1])
        t = s // LANES
        off = s & (LANES - 1)
        a = mine[pl.ds(jnp.minimum(t, tiles - 1), 1), :]
        b = mine[pl.ds(jnp.minimum(t + 1, tiles - 1), 1), :]
        shift = (LANES - off) & (LANES - 1)
        v = jnp.where(lane < LANES - off, pltpu.roll(a, shift, 1), pltpu.roll(b, shift, 1))
        msg_ref[j, 0:1] = jnp.where(lane < stop - s, v, PAD_KEY)
        msg_ref[j, 1:2] = edges

    def body(b, carry):
        for u in range(4):
            one(b * 4 + u)
        return carry

    lax.fori_loop(0, group_size // 4, body, 0)


def sort_exchange_kernel(
    group_size, cap, relay, block,
    keys_ref, rows_ref,
    out_ref, merged_ref, idx_ref, order_ref, split_ref, start_ref, seg_ref, own_ref, short_ref,
    fetched, held, outgoing, first, arrived, second, mine, my_samples, samples, msgs, inbox, edge_ref, edge_row, table_ref, order, starts, table,
    in_sem, own_sem, send_sem, recv_sem,
):
    me = lax.axis_index("g")
    core, x, y = lax.rem(me, CORES), lax.rem(me // CORES, SIDE), me // (CORES * SIDE)
    n, width = rows_ref.shape
    tiles = width // LANES

    def peer(d):
        return lax.rem(me + d, group_size)

    barrier = pltpu.get_barrier_semaphore()
    for d in range(1, group_size):
        pl.semaphore_signal(barrier, inc=1, device_id={"g": peer(d)}, device_id_type=MESH)

    def fetch(s):
        return pltpu.make_async_copy(rows_ref.at[pl.ds(s * block, block)], fetched.at[s], in_sem.at[s])

    def split(s):
        fetch(s).wait()

        def body(g, carry):
            r = pl.multiple_of(g * 16, 16)
            v = fetched[s, pl.ds(r, 16), :].reshape(16, tiles, LANES)
            for q in range(tiles // SUB):
                held[pl.ds(s * block + r, 16), q] = v[:, SUB * q : SUB * (q + 1)]
            return carry

        lax.fori_loop(0, block // 16, body, 0)

    for s in range(n // block):
        fetch(s).start()
    shape = keys_ref.shape
    places = lax.broadcasted_iota(jnp.int32, shape, 0) * LANES + lax.broadcasted_iota(jnp.int32, shape, 1)
    sorted_keys, sorted_places = bitonic_sort(keys_ref[...], places)
    mine[...] = sorted_keys
    order_ref[...] = sorted_places
    my_samples[...] = sample_row(sorted_keys, group_size)
    samples[pl.ds(me, 1)] = my_samples[...][None]
    split(0)
    pl.semaphore_wait(barrier, group_size - 1)

    def remote(d, dst, src_ref, dst_ref, kind):
        return pltpu.make_async_remote_copy(
            src_ref=src_ref, dst_ref=dst_ref, send_sem=send_sem.at[kind, d], recv_sem=recv_sem.at[kind, d], device_id={"g": dst}, device_id_type=MESH
        )

    def share(d):
        return remote(d, peer(d), msgs.at[peer(d)], inbox.at[me], 3)

    def share_samples(d):
        return remote(d, peer(d), my_samples, samples.at[me], 4)

    def hop_one(d):
        return remote(d, peer(d), first.at[peer(d)], arrived.at[me], 1)

    def hop_two(d):
        return remote(d, peer(d), second.at[peer(d)], out_ref.at[pl.ds(group_size * cap + me * relay, relay)], 2)

    def far(s):
        dx, dy, dc = STEPS[s]
        return (lax.rem(y + dy, SIDE) * SIDE + lax.rem(x + dx, SIDE)) * CORES + lax.rem(core + dc, CORES)

    def base(s):
        return remote(s, far(s), outgoing.at[far(s)], out_ref.at[pl.ds(me * cap, cap)], 0)

    def each(act):
        def body(d, carry):
            act(d)
            return carry

        lax.fori_loop(1, group_size, body, 0)

    each(lambda d: share_samples(d).start())
    to_order = pltpu.make_async_copy(order_ref, order, own_sem.at[2])
    to_order.start()
    for s in range(1, n // block):
        split(s)
    each(lambda d: share_samples(d).wait())
    for i in range(group_size):
        edge_ref[i : i + 1] = samples[i]
    edges = to_row(count_below(mine[...], pick_splitters(edge_ref[...])), edge_ref.shape)
    edge_row[...] = edges
    start_ref[...] = to_table([edges])
    to_starts = pltpu.make_async_copy(start_ref, starts, own_sem.at[3])
    to_starts.start()
    to_order.wait()
    to_starts.wait()

    last = n - 1

    def row(k):
        k = k & last
        return held[order[k >> 7, k & (LANES - 1)] & last]

    def gather(dst):
        begin = starts[0, dst]

        def body(b, carry):
            for u in range(13):
                k = b * 13 + u
                outgoing[dst, k] = row(begin + k)
            return carry

        lax.fori_loop(0, cap // 13, body, 0)

    own_two = pltpu.make_async_copy(second.at[me], out_ref.at[pl.ds(group_size * cap + me * relay, relay)], own_sem.at[1])
    own_base = pltpu.make_async_copy(outgoing.at[me], out_ref.at[pl.ds(me * cap, cap)], own_sem.at[0])

    def send(begin, end):
        for s in range(begin, end):
            gather(far(s))
            if s > begin:
                base(s - 1).start()
        return end - 1

    waiting = send(0, FIRST)
    write_messages(starts, mine, msgs, edge_row[...])
    base(waiting).start()
    inbox[pl.ds(me, 1)] = msgs[pl.ds(me, 1)]
    gather(far(FIRST))
    each(lambda d: share(d).start())
    base(FIRST).start()
    waiting = send(FIRST + 1, SECOND)
    gather(me)
    base(waiting).start()
    each(lambda d: share(d).wait())
    for i in range(group_size):
        seg_ref[i : i + 1] = inbox[i, 0:1]
        edge_ref[i : i + 1] = inbox[i, 1:2]
    table_ref[...], slots = make_plan(me, cap, relay, n, edge_ref[...])
    to_smem = pltpu.make_async_copy(table_ref, table, own_sem.at[5])
    to_smem.start()
    own_base.start()
    to_smem.wait()
    extra = table[EXTRA, 0]

    def gather_extra(b, carry):
        for u in range(8):
            m = b * 8 + u
            for r in range(relay):
                first[m, r] = row(extra + r * group_size + m)
        return carry

    lax.fori_loop(0, group_size // 8, gather_extra, 0)
    arrived[pl.ds(me, 1)] = first[pl.ds(me, 1)]
    gather(far(SECOND))
    each(lambda d: hop_one(d).start())
    base(SECOND).start()
    waiting = send(SECOND + 1, THIRD)
    own_ref[0] = table[OWN, 0]
    short_ref[0] = table[SHORT, 0]
    base(waiting).start()
    merged_ref[...], idx_ref[...] = bitonic_sort(seg_ref[...], slots)
    each(lambda d: hop_one(d).wait())
    for j in range(group_size):
        second[j] = arrived[table[FROM_SRC, j] & (group_size - 1)]
    gather(far(THIRD))
    each(lambda d: hop_two(d).start())
    own_two.start()
    base(THIRD).start()
    waiting = send(THIRD + 1, group_size - 1)
    keep = pltpu.make_async_copy(held, split_ref, own_sem.at[4])
    keep.start()
    base(waiting).start()
    for s in range(group_size - 1):
        base(s).wait()
    each(lambda d: hop_two(d).wait())
    own_two.wait()
    own_base.wait()
    keep.wait()


def sort_exchange(keys, rows, cap, relay, group_size):
    n, width = rows.shape
    block = 512
    row = (width // (SUB * LANES), SUB, LANES)
    segs = (group_size, LANES)
    sems = pltpu.SemaphoreType.DMA
    return pl.pallas_call(
        functools.partial(sort_exchange_kernel, group_size, cap, relay, block),
        out_shape=[
            pltpu.VMEM((group_size * (cap + relay), *row), rows.dtype),
            jax.ShapeDtypeStruct(segs, keys.dtype),
            pltpu.VMEM(segs, jnp.int32),
            jax.ShapeDtypeStruct(keys.shape, jnp.int32),
            jax.ShapeDtypeStruct((n, *row), rows.dtype),
            jax.ShapeDtypeStruct((8, LANES), jnp.int32),
            jax.ShapeDtypeStruct(segs, keys.dtype),
            jax.ShapeDtypeStruct((1,), jnp.int32),
            jax.ShapeDtypeStruct((1,), jnp.int32),
        ],
        in_specs=[VMEM, HBM],
        out_specs=[VMEM, VMEM, VMEM, VMEM, HBM, VMEM, VMEM, SMEM, SMEM],
        scratch_shapes=[
            pltpu.VMEM((n // block, block, width), rows.dtype),
            pltpu.VMEM((n, *row), rows.dtype),
            pltpu.VMEM((group_size, cap, *row), rows.dtype),
            pltpu.VMEM((group_size, relay, *row), rows.dtype),
            pltpu.VMEM((group_size, relay, *row), rows.dtype),
            pltpu.VMEM((group_size, relay, *row), rows.dtype),
            pltpu.VMEM(keys.shape, keys.dtype),
            pltpu.VMEM((1, LANES), keys.dtype),
            pltpu.VMEM((group_size, 1, LANES), keys.dtype),
            pltpu.VMEM((group_size, 2, LANES), keys.dtype),
            pltpu.VMEM((group_size, 2, LANES), keys.dtype),
            pltpu.VMEM(segs, jnp.float32),
            pltpu.VMEM((1, LANES), jnp.float32),
            pltpu.VMEM((8, LANES), jnp.int32),
            pltpu.SMEM(keys.shape, jnp.int32),
            pltpu.SMEM((8, LANES), jnp.int32),
            pltpu.SMEM((8, LANES), jnp.int32),
            sems((n // block,)),
            sems((6,)),
            sems((5, group_size)),
            sems((5, group_size)),
        ],
        compiler_params=pltpu.CompilerParams(collective_id=0, has_side_effects=True, vmem_limit_bytes=52 * 1024 * 1024),
        name="sort_exchange",
    )(keys, rows)


def pick_kernel(cap, group_size, order_ref, table_ref, rows_ref, out_ref):
    last = rows_ref.shape[0] - 1

    def per_dst(j, carry):
        first = table_ref[0, j]

        def body(b, c):
            for u in range(8):
                k = b * 8 + u
                out_ref[j, k] = rows_ref[order_ref[jnp.minimum(first + k, last)]]
            return c

        return lax.fori_loop(0, cap // 8, body, carry)

    lax.fori_loop(0, group_size, per_dst, 0)


def pick(order, table, rows, cap, group_size):
    return pl.pallas_call(
        functools.partial(pick_kernel, cap, group_size),
        out_shape=jax.ShapeDtypeStruct((group_size, cap, *rows.shape[1:]), rows.dtype),
        in_specs=[SMEM, SMEM, VMEM],
        out_specs=VMEM,
        name="pick_rows",
    )(order, table, rows)


def place_kernel(idx_ref, count_ref, held, keys_ref, out_ref, out_keys_ref, staged, blank, out_sem, blank_sem):
    slots, block, width = staged.shape
    parts = held.shape[1]
    out_keys_ref[...] = keys_ref[...]
    blank[...] = jnp.zeros(blank.shape, blank.dtype)
    steps = out_ref.shape[0] // block
    count = count_ref[0]
    live = pl.cdiv(count, block)

    def clear(s):
        return pltpu.make_async_copy(blank, out_ref.at[pl.ds(s * block, block)], blank_sem)

    def store(s):
        slot = lax.rem(s, slots)
        return pltpu.make_async_copy(staged.at[slot], out_ref.at[pl.ds(s * block, block)], out_sem.at[slot])

    def start_clear(s, carry):
        clear(s).start()
        return carry

    def step(s, carry):
        @pl.when(s >= slots)
        def _():
            store(s - slots).wait()

        slot = lax.rem(s, slots)

        def body(g, c):
            r = pl.multiple_of(g * 16, 16)
            rows = []
            for u in range(16):
                k = idx_ref[s * block + r + u]
                rows.append(jnp.concatenate([held[k, q] for q in range(parts)], 0))
            staged[slot, pl.ds(r, 16), :] = jnp.stack(rows, 0).reshape(16, width)
            return c

        lax.fori_loop(0, block // 16, body, 0)

        @pl.when((s + 1) * block > count)
        def _():
            row = lax.broadcasted_iota(jnp.int32, (block, width), 0) + s * block
            staged[slot] = jnp.where(row < count, staged[slot], jnp.zeros((block, width), staged.dtype))

        store(s).start()
        return carry

    lax.fori_loop(0, jnp.minimum(live, 1), step, 0)
    lax.fori_loop(live, steps, start_clear, 0)
    lax.fori_loop(1, live, step, 0)

    def end_store(s, carry):
        store(s).wait()
        return carry

    lax.fori_loop(jnp.maximum(live - slots, 0), live, end_store, 0)

    def end_clear(s, carry):
        clear(s).wait()
        return carry

    lax.fori_loop(live, steps, end_clear, 0)


def place(idx, count, rows, keys, width):
    n_out = idx.shape[0]
    block, slots = 128, 4
    return pl.pallas_call(
        place_kernel,
        out_shape=[jax.ShapeDtypeStruct((n_out, width), rows.dtype), jax.ShapeDtypeStruct(keys.shape, keys.dtype)],
        in_specs=[SMEM, SMEM, VMEM, VMEM],
        out_specs=[ANY, VMEM],
        scratch_shapes=[
            pltpu.VMEM((slots, block, width), rows.dtype),
            pltpu.VMEM((block, width), rows.dtype),
            pltpu.SemaphoreType.DMA((slots,)),
            pltpu.SemaphoreType.DMA,
        ],
        compiler_params=pltpu.CompilerParams(vmem_limit_bytes=24 * 1024 * 1024),
        name="place_rows",
    )(idx, count, rows, keys)


def solution(mesh):
    group_size = mesh.shape["g"]

    def local_part(keys_loc, rows_loc):
        n_dev = keys_loc.shape[0]
        width = rows_loc.shape[1]
        cap_rows = 2 * n_dev // group_size
        blocks, merged, idx, order, rows, starts, segs, own_count, short = sort_exchange(keys_loc.reshape(n_dev // LANES, LANES), rows_loc, BASE, RELAY, group_size)
        out_rows, out_keys = place(idx.reshape(-1), own_count, blocks, merged, width)

        def general(carry):
            wide = lax.all_to_all(pick(order.reshape(-1), starts, rows, cap_rows, group_size), "g", 0, 0, tiled=True)
            _, at = lax.sort((segs.reshape(-1), lax.iota(jnp.int32, segs.size)), num_keys=1)
            return jnp.int32(1), place(at, own_count, wide.reshape(-1, *wide.shape[2:]), merged, width)[0]

        _, out_rows = lax.while_loop(lambda carry: carry[0] == 0, general, (short[0], out_rows))
        return out_keys.reshape(-1), out_rows, own_count

    row_spec = P(("batch", "g"))
    mat_spec = P(("batch", "g"), None)
    return jax.shard_map(local_part, mesh=mesh, in_specs=(row_spec, mat_spec), out_specs=(row_spec, mat_spec, row_spec), check_vma=False)
```

```python
import functools

import jax
import jax.numpy as jnp
from jax import lax
from jax.experimental import pallas as pl
from jax.experimental.pallas import tpu as pltpu
from jax.sharding import PartitionSpec as P

PAD_KEY = 128.0
LANES = 128
SUB = 4
BASE = 65
RELAY = 2
FIRST, LATE = 12, 27
SIDE = 4
CORES = 2
SLOTS = (((0, 2), (2, 0)), ((0, 1), (2, 3)), ((0, 3), (2, 1)), ((1, 0), (3, 2)), ((3, 0), (1, 2)), ((3, 1), (1, 3)), ((3, 3), (1, 1)), ((2, 2),))
STEPS = ((0, 0, 1), *((dx, dy, dc) for slot in SLOTS for dc in (1, 0) for dx, dy in slot))

VMEM = pl.BlockSpec(memory_space=pltpu.VMEM)
SMEM = pl.BlockSpec(memory_space=pltpu.SMEM)
ANY = pl.BlockSpec(memory_space=pl.ANY)
HBM = pl.BlockSpec(memory_space=pltpu.HBM)
MESH = pl.DeviceIdType.MESH
FROM_SRC, EXTRA, SHORT, OWN = range(4)


def bitonic_sort(keys, vals):
    rows, lanes = keys.shape
    pos = lax.broadcasted_iota(jnp.int32, keys.shape, 0) * lanes + lax.broadcasted_iota(jnp.int32, keys.shape, 1)

    def partner(x, j, low):
        axis, size, d = (1, lanes, j) if j < lanes else (0, rows, j // lanes)
        return jnp.where(low, pltpu.roll(x, size - d, axis), pltpu.roll(x, d, axis))

    k = 2
    while k <= rows * lanes:
        j = k // 2
        while j:
            low = (pos & j) == 0
            keep_min = jnp.logical_xor(low, (pos & k) != 0)
            other = partner(keys, j, low)
            swap = jnp.logical_or(jnp.logical_and(keep_min, keys > other), jnp.logical_and(jnp.logical_not(keep_min), keys < other))
            vals = jnp.where(swap, partner(vals, j, low), vals)
            keys = jnp.where(swap, other, keys)
            j //= 2
        k *= 2
    return keys, vals


def sample_row(keys, group_size):
    rows, lanes = keys.shape
    per = rows * lanes // group_size
    each = lanes // per
    lane = lax.broadcasted_iota(jnp.int32, keys.shape, 1)
    sub = lax.broadcasted_iota(jnp.int32, keys.shape, 0)
    acc = jnp.zeros(keys.shape, keys.dtype)
    for l in range(each):
        acc = jnp.where(lane == each * sub + l, keys[:, l * per : l * per + 1], acc)
    return jnp.sum(acc, axis=0, keepdims=True)


def pick_splitters(samples):
    group_size = samples.shape[0]
    lane = lax.broadcasted_iota(jnp.int32, samples.shape, 1)
    sub = lax.broadcasted_iota(jnp.int32, samples.shape, 0)
    fit = LANES // group_size
    merged = samples
    for f in range(1, fit):
        merged = jnp.where(lax.rem(sub, fit) == f, pltpu.roll(samples, f * group_size, 1), merged)
    packed = [jnp.sum(merged[c * fit : (c + 1) * fit], axis=0, keepdims=True) for c in range(group_size // fit)]
    less = [jnp.zeros(samples.shape, jnp.float32) for _ in packed]
    for q in range(group_size):
        a = jnp.broadcast_to(samples[:, q : q + 1], samples.shape)
        less = [n + (a < b).astype(jnp.float32) for n, b in zip(less, packed)]
    target = (sub * group_size + group_size // 2).astype(jnp.float32)
    found = jnp.zeros(samples.shape, jnp.float32)
    for n, b in zip(less, packed):
        found += jnp.where(jnp.sum(n, axis=0, keepdims=True) == target, b, 0.0)
    return jnp.where(sub == 0, -PAD_KEY, jnp.sum(found, axis=1, keepdims=True))


def count_below(keys, splitters):
    less = jnp.zeros(splitters.shape, jnp.float32)
    for r in range(keys.shape[0]):
        less += (keys[r : r + 1] < splitters).astype(jnp.float32)
    return jnp.sum(less, axis=1, keepdims=True)


def to_row(column, shape):
    lane = lax.broadcasted_iota(jnp.int32, shape, 1)
    sub = lax.broadcasted_iota(jnp.int32, shape, 0)
    return jnp.sum(jnp.where(lane == sub, column, 0.0), axis=0, keepdims=True)


def to_table(rows):
    rows = rows + [rows[-1]] * (8 - len(rows))
    return jnp.concatenate([jnp.broadcast_to(r, (1, LANES)) for r in rows], 0).astype(jnp.int32)


def make_plan(me, cap, relay, n_dev, edges):
    group_size = edges.shape[0]
    lane = lax.broadcasted_iota(jnp.int32, edges.shape, 1)
    sub = lax.broadcasted_iota(jnp.int32, edges.shape, 0)
    after = jnp.where(lane == group_size - 1, float(n_dev), pltpu.roll(edges, LANES - 1, 1))
    counts = jnp.where(lane < group_size, after - edges, 0.0)
    over = jnp.maximum(counts - cap, 0.0)
    has = (over > 0).astype(jnp.float32)
    worst = jnp.maximum(jnp.max(jnp.sum(has, axis=0, keepdims=True), axis=1, keepdims=True), jnp.max(jnp.sum(has, axis=1, keepdims=True), axis=0, keepdims=True))
    most_over = jnp.max(jnp.max(over, axis=0, keepdims=True), axis=1, keepdims=True)
    short = ((worst <= 1) & (most_over <= relay * group_size)).astype(jnp.float32)
    my_counts = jnp.sum(jnp.where(lane == me, counts, 0.0), axis=1, keepdims=True)
    own = jnp.sum(my_counts, axis=0, keepdims=True)
    from_src = jnp.sum(has * sub.astype(jnp.float32), axis=0, keepdims=True)
    extra = jnp.sum(jnp.sum(jnp.where(sub == me, has * (edges + cap), 0.0), axis=0, keepdims=True), axis=1, keepdims=True)
    past = lane - cap
    slot = jnp.where(past < 0, sub * cap + lane, group_size * cap + lax.rem(past, group_size) * relay + past // group_size)
    slot = jnp.where(lane.astype(jnp.float32) < my_counts, slot, 0)
    return to_table([from_src, extra, short, own]), slot


def write_segments(start_ref, mine, msg_ref):
    group_size = msg_ref.shape[0]
    tiles = mine.shape[0]
    n_dev = tiles * LANES
    lane = lax.broadcasted_iota(jnp.int32, (1, LANES), 1)

    def one(j):
        s = start_ref[0, j] & (2 * n_dev - 1)
        stop = jnp.where(j == group_size - 1, n_dev, start_ref[0, j + 1])
        t = s // LANES
        off = s & (LANES - 1)
        a = mine[pl.ds(jnp.minimum(t, tiles - 1), 1), :]
        b = mine[pl.ds(jnp.minimum(t + 1, tiles - 1), 1), :]
        shift = (LANES - off) & (LANES - 1)
        v = jnp.where(lane < LANES - off, pltpu.roll(a, shift, 1), pltpu.roll(b, shift, 1))
        msg_ref[j] = jnp.where(lane < stop - s, v, PAD_KEY)

    def body(b, carry):
        for u in range(4):
            one(b * 4 + u)
        return carry

    lax.fori_loop(0, group_size // 4, body, 0)


def sort_exchange_kernel(
    group_size, cap, relay, block,
    keys_ref, rows_ref,
    out_ref, merged_ref, idx_ref, order_ref, split_ref, start_ref, seg_ref, own_ref, short_ref,
    fetched, held, outgoing, first, arrived, second, mine, my_samples, samples, msgs, inbox, all_edges, edge_ref, edge_row, table_ref, slot_ref, order, starts, table,
    in_sem, own_sem, send_sem, recv_sem,
):
    me = lax.axis_index("g")
    core, x, y = lax.rem(me, CORES), lax.rem(me // CORES, SIDE), me // (CORES * SIDE)
    n, width = rows_ref.shape
    tiles = width // LANES

    def peer(d):
        return lax.rem(me + d, group_size)

    barrier = pltpu.get_barrier_semaphore()
    for d in range(1, group_size):
        pl.semaphore_signal(barrier, inc=1, device_id={"g": peer(d)}, device_id_type=MESH)

    def fetch(s):
        return pltpu.make_async_copy(rows_ref.at[pl.ds(s * block, block)], fetched.at[s], in_sem.at[s])

    def split(s):
        fetch(s).wait()

        def body(g, carry):
            r = pl.multiple_of(g * 16, 16)
            v = fetched[s, pl.ds(r, 16), :].reshape(16, tiles, LANES)
            for q in range(tiles // SUB):
                held[pl.ds(s * block + r, 16), q] = v[:, SUB * q : SUB * (q + 1)]
            return carry

        lax.fori_loop(0, block // 16, body, 0)

    for s in range(n // block):
        fetch(s).start()
    shape = keys_ref.shape
    places = lax.broadcasted_iota(jnp.int32, shape, 0) * LANES + lax.broadcasted_iota(jnp.int32, shape, 1)
    sorted_keys, sorted_places = bitonic_sort(keys_ref[...], places)
    mine[...] = sorted_keys
    order_ref[...] = sorted_places
    my_samples[...] = sample_row(sorted_keys, group_size)
    samples[pl.ds(me, 1)] = my_samples[...][None]
    split(0)
    pl.semaphore_wait(barrier, group_size - 1)

    def remote(d, dst, src_ref, dst_ref, kind):
        return pltpu.make_async_remote_copy(
            src_ref=src_ref, dst_ref=dst_ref, send_sem=send_sem.at[kind, d], recv_sem=recv_sem.at[kind, d], device_id={"g": dst}, device_id_type=MESH
        )

    def share(d):
        return remote(d, peer(d), msgs.at[peer(d)], inbox.at[me], 3)

    def share_edges(d):
        return remote(d, peer(d), edge_row, all_edges.at[me], 5)

    def share_samples(d):
        return remote(d, peer(d), my_samples, samples.at[me], 4)

    def hop_one(d):
        return remote(d, peer(d), first.at[peer(d)], arrived.at[me], 1)

    def hop_two(d):
        return remote(d, peer(d), second.at[peer(d)], out_ref.at[pl.ds(group_size * cap + me * relay, relay)], 2)

    def far(s):
        dx, dy, dc = STEPS[s]
        return (lax.rem(y + dy, SIDE) * SIDE + lax.rem(x + dx, SIDE)) * CORES + lax.rem(core + dc, CORES)

    def base(s):
        return remote(s, far(s), outgoing.at[far(s)], out_ref.at[pl.ds(me * cap, cap)], 0)

    def each(act):
        def body(d, carry):
            act(d)
            return carry

        lax.fori_loop(1, group_size, body, 0)

    each(lambda d: share_samples(d).start())
    to_order = pltpu.make_async_copy(order_ref, order, own_sem.at[2])
    to_order.start()
    for s in range(1, n // block):
        split(s)
    each(lambda d: share_samples(d).wait())
    for i in range(group_size):
        edge_ref[i : i + 1] = samples[i]
    edges = to_row(count_below(mine[...], pick_splitters(edge_ref[...])), edge_ref.shape)
    edge_row[...] = edges
    start_ref[...] = to_table([edges])
    to_starts = pltpu.make_async_copy(start_ref, starts, own_sem.at[3])
    all_edges[pl.ds(me, 1)] = edges[None]
    to_starts.start()
    to_order.wait()
    to_starts.wait()
    each(lambda d: share_edges(d).start())

    last = n - 1

    def row(k):
        k = k & last
        return held[order[k >> 7, k & (LANES - 1)] & last]

    def gather(dst):
        begin = starts[0, dst]

        def body(b, carry):
            for u in range(13):
                k = b * 13 + u
                outgoing[dst, k] = row(begin + k)
            return carry

        lax.fori_loop(0, cap // 13, body, 0)

    own_two = pltpu.make_async_copy(second.at[me], out_ref.at[pl.ds(group_size * cap + me * relay, relay)], own_sem.at[1])
    own_base = pltpu.make_async_copy(outgoing.at[me], out_ref.at[pl.ds(me * cap, cap)], own_sem.at[0])

    def send(begin, end):
        for s in range(begin, end):
            gather(far(s))
            if s > begin:
                base(s - 1).start()
        return end - 1

    waiting = send(0, FIRST)
    write_segments(starts, mine, msgs)
    base(waiting).start()
    inbox[pl.ds(me, 1)] = msgs[pl.ds(me, 1)]
    each(lambda d: share_edges(d).wait())
    for i in range(group_size):
        edge_ref[i : i + 1] = all_edges[i]
    table_ref[...], slots = make_plan(me, cap, relay, n, edge_ref[...])
    slot_ref[...] = slots
    to_smem = pltpu.make_async_copy(table_ref, table, own_sem.at[5])
    to_smem.start()
    gather(far(FIRST))
    base(FIRST).start()
    to_smem.wait()
    extra = table[EXTRA, 0]

    def gather_extra(b, carry):
        for u in range(8):
            m = b * 8 + u
            for r in range(relay):
                first[m, r] = row(extra + r * group_size + m)
        return carry

    lax.fori_loop(0, group_size // 8, gather_extra, 0)
    arrived[pl.ds(me, 1)] = first[pl.ds(me, 1)]
    gather(far(FIRST + 1))
    each(lambda d: hop_one(d).start())
    each(lambda d: share(d).start())
    base(FIRST + 1).start()
    waiting = send(FIRST + 2, LATE)
    gather(me)
    base(waiting).start()
    for s in range(LATE, group_size - 1):
        gather(far(s))
    own_base.start()
    own_ref[0] = table[OWN, 0]
    short_ref[0] = table[SHORT, 0]
    each(lambda d: share(d).wait())
    for i in range(group_size):
        seg_ref[i : i + 1] = inbox[i]
    each(lambda d: hop_one(d).wait())
    for j in range(group_size):
        second[j] = arrived[table[FROM_SRC, j] & (group_size - 1)]
    merged_ref[...], idx_ref[...] = bitonic_sort(seg_ref[...], slot_ref[...])
    each(lambda d: hop_two(d).start())
    own_two.start()
    for s in range(LATE, group_size - 1):
        base(s).start()
    keep = pltpu.make_async_copy(held, split_ref, own_sem.at[4])
    keep.start()
    for s in range(group_size - 1):
        base(s).wait()
    each(lambda d: hop_two(d).wait())
    own_two.wait()
    own_base.wait()
    keep.wait()


def sort_exchange(keys, rows, cap, relay, group_size):
    n, width = rows.shape
    block = 512
    row = (width // (SUB * LANES), SUB, LANES)
    segs = (group_size, LANES)
    sems = pltpu.SemaphoreType.DMA
    return pl.pallas_call(
        functools.partial(sort_exchange_kernel, group_size, cap, relay, block),
        out_shape=[
            pltpu.VMEM((group_size * (cap + relay), *row), rows.dtype),
            jax.ShapeDtypeStruct(segs, keys.dtype),
            pltpu.VMEM(segs, jnp.int32),
            jax.ShapeDtypeStruct(keys.shape, jnp.int32),
            jax.ShapeDtypeStruct((n, *row), rows.dtype),
            jax.ShapeDtypeStruct((8, LANES), jnp.int32),
            jax.ShapeDtypeStruct(segs, keys.dtype),
            jax.ShapeDtypeStruct((1,), jnp.int32),
            jax.ShapeDtypeStruct((1,), jnp.int32),
        ],
        in_specs=[VMEM, HBM],
        out_specs=[VMEM, VMEM, VMEM, VMEM, HBM, VMEM, VMEM, SMEM, SMEM],
        scratch_shapes=[
            pltpu.VMEM((n // block, block, width), rows.dtype),
            pltpu.VMEM((n, *row), rows.dtype),
            pltpu.VMEM((group_size, cap, *row), rows.dtype),
            pltpu.VMEM((group_size, relay, *row), rows.dtype),
            pltpu.VMEM((group_size, relay, *row), rows.dtype),
            pltpu.VMEM((group_size, relay, *row), rows.dtype),
            pltpu.VMEM(keys.shape, keys.dtype),
            pltpu.VMEM((1, LANES), keys.dtype),
            pltpu.VMEM((group_size, 1, LANES), keys.dtype),
            pltpu.VMEM((group_size, 1, LANES), keys.dtype),
            pltpu.VMEM((group_size, 1, LANES), keys.dtype),
            pltpu.VMEM((group_size, 1, LANES), jnp.float32),
            pltpu.VMEM(segs, jnp.float32),
            pltpu.VMEM((1, LANES), jnp.float32),
            pltpu.VMEM((8, LANES), jnp.int32),
            pltpu.VMEM(segs, jnp.int32),
            pltpu.SMEM(keys.shape, jnp.int32),
            pltpu.SMEM((8, LANES), jnp.int32),
            pltpu.SMEM((8, LANES), jnp.int32),
            sems((n // block,)),
            sems((6,)),
            sems((6, group_size)),
            sems((6, group_size)),
        ],
        compiler_params=pltpu.CompilerParams(collective_id=0, has_side_effects=True, vmem_limit_bytes=52 * 1024 * 1024),
        name="sort_exchange",
    )(keys, rows)


def pick_kernel(cap, group_size, order_ref, table_ref, rows_ref, out_ref):
    last = rows_ref.shape[0] - 1

    def per_dst(j, carry):
        first = table_ref[0, j]

        def body(b, c):
            for u in range(8):
                k = b * 8 + u
                out_ref[j, k] = rows_ref[order_ref[jnp.minimum(first + k, last)]]
            return c

        return lax.fori_loop(0, cap // 8, body, carry)

    lax.fori_loop(0, group_size, per_dst, 0)


def pick(order, table, rows, cap, group_size):
    return pl.pallas_call(
        functools.partial(pick_kernel, cap, group_size),
        out_shape=jax.ShapeDtypeStruct((group_size, cap, *rows.shape[1:]), rows.dtype),
        in_specs=[SMEM, SMEM, VMEM],
        out_specs=VMEM,
        name="pick_rows",
    )(order, table, rows)


def place_kernel(idx_ref, count_ref, held, keys_ref, out_ref, out_keys_ref, staged, blank, out_sem, blank_sem):
    slots, block, width = staged.shape
    parts = held.shape[1]
    out_keys_ref[...] = keys_ref[...]
    blank[...] = jnp.zeros(blank.shape, blank.dtype)
    steps = out_ref.shape[0] // block
    count = count_ref[0]
    live = pl.cdiv(count, block)

    def clear(s):
        return pltpu.make_async_copy(blank, out_ref.at[pl.ds(s * block, block)], blank_sem)

    def store(s):
        slot = lax.rem(s, slots)
        return pltpu.make_async_copy(staged.at[slot], out_ref.at[pl.ds(s * block, block)], out_sem.at[slot])

    def start_clear(s, carry):
        clear(s).start()
        return carry

    def step(s, carry):
        @pl.when(s >= slots)
        def _():
            store(s - slots).wait()

        slot = lax.rem(s, slots)

        def body(g, c):
            r = pl.multiple_of(g * 16, 16)
            rows = []
            for u in range(16):
                k = idx_ref[s * block + r + u]
                rows.append(jnp.concatenate([held[k, q] for q in range(parts)], 0))
            staged[slot, pl.ds(r, 16), :] = jnp.stack(rows, 0).reshape(16, width)
            return c

        lax.fori_loop(0, block // 16, body, 0)

        @pl.when((s + 1) * block > count)
        def _():
            row = lax.broadcasted_iota(jnp.int32, (block, width), 0) + s * block
            staged[slot] = jnp.where(row < count, staged[slot], jnp.zeros((block, width), staged.dtype))

        store(s).start()
        return carry

    lax.fori_loop(0, jnp.minimum(live, 1), step, 0)
    lax.fori_loop(live, steps, start_clear, 0)
    lax.fori_loop(1, live, step, 0)

    def end_store(s, carry):
        store(s).wait()
        return carry

    lax.fori_loop(jnp.maximum(live - slots, 0), live, end_store, 0)

    def end_clear(s, carry):
        clear(s).wait()
        return carry

    lax.fori_loop(live, steps, end_clear, 0)


def place(idx, count, rows, keys, width):
    n_out = idx.shape[0]
    block, slots = 128, 4
    return pl.pallas_call(
        place_kernel,
        out_shape=[jax.ShapeDtypeStruct((n_out, width), rows.dtype), jax.ShapeDtypeStruct(keys.shape, keys.dtype)],
        in_specs=[SMEM, SMEM, VMEM, VMEM],
        out_specs=[ANY, VMEM],
        scratch_shapes=[
            pltpu.VMEM((slots, block, width), rows.dtype),
            pltpu.VMEM((block, width), rows.dtype),
            pltpu.SemaphoreType.DMA((slots,)),
            pltpu.SemaphoreType.DMA,
        ],
        compiler_params=pltpu.CompilerParams(vmem_limit_bytes=24 * 1024 * 1024),
        name="place_rows",
    )(idx, count, rows, keys)


def solution(mesh):
    group_size = mesh.shape["g"]

    def local_part(keys_loc, rows_loc):
        n_dev = keys_loc.shape[0]
        width = rows_loc.shape[1]
        cap_rows = 2 * n_dev // group_size
        blocks, merged, idx, order, rows, starts, segs, own_count, short = sort_exchange(keys_loc.reshape(n_dev // LANES, LANES), rows_loc, BASE, RELAY, group_size)
        out_rows, out_keys = place(idx.reshape(-1), own_count, blocks, merged, width)

        def general(carry):
            wide = lax.all_to_all(pick(order.reshape(-1), starts, rows, cap_rows, group_size), "g", 0, 0, tiled=True)
            _, at = lax.sort((segs.reshape(-1), lax.iota(jnp.int32, segs.size)), num_keys=1)
            return jnp.int32(1), place(at, own_count, wide.reshape(-1, *wide.shape[2:]), merged, width)[0]

        _, out_rows = lax.while_loop(lambda carry: carry[0] == 0, general, (short[0], out_rows))
        return out_keys.reshape(-1), out_rows, own_count

    row_spec = P(("batch", "g"))
    mat_spec = P(("batch", "g"), None)
    return jax.shard_map(local_part, mesh=mesh, in_specs=(row_spec, mat_spec), out_specs=(row_spec, mat_spec, row_spec), check_vma=False)
```

```python
import functools

import jax
import jax.numpy as jnp
from jax import lax
from jax.experimental import pallas as pl
from jax.experimental.pallas import tpu as pltpu
from jax.sharding import PartitionSpec as P

PAD_KEY = 128.0
LANES = 128
SUB = 4
BASE = 65
RELAY = 4
FIRST, SECOND, THIRD = 6, 12, 22
SIDE = 4
CORES = 2
SLOTS = (((0, 2), (2, 0)), ((0, 1), (2, 3)), ((0, 3), (2, 1)), ((1, 0), (3, 2)), ((3, 0), (1, 2)), ((3, 1), (1, 3)), ((3, 3), (1, 1)), ((2, 2),))
STEPS = (*((dx, dy, dc) for slot in SLOTS for dc in (1, 0) for dx, dy in slot), (0, 0, 1))

VMEM = pl.BlockSpec(memory_space=pltpu.VMEM)
SMEM = pl.BlockSpec(memory_space=pltpu.SMEM)
ANY = pl.BlockSpec(memory_space=pl.ANY)
HBM = pl.BlockSpec(memory_space=pltpu.HBM)
MESH = pl.DeviceIdType.MESH
FROM_SRC, EXTRA, SHORT, OWN = range(4)


def bitonic_sort(keys, vals):
    rows, lanes = keys.shape
    pos = lax.broadcasted_iota(jnp.int32, keys.shape, 0) * lanes + lax.broadcasted_iota(jnp.int32, keys.shape, 1)

    def partner(x, j, low):
        axis, size, d = (1, lanes, j) if j < lanes else (0, rows, j // lanes)
        return jnp.where(low, pltpu.roll(x, size - d, axis), pltpu.roll(x, d, axis))

    k = 2
    while k <= rows * lanes:
        j = k // 2
        while j:
            low = (pos & j) == 0
            keep_min = jnp.logical_xor(low, (pos & k) != 0)
            other = partner(keys, j, low)
            swap = jnp.logical_or(jnp.logical_and(keep_min, keys > other), jnp.logical_and(jnp.logical_not(keep_min), keys < other))
            vals = jnp.where(swap, partner(vals, j, low), vals)
            keys = jnp.where(swap, other, keys)
            j //= 2
        k *= 2
    return keys, vals


def sample_row(keys, group_size):
    rows, lanes = keys.shape
    per = rows * lanes // group_size
    each = lanes // per
    lane = lax.broadcasted_iota(jnp.int32, keys.shape, 1)
    sub = lax.broadcasted_iota(jnp.int32, keys.shape, 0)
    acc = jnp.zeros(keys.shape, keys.dtype)
    for l in range(each):
        acc = jnp.where(lane == each * sub + l, keys[:, l * per : l * per + 1], acc)
    return jnp.sum(acc, axis=0, keepdims=True)


def pick_splitters(samples):
    group_size = samples.shape[0]
    lane = lax.broadcasted_iota(jnp.int32, samples.shape, 1)
    sub = lax.broadcasted_iota(jnp.int32, samples.shape, 0)
    fit = LANES // group_size
    merged = samples
    for f in range(1, fit):
        merged = jnp.where(lax.rem(sub, fit) == f, pltpu.roll(samples, f * group_size, 1), merged)
    packed = [jnp.sum(merged[c * fit : (c + 1) * fit], axis=0, keepdims=True) for c in range(group_size // fit)]
    less = [jnp.zeros(samples.shape, jnp.float32) for _ in packed]
    for q in range(group_size):
        a = jnp.broadcast_to(samples[:, q : q + 1], samples.shape)
        less = [n + (a < b).astype(jnp.float32) for n, b in zip(less, packed)]
    target = (sub * group_size + group_size // 2).astype(jnp.float32)
    found = jnp.zeros(samples.shape, jnp.float32)
    for n, b in zip(less, packed):
        found += jnp.where(jnp.sum(n, axis=0, keepdims=True) == target, b, 0.0)
    return jnp.where(sub == 0, -PAD_KEY, jnp.sum(found, axis=1, keepdims=True))


def count_below(keys, splitters):
    less = jnp.zeros(splitters.shape, jnp.float32)
    for r in range(keys.shape[0]):
        less += (keys[r : r + 1] < splitters).astype(jnp.float32)
    return jnp.sum(less, axis=1, keepdims=True)


def to_row(column, shape):
    lane = lax.broadcasted_iota(jnp.int32, shape, 1)
    sub = lax.broadcasted_iota(jnp.int32, shape, 0)
    return jnp.sum(jnp.where(lane == sub, column, 0.0), axis=0, keepdims=True)


def to_table(rows):
    rows = rows + [rows[-1]] * (8 - len(rows))
    return jnp.concatenate([jnp.broadcast_to(r, (1, LANES)) for r in rows], 0).astype(jnp.int32)


def make_plan(me, cap, relay, n_dev, edges):
    group_size = edges.shape[0]
    hubs = group_size // CORES
    lane = lax.broadcasted_iota(jnp.int32, edges.shape, 1)
    sub = lax.broadcasted_iota(jnp.int32, edges.shape, 0)
    after = jnp.where(lane == group_size - 1, float(n_dev), pltpu.roll(edges, LANES - 1, 1))
    counts = jnp.where(lane < group_size, after - edges, 0.0)
    over = jnp.maximum(counts - cap, 0.0)
    has = (over > 0).astype(jnp.float32)
    worst = jnp.maximum(jnp.max(jnp.sum(has, axis=0, keepdims=True), axis=1, keepdims=True), jnp.max(jnp.sum(has, axis=1, keepdims=True), axis=0, keepdims=True))
    most_over = jnp.max(jnp.max(over, axis=0, keepdims=True), axis=1, keepdims=True)
    short = ((worst <= 1) & (most_over <= relay * hubs)).astype(jnp.float32)
    my_counts = jnp.sum(jnp.where(lane == me, counts, 0.0), axis=1, keepdims=True)
    own = jnp.sum(my_counts, axis=0, keepdims=True)
    from_src = jnp.sum(has * sub.astype(jnp.float32), axis=0, keepdims=True)
    extra = jnp.sum(jnp.sum(jnp.where(sub == me, has * (edges + cap), 0.0), axis=0, keepdims=True), axis=1, keepdims=True)
    past = lane - cap
    slot = jnp.where(past < 0, sub * cap + lane, group_size * cap + lax.rem(past, hubs) * relay + past // hubs)
    slot = jnp.where(lane.astype(jnp.float32) < my_counts, slot, 0)
    return to_table([from_src, extra, short, own]), slot


def write_messages(start_ref, mine, msg_ref, edges):
    group_size = msg_ref.shape[0]
    tiles = mine.shape[0]
    n_dev = tiles * LANES
    lane = lax.broadcasted_iota(jnp.int32, (1, LANES), 1)

    def one(j):
        s = start_ref[0, j] & (2 * n_dev - 1)
        stop = jnp.where(j == group_size - 1, n_dev, start_ref[0, j + 1])
        t = s // LANES
        off = s & (LANES - 1)
        a = mine[pl.ds(jnp.minimum(t, tiles - 1), 1), :]
        b = mine[pl.ds(jnp.minimum(t + 1, tiles - 1), 1), :]
        shift = (LANES - off) & (LANES - 1)
        v = jnp.where(lane < LANES - off, pltpu.roll(a, shift, 1), pltpu.roll(b, shift, 1))
        msg_ref[j, 0:1] = jnp.where(lane < stop - s, v, PAD_KEY)
        msg_ref[j, 1:2] = edges

    def body(b, carry):
        for u in range(4):
            one(b * 4 + u)
        return carry

    lax.fori_loop(0, group_size // 4, body, 0)


def sort_exchange_kernel(
    group_size, cap, relay, block,
    keys_ref, rows_ref,
    out_ref, merged_ref, idx_ref, order_ref, split_ref, start_ref, seg_ref, own_ref, short_ref,
    fetched, held, outgoing, first, arrived, second, mine, my_samples, samples, msgs, inbox, edge_ref, edge_row, table_ref, order, starts, table,
    in_sem, own_sem, send_sem, recv_sem,
):
    me = lax.axis_index("g")
    core, x, y = lax.rem(me, CORES), lax.rem(me // CORES, SIDE), me // (CORES * SIDE)
    n, width = rows_ref.shape
    tiles = width // LANES

    def peer(d):
        return lax.rem(me + d, group_size)

    barrier = pltpu.get_barrier_semaphore()
    for d in range(1, group_size):
        pl.semaphore_signal(barrier, inc=1, device_id={"g": peer(d)}, device_id_type=MESH)

    def fetch(s):
        return pltpu.make_async_copy(rows_ref.at[pl.ds(s * block, block)], fetched.at[s], in_sem.at[s])

    def split(s):
        fetch(s).wait()

        def body(g, carry):
            r = pl.multiple_of(g * 16, 16)
            v = fetched[s, pl.ds(r, 16), :].reshape(16, tiles, LANES)
            for q in range(tiles // SUB):
                held[pl.ds(s * block + r, 16), q] = v[:, SUB * q : SUB * (q + 1)]
            return carry

        lax.fori_loop(0, block // 16, body, 0)

    for s in range(n // block):
        fetch(s).start()
    shape = keys_ref.shape
    places = lax.broadcasted_iota(jnp.int32, shape, 0) * LANES + lax.broadcasted_iota(jnp.int32, shape, 1)
    sorted_keys, sorted_places = bitonic_sort(keys_ref[...], places)
    mine[...] = sorted_keys
    order_ref[...] = sorted_places
    my_samples[...] = sample_row(sorted_keys, group_size)
    samples[pl.ds(me, 1)] = my_samples[...][None]
    pl.semaphore_wait(barrier, group_size - 1)

    def remote(d, dst, src_ref, dst_ref, kind):
        return pltpu.make_async_remote_copy(
            src_ref=src_ref, dst_ref=dst_ref, send_sem=send_sem.at[kind, d], recv_sem=recv_sem.at[kind, d], device_id={"g": dst}, device_id_type=MESH
        )

    def share(d):
        return remote(d, peer(d), msgs.at[peer(d)], inbox.at[me], 3)

    def share_samples(d):
        return remote(d, peer(d), my_samples, samples.at[me], 4)

    hubs = group_size // CORES
    chip = me // CORES
    forward = core == CORES - 1

    def near(d):
        return lax.rem(chip + d, hubs)

    def hop_one(d, c):
        return pltpu.make_async_remote_copy(
            src_ref=first.at[near(d)],
            dst_ref=arrived.at[me],
            send_sem=send_sem.at[1, d],
            recv_sem=recv_sem.at[1, c * hubs + d],
            device_id={"g": near(d) * CORES + CORES - 1},
            device_id_type=MESH,
        )

    def hop_two(d, hub):
        return pltpu.make_async_remote_copy(
            src_ref=second.at[peer(d)],
            dst_ref=out_ref.at[pl.ds(group_size * cap + chip * relay, relay)],
            send_sem=send_sem.at[2, d],
            recv_sem=recv_sem.at[2, hub],
            device_id={"g": peer(d)},
            device_id_type=MESH,
        )

    def far(s):
        dx, dy, dc = STEPS[s]
        return (lax.rem(y + dy, SIDE) * SIDE + lax.rem(x + dx, SIDE)) * CORES + lax.rem(core + dc, CORES)

    def base(s):
        return remote(s, far(s), outgoing.at[far(s)], out_ref.at[pl.ds(me * cap, cap)], 0)

    def each(act, begin=1, end=group_size):
        def body(d, carry):
            act(d)
            return carry

        lax.fori_loop(begin, end, body, 0)

    each(lambda d: share_samples(d).start())
    to_order = pltpu.make_async_copy(order_ref, order, own_sem.at[2])
    to_order.start()
    for s in range(n // block):
        split(s)
    each(lambda d: share_samples(d).wait())
    for i in range(group_size):
        edge_ref[i : i + 1] = samples[i]
    edges = to_row(count_below(mine[...], pick_splitters(edge_ref[...])), edge_ref.shape)
    edge_row[...] = edges
    start_ref[...] = to_table([edges])
    to_starts = pltpu.make_async_copy(start_ref, starts, own_sem.at[3])
    to_starts.start()
    to_order.wait()
    to_starts.wait()

    last = n - 1

    def row(k):
        k = k & last
        return held[order[k >> 7, k & (LANES - 1)] & last]

    def gather(dst):
        begin = starts[0, dst]

        def body(b, carry):
            for u in range(13):
                k = b * 13 + u
                outgoing[dst, k] = row(begin + k)
            return carry

        lax.fori_loop(0, cap // 13, body, 0)

    own_base = pltpu.make_async_copy(outgoing.at[me], out_ref.at[pl.ds(me * cap, cap)], own_sem.at[0])

    def send(begin, end):
        for s in range(begin, end):
            gather(far(s))
            if s > begin:
                base(s - 1).start()
        return end - 1

    waiting = send(0, FIRST)
    write_messages(starts, mine, msgs, edge_row[...])
    base(waiting).start()
    inbox[pl.ds(me, 1)] = msgs[pl.ds(me, 1)]
    gather(far(FIRST))
    each(lambda d: share(d).start())
    base(FIRST).start()
    waiting = send(FIRST + 1, SECOND)
    gather(me)
    base(waiting).start()
    each(lambda d: share(d).wait())
    for i in range(group_size):
        seg_ref[i : i + 1] = inbox[i, 0:1]
        edge_ref[i : i + 1] = inbox[i, 1:2]
    table_ref[...], slots = make_plan(me, cap, relay, n, edge_ref[...])
    to_smem = pltpu.make_async_copy(table_ref, table, own_sem.at[5])
    to_smem.start()
    own_base.start()
    to_smem.wait()
    extra = table[EXTRA, 0]

    def gather_extra(b, carry):
        for u in range(4):
            m = b * 4 + u
            for r in range(relay):
                first[m, r] = row(extra + r * hubs + m)
        return carry

    lax.fori_loop(0, hubs // 4, gather_extra, 0)
    gather(far(SECOND))
    each(lambda d: hop_one(d, core).start(), 1, hubs)

    @pl.when(jnp.logical_not(forward))
    def _():
        hop_one(0, 0).start()

    @pl.when(forward)
    def _():
        arrived[me] = first[chip]

    base(SECOND).start()
    waiting = send(SECOND + 1, THIRD)
    own_ref[0] = table[OWN, 0]
    short_ref[0] = table[SHORT, 0]
    base(waiting).start()
    merged_ref[...], idx_ref[...] = bitonic_sort(seg_ref[...], slots)
    gather(far(THIRD))
    each(lambda d: hop_one(d, core).wait_send(), 1, hubs)

    @pl.when(jnp.logical_not(forward))
    def _():
        hop_one(0, 0).wait_send()

    @pl.when(forward)
    def _():
        for c in range(CORES - 1):
            hop_one(0, c).wait_recv()
        for c in range(CORES):
            each(lambda d: hop_one(d, c).wait_recv(), 1, hubs)
        for j in range(group_size):
            second[j] = arrived[table[FROM_SRC, j] & (group_size - 1)]
        each(lambda d: hop_two(d, chip).start())
        out_ref[pl.ds(group_size * cap + chip * relay, relay)] = second[me]

    base(THIRD).start()
    waiting = send(THIRD + 1, group_size - 1)
    keep = pltpu.make_async_copy(held, split_ref, own_sem.at[4])
    keep.start()
    base(waiting).start()
    for s in range(group_size - 1):
        base(s).wait()
    each(lambda d: hop_two(0, near(d)).wait_recv(), 1, hubs)

    @pl.when(jnp.logical_not(forward))
    def _():
        hop_two(0, chip).wait_recv()

    @pl.when(forward)
    def _():
        each(lambda d: hop_two(d, chip).wait_send())

    own_base.wait()
    keep.wait()


def sort_exchange(keys, rows, cap, relay, group_size):
    n, width = rows.shape
    block = 512
    row = (width // (SUB * LANES), SUB, LANES)
    segs = (group_size, LANES)
    sems = pltpu.SemaphoreType.DMA
    return pl.pallas_call(
        functools.partial(sort_exchange_kernel, group_size, cap, relay, block),
        out_shape=[
            pltpu.VMEM((group_size * cap + group_size // CORES * relay, *row), rows.dtype),
            jax.ShapeDtypeStruct(segs, keys.dtype),
            pltpu.VMEM(segs, jnp.int32),
            jax.ShapeDtypeStruct(keys.shape, jnp.int32),
            jax.ShapeDtypeStruct((n, *row), rows.dtype),
            jax.ShapeDtypeStruct((8, LANES), jnp.int32),
            jax.ShapeDtypeStruct(segs, keys.dtype),
            jax.ShapeDtypeStruct((1,), jnp.int32),
            jax.ShapeDtypeStruct((1,), jnp.int32),
        ],
        in_specs=[VMEM, HBM],
        out_specs=[VMEM, VMEM, VMEM, VMEM, HBM, VMEM, VMEM, SMEM, SMEM],
        scratch_shapes=[
            pltpu.VMEM((n // block, block, width), rows.dtype),
            pltpu.VMEM((n, *row), rows.dtype),
            pltpu.VMEM((group_size, cap, *row), rows.dtype),
            pltpu.VMEM((group_size // CORES, relay, *row), rows.dtype),
            pltpu.VMEM((group_size, relay, *row), rows.dtype),
            pltpu.VMEM((group_size, relay, *row), rows.dtype),
            pltpu.VMEM(keys.shape, keys.dtype),
            pltpu.VMEM((1, LANES), keys.dtype),
            pltpu.VMEM((group_size, 1, LANES), keys.dtype),
            pltpu.VMEM((group_size, 2, LANES), keys.dtype),
            pltpu.VMEM((group_size, 2, LANES), keys.dtype),
            pltpu.VMEM(segs, jnp.float32),
            pltpu.VMEM((1, LANES), jnp.float32),
            pltpu.VMEM((8, LANES), jnp.int32),
            pltpu.SMEM(keys.shape, jnp.int32),
            pltpu.SMEM((8, LANES), jnp.int32),
            pltpu.SMEM((8, LANES), jnp.int32),
            sems((n // block,)),
            sems((6,)),
            sems((5, group_size)),
            sems((5, group_size)),
        ],
        compiler_params=pltpu.CompilerParams(collective_id=0, has_side_effects=True, vmem_limit_bytes=52 * 1024 * 1024),
        name="sort_exchange",
    )(keys, rows)


def pick_kernel(cap, group_size, order_ref, table_ref, rows_ref, out_ref):
    last = rows_ref.shape[0] - 1

    def per_dst(j, carry):
        first = table_ref[0, j]

        def body(b, c):
            for u in range(8):
                k = b * 8 + u
                out_ref[j, k] = rows_ref[order_ref[jnp.minimum(first + k, last)]]
            return c

        return lax.fori_loop(0, cap // 8, body, carry)

    lax.fori_loop(0, group_size, per_dst, 0)


def pick(order, table, rows, cap, group_size):
    return pl.pallas_call(
        functools.partial(pick_kernel, cap, group_size),
        out_shape=jax.ShapeDtypeStruct((group_size, cap, *rows.shape[1:]), rows.dtype),
        in_specs=[SMEM, SMEM, VMEM],
        out_specs=VMEM,
        name="pick_rows",
    )(order, table, rows)


def place_kernel(idx_ref, count_ref, held, keys_ref, out_ref, out_keys_ref, staged, blank, out_sem, blank_sem):
    slots, block, width = staged.shape
    parts = held.shape[1]
    out_keys_ref[...] = keys_ref[...]
    blank[...] = jnp.zeros(blank.shape, blank.dtype)
    steps = out_ref.shape[0] // block
    count = count_ref[0]
    live = pl.cdiv(count, block)

    def clear(s):
        return pltpu.make_async_copy(blank, out_ref.at[pl.ds(s * block, block)], blank_sem)

    def store(s):
        slot = lax.rem(s, slots)
        return pltpu.make_async_copy(staged.at[slot], out_ref.at[pl.ds(s * block, block)], out_sem.at[slot])

    def start_clear(s, carry):
        clear(s).start()
        return carry

    def step(s, carry):
        @pl.when(s >= slots)
        def _():
            store(s - slots).wait()

        slot = lax.rem(s, slots)

        def body(g, c):
            r = pl.multiple_of(g * 16, 16)
            rows = []
            for u in range(16):
                k = idx_ref[s * block + r + u]
                rows.append(jnp.concatenate([held[k, q] for q in range(parts)], 0))
            staged[slot, pl.ds(r, 16), :] = jnp.stack(rows, 0).reshape(16, width)
            return c

        lax.fori_loop(0, pl.cdiv(jnp.minimum(count - s * block, block), 16), body, 0)

        @pl.when((s + 1) * block > count)
        def _():
            row = lax.broadcasted_iota(jnp.int32, (block, width), 0) + s * block
            staged[slot] = jnp.where(row < count, staged[slot], jnp.zeros((block, width), staged.dtype))

        store(s).start()
        return carry

    lax.fori_loop(live, steps, start_clear, 0)
    lax.fori_loop(0, live, step, 0)

    def end_store(s, carry):
        store(s).wait()
        return carry

    lax.fori_loop(jnp.maximum(live - slots, 0), live, end_store, 0)

    def end_clear(s, carry):
        clear(s).wait()
        return carry

    lax.fori_loop(live, steps, end_clear, 0)


def place(idx, count, rows, keys, width):
    n_out = idx.shape[0]
    block, slots = 128, 4
    return pl.pallas_call(
        place_kernel,
        out_shape=[jax.ShapeDtypeStruct((n_out, width), rows.dtype), jax.ShapeDtypeStruct(keys.shape, keys.dtype)],
        in_specs=[SMEM, SMEM, VMEM, VMEM],
        out_specs=[ANY, VMEM],
        scratch_shapes=[
            pltpu.VMEM((slots, block, width), rows.dtype),
            pltpu.VMEM((block, width), rows.dtype),
            pltpu.SemaphoreType.DMA((slots,)),
            pltpu.SemaphoreType.DMA,
        ],
        compiler_params=pltpu.CompilerParams(vmem_limit_bytes=24 * 1024 * 1024),
        name="place_rows",
    )(idx, count, rows, keys)


def solution(mesh):
    group_size = mesh.shape["g"]

    def local_part(keys_loc, rows_loc):
        n_dev = keys_loc.shape[0]
        width = rows_loc.shape[1]
        cap_rows = 2 * n_dev // group_size
        blocks, merged, idx, order, rows, starts, segs, own_count, short = sort_exchange(keys_loc.reshape(n_dev // LANES, LANES), rows_loc, BASE, RELAY, group_size)
        out_rows, out_keys = place(idx.reshape(-1), own_count, blocks, merged, width)

        def general(carry):
            wide = lax.all_to_all(pick(order.reshape(-1), starts, rows, cap_rows, group_size), "g", 0, 0, tiled=True)
            _, at = lax.sort((segs.reshape(-1), lax.iota(jnp.int32, segs.size)), num_keys=1)
            return jnp.int32(1), place(at, own_count, wide.reshape(-1, *wide.shape[2:]), merged, width)[0]

        _, out_rows = lax.while_loop(lambda carry: carry[0] == 0, general, (short[0], out_rows))
        return out_keys.reshape(-1), out_rows, own_count

    row_spec = P(("batch", "g"))
    mat_spec = P(("batch", "g"), None)
    return jax.shard_map(local_part, mesh=mesh, in_specs=(row_spec, mat_spec), out_specs=(row_spec, mat_spec, row_spec), check_vma=False)
```

```python
import functools

import jax
import jax.numpy as jnp
from jax import lax
from jax.experimental import pallas as pl
from jax.experimental.pallas import tpu as pltpu
from jax.sharding import PartitionSpec as P

PAD_KEY = 128.0
LANES = 128
SUB = 4
BASE = 65
RELAY = 4
FIRST, SECOND, THIRD = 6, 12, 22
SIDE = 4
CORES = 2
SLOTS = (((0, 2), (2, 0)), ((0, 1), (2, 3)), ((0, 3), (2, 1)), ((1, 0), (3, 2)), ((3, 0), (1, 2)), ((3, 1), (1, 3)), ((3, 3), (1, 1)), ((2, 2),))
STEPS = (*((dx, dy, dc) for slot in SLOTS for dc in (1, 0) for dx, dy in slot), (0, 0, 1))

VMEM = pl.BlockSpec(memory_space=pltpu.VMEM)
SMEM = pl.BlockSpec(memory_space=pltpu.SMEM)
ANY = pl.BlockSpec(memory_space=pl.ANY)
HBM = pl.BlockSpec(memory_space=pltpu.HBM)
MESH = pl.DeviceIdType.MESH
FROM_SRC, EXTRA, SHORT, OWN = range(4)


def bitonic_sort(keys, vals):
    rows, lanes = keys.shape
    pos = lax.broadcasted_iota(jnp.int32, keys.shape, 0) * lanes + lax.broadcasted_iota(jnp.int32, keys.shape, 1)

    def partner(x, j, low):
        axis, size, d = (1, lanes, j) if j < lanes else (0, rows, j // lanes)
        return jnp.where(low, pltpu.roll(x, size - d, axis), pltpu.roll(x, d, axis))

    k = 2
    while k <= rows * lanes:
        j = k // 2
        while j:
            low = (pos & j) == 0
            keep_min = jnp.logical_xor(low, (pos & k) != 0)
            other = partner(keys, j, low)
            swap = jnp.logical_or(jnp.logical_and(keep_min, keys > other), jnp.logical_and(jnp.logical_not(keep_min), keys < other))
            vals = jnp.where(swap, partner(vals, j, low), vals)
            keys = jnp.where(swap, other, keys)
            j //= 2
        k *= 2
    return keys, vals


def sample_row(keys, group_size):
    rows, lanes = keys.shape
    per = rows * lanes // group_size
    each = lanes // per
    lane = lax.broadcasted_iota(jnp.int32, keys.shape, 1)
    sub = lax.broadcasted_iota(jnp.int32, keys.shape, 0)
    acc = jnp.zeros(keys.shape, keys.dtype)
    for l in range(each):
        acc = jnp.where(lane == each * sub + l, keys[:, l * per : l * per + 1], acc)
    return jnp.sum(acc, axis=0, keepdims=True)


def pick_splitters(samples):
    group_size = samples.shape[0]
    lane = lax.broadcasted_iota(jnp.int32, samples.shape, 1)
    sub = lax.broadcasted_iota(jnp.int32, samples.shape, 0)
    fit = LANES // group_size
    merged = samples
    for f in range(1, fit):
        merged = jnp.where(lax.rem(sub, fit) == f, pltpu.roll(samples, f * group_size, 1), merged)
    packed = [jnp.sum(merged[c * fit : (c + 1) * fit], axis=0, keepdims=True) for c in range(group_size // fit)]
    less = [jnp.zeros(samples.shape, jnp.float32) for _ in packed]
    for q in range(group_size):
        a = jnp.broadcast_to(samples[:, q : q + 1], samples.shape)
        less = [n + (a < b).astype(jnp.float32) for n, b in zip(less, packed)]
    target = (sub * group_size + group_size // 2).astype(jnp.float32)
    found = jnp.zeros(samples.shape, jnp.float32)
    for n, b in zip(less, packed):
        found += jnp.where(jnp.sum(n, axis=0, keepdims=True) == target, b, 0.0)
    return jnp.where(sub == 0, -PAD_KEY, jnp.sum(found, axis=1, keepdims=True))


def count_below(keys, splitters):
    less = jnp.zeros(splitters.shape, jnp.float32)
    for r in range(keys.shape[0]):
        less += (keys[r : r + 1] < splitters).astype(jnp.float32)
    return jnp.sum(less, axis=1, keepdims=True)


def to_row(column, shape):
    lane = lax.broadcasted_iota(jnp.int32, shape, 1)
    sub = lax.broadcasted_iota(jnp.int32, shape, 0)
    return jnp.sum(jnp.where(lane == sub, column, 0.0), axis=0, keepdims=True)


def to_table(rows):
    rows = rows + [rows[-1]] * (8 - len(rows))
    return jnp.concatenate([jnp.broadcast_to(r, (1, LANES)) for r in rows], 0).astype(jnp.int32)


def make_plan(me, cap, relay, n_dev, edges):
    group_size = edges.shape[0]
    hubs = group_size // CORES
    lane = lax.broadcasted_iota(jnp.int32, edges.shape, 1)
    sub = lax.broadcasted_iota(jnp.int32, edges.shape, 0)
    after = jnp.where(lane == group_size - 1, float(n_dev), pltpu.roll(edges, LANES - 1, 1))
    counts = jnp.where(lane < group_size, after - edges, 0.0)
    over = jnp.maximum(counts - cap, 0.0)
    has = (over > 0).astype(jnp.float32)
    worst = jnp.maximum(jnp.max(jnp.sum(has, axis=0, keepdims=True), axis=1, keepdims=True), jnp.max(jnp.sum(has, axis=1, keepdims=True), axis=0, keepdims=True))
    most_over = jnp.max(jnp.max(over, axis=0, keepdims=True), axis=1, keepdims=True)
    short = ((worst <= 1) & (most_over <= relay * hubs)).astype(jnp.float32)
    my_counts = jnp.sum(jnp.where(lane == me, counts, 0.0), axis=1, keepdims=True)
    own = jnp.sum(my_counts, axis=0, keepdims=True)
    from_src = jnp.sum(has * sub.astype(jnp.float32), axis=0, keepdims=True)
    extra = jnp.sum(jnp.sum(jnp.where(sub == me, has * (edges + cap), 0.0), axis=0, keepdims=True), axis=1, keepdims=True)
    past = lane - cap
    slot = jnp.where(past < 0, sub * cap + lane, group_size * cap + lax.rem(past, hubs) * relay + past // hubs)
    slot = jnp.where(lane.astype(jnp.float32) < my_counts, slot, 0)
    return to_table([from_src, extra, short, own]), slot


def write_messages(start_ref, mine, msg_ref, edges):
    group_size = msg_ref.shape[0]
    tiles = mine.shape[0]
    n_dev = tiles * LANES
    lane = lax.broadcasted_iota(jnp.int32, (1, LANES), 1)

    def one(j):
        s = start_ref[0, j] & (2 * n_dev - 1)
        stop = jnp.where(j == group_size - 1, n_dev, start_ref[0, j + 1])
        t = s // LANES
        off = s & (LANES - 1)
        a = mine[pl.ds(jnp.minimum(t, tiles - 1), 1), :]
        b = mine[pl.ds(jnp.minimum(t + 1, tiles - 1), 1), :]
        shift = (LANES - off) & (LANES - 1)
        v = jnp.where(lane < LANES - off, pltpu.roll(a, shift, 1), pltpu.roll(b, shift, 1))
        msg_ref[j, 0:1] = jnp.where(lane < stop - s, v, PAD_KEY)
        msg_ref[j, 1:2] = edges

    def body(b, carry):
        for u in range(4):
            one(b * 4 + u)
        return carry

    lax.fori_loop(0, group_size // 4, body, 0)


def sort_exchange_kernel(
    group_size, cap, relay, block,
    keys_ref, rows_ref,
    out_ref, merged_ref, idx_ref, order_ref, split_ref, start_ref, seg_ref, own_ref, short_ref,
    fetched, held, outgoing, first, arrived, second, mine, my_samples, samples, msgs, inbox, edge_ref, edge_row, table_ref, order, starts, table,
    in_sem, own_sem, send_sem, recv_sem,
):
    me = lax.axis_index("g")
    core, x, y = lax.rem(me, CORES), lax.rem(me // CORES, SIDE), me // (CORES * SIDE)
    n, width = rows_ref.shape
    tiles = width // LANES

    def peer(d):
        return lax.rem(me + d, group_size)

    barrier = pltpu.get_barrier_semaphore()
    for d in range(1, group_size):
        pl.semaphore_signal(barrier, inc=1, device_id={"g": peer(d)}, device_id_type=MESH)

    def fetch(s):
        return pltpu.make_async_copy(rows_ref.at[pl.ds(s * block, block)], fetched.at[s], in_sem.at[s])

    def split(s):
        fetch(s).wait()

        def body(g, carry):
            r = pl.multiple_of(g * 16, 16)
            v = fetched[s, pl.ds(r, 16), :].reshape(16, tiles, LANES)
            for q in range(tiles // SUB):
                held[pl.ds(s * block + r, 16), q] = v[:, SUB * q : SUB * (q + 1)]
            return carry

        lax.fori_loop(0, block // 16, body, 0)

    for s in range(n // block):
        fetch(s).start()
    shape = keys_ref.shape
    places = lax.broadcasted_iota(jnp.int32, shape, 0) * LANES + lax.broadcasted_iota(jnp.int32, shape, 1)
    sorted_keys, sorted_places = bitonic_sort(keys_ref[...], places)
    mine[...] = sorted_keys
    order_ref[...] = sorted_places
    my_samples[...] = sample_row(sorted_keys, group_size)
    samples[pl.ds(me, 1)] = my_samples[...][None]
    pl.semaphore_wait(barrier, group_size - 1)

    def remote(d, dst, src_ref, dst_ref, kind):
        return pltpu.make_async_remote_copy(
            src_ref=src_ref, dst_ref=dst_ref, send_sem=send_sem.at[kind, d], recv_sem=recv_sem.at[kind, d], device_id={"g": dst}, device_id_type=MESH
        )

    def share(d):
        return remote(d, peer(d), msgs.at[peer(d)], inbox.at[me], 3)

    def share_samples(d):
        return remote(d, peer(d), my_samples, samples.at[me], 4)

    hubs = group_size // CORES
    chip = me // CORES
    forward = core == CORES - 1

    def near(d):
        return lax.rem(chip + d, hubs)

    def hop_one(d, c):
        return pltpu.make_async_remote_copy(
            src_ref=first.at[near(d)],
            dst_ref=arrived.at[me],
            send_sem=send_sem.at[1, d],
            recv_sem=recv_sem.at[1, c * hubs + d],
            device_id={"g": near(d) * CORES + CORES - 1},
            device_id_type=MESH,
        )

    def hop_two(d, hub):
        return pltpu.make_async_remote_copy(
            src_ref=second.at[peer(d)],
            dst_ref=out_ref.at[pl.ds(group_size * cap + chip * relay, relay)],
            send_sem=send_sem.at[2, d],
            recv_sem=recv_sem.at[2, hub],
            device_id={"g": peer(d)},
            device_id_type=MESH,
        )

    def far(s):
        dx, dy, dc = STEPS[s]
        return (lax.rem(y + dy, SIDE) * SIDE + lax.rem(x + dx, SIDE)) * CORES + lax.rem(core + dc, CORES)

    def base(s):
        return remote(s, far(s), outgoing.at[far(s)], out_ref.at[pl.ds(me * cap, cap)], 0)

    def each(act, begin=1, end=group_size):
        def body(d, carry):
            act(d)
            return carry

        lax.fori_loop(begin, end, body, 0)

    each(lambda d: share_samples(d).start())
    to_order = pltpu.make_async_copy(order_ref, order, own_sem.at[2])
    to_order.start()
    for s in range(n // block):
        split(s)
    each(lambda d: share_samples(d).wait())
    for i in range(group_size):
        edge_ref[i : i + 1] = samples[i]
    edges = to_row(count_below(mine[...], pick_splitters(edge_ref[...])), edge_ref.shape)
    edge_row[...] = edges
    start_ref[...] = to_table([edges])
    to_starts = pltpu.make_async_copy(start_ref, starts, own_sem.at[3])
    to_starts.start()
    to_order.wait()
    to_starts.wait()

    last = n - 1

    def row(k):
        k = k & last
        return held[order[k >> 7, k & (LANES - 1)] & last]

    def gather(dst):
        begin = starts[0, dst]

        def body(b, carry):
            for u in range(13):
                k = b * 13 + u
                outgoing[dst, k] = row(begin + k)
            return carry

        lax.fori_loop(0, cap // 13, body, 0)

    own_base = pltpu.make_async_copy(outgoing.at[me], out_ref.at[pl.ds(me * cap, cap)], own_sem.at[0])

    def send(begin, end):
        for s in range(begin, end):
            gather(far(s))
            if s > begin:
                base(s - 1).start()
        return end - 1

    waiting = send(0, FIRST)
    write_messages(starts, mine, msgs, edge_row[...])
    base(waiting).start()
    inbox[pl.ds(me, 1)] = msgs[pl.ds(me, 1)]
    gather(far(FIRST))
    each(lambda d: share(d).start())
    base(FIRST).start()
    waiting = send(FIRST + 1, SECOND)
    gather(me)
    base(waiting).start()
    each(lambda d: share(d).wait())
    for i in range(group_size):
        seg_ref[i : i + 1] = inbox[i, 0:1]
        edge_ref[i : i + 1] = inbox[i, 1:2]
    table_ref[...], slots = make_plan(me, cap, relay, n, edge_ref[...])
    to_smem = pltpu.make_async_copy(table_ref, table, own_sem.at[5])
    to_smem.start()
    own_base.start()
    to_smem.wait()
    extra = table[EXTRA, 0]

    def gather_extra(b, carry):
        for u in range(4):
            m = b * 4 + u
            for r in range(relay):
                first[m, r] = row(extra + r * hubs + m)
        return carry

    lax.fori_loop(0, hubs // 4, gather_extra, 0)
    gather(far(SECOND))
    each(lambda d: hop_one(d, core).start(), 1, hubs)

    @pl.when(jnp.logical_not(forward))
    def _():
        hop_one(0, 0).start()

    @pl.when(forward)
    def _():
        arrived[me] = first[chip]

    base(SECOND).start()
    waiting = send(SECOND + 1, THIRD)
    own_ref[0] = table[OWN, 0]
    short_ref[0] = table[SHORT, 0]
    base(waiting).start()
    merged_ref[...], idx_ref[...] = bitonic_sort(seg_ref[...], slots)
    gather(far(THIRD))
    each(lambda d: hop_one(d, core).wait_send(), 1, hubs)

    @pl.when(jnp.logical_not(forward))
    def _():
        hop_one(0, 0).wait_send()

    @pl.when(forward)
    def _():
        for c in range(CORES - 1):
            hop_one(0, c).wait_recv()
        for c in range(CORES):
            each(lambda d: hop_one(d, c).wait_recv(), 1, hubs)
        for j in range(group_size):
            second[j] = arrived[table[FROM_SRC, j] & (group_size - 1)]
        each(lambda d: hop_two(d, chip).start())
        out_ref[pl.ds(group_size * cap + chip * relay, relay)] = second[me]

    base(THIRD).start()
    waiting = send(THIRD + 1, group_size - 1)
    keep = pltpu.make_async_copy(held, split_ref, own_sem.at[4])
    keep.start()
    base(waiting).start()
    for s in range(group_size - 1):
        base(s).wait()
    each(lambda d: hop_two(0, near(d)).wait_recv(), 1, hubs)

    @pl.when(jnp.logical_not(forward))
    def _():
        hop_two(0, chip).wait_recv()

    @pl.when(forward)
    def _():
        each(lambda d: hop_two(d, chip).wait_send())

    own_base.wait()
    keep.wait()


def sort_exchange(keys, rows, cap, relay, group_size):
    n, width = rows.shape
    block = 512
    row = (width // (SUB * LANES), SUB, LANES)
    segs = (group_size, LANES)
    sems = pltpu.SemaphoreType.DMA
    return pl.pallas_call(
        functools.partial(sort_exchange_kernel, group_size, cap, relay, block),
        out_shape=[
            pltpu.VMEM((group_size * cap + group_size // CORES * relay, *row), rows.dtype),
            jax.ShapeDtypeStruct(segs, keys.dtype),
            pltpu.VMEM(segs, jnp.int32),
            jax.ShapeDtypeStruct(keys.shape, jnp.int32),
            jax.ShapeDtypeStruct((n, *row), rows.dtype),
            jax.ShapeDtypeStruct((8, LANES), jnp.int32),
            jax.ShapeDtypeStruct(segs, keys.dtype),
            jax.ShapeDtypeStruct((1,), jnp.int32),
            jax.ShapeDtypeStruct((1,), jnp.int32),
        ],
        in_specs=[VMEM, HBM],
        out_specs=[VMEM, VMEM, VMEM, VMEM, HBM, VMEM, VMEM, SMEM, SMEM],
        scratch_shapes=[
            pltpu.VMEM((n // block, block, width), rows.dtype),
            pltpu.VMEM((n, *row), rows.dtype),
            pltpu.VMEM((group_size, cap, *row), rows.dtype),
            pltpu.VMEM((group_size // CORES, relay, *row), rows.dtype),
            pltpu.VMEM((group_size, relay, *row), rows.dtype),
            pltpu.VMEM((group_size, relay, *row), rows.dtype),
            pltpu.VMEM(keys.shape, keys.dtype),
            pltpu.VMEM((1, LANES), keys.dtype),
            pltpu.VMEM((group_size, 1, LANES), keys.dtype),
            pltpu.VMEM((group_size, 2, LANES), keys.dtype),
            pltpu.VMEM((group_size, 2, LANES), keys.dtype),
            pltpu.VMEM(segs, jnp.float32),
            pltpu.VMEM((1, LANES), jnp.float32),
            pltpu.VMEM((8, LANES), jnp.int32),
            pltpu.SMEM(keys.shape, jnp.int32),
            pltpu.SMEM((8, LANES), jnp.int32),
            pltpu.SMEM((8, LANES), jnp.int32),
            sems((n // block,)),
            sems((6,)),
            sems((5, group_size)),
            sems((5, group_size)),
        ],
        compiler_params=pltpu.CompilerParams(collective_id=0, has_side_effects=True, vmem_limit_bytes=52 * 1024 * 1024),
        name="sort_exchange",
    )(keys, rows)


def pick_kernel(cap, group_size, order_ref, table_ref, rows_ref, out_ref):
    last = rows_ref.shape[0] - 1

    def per_dst(j, carry):
        first = table_ref[0, j]

        def body(b, c):
            for u in range(8):
                k = b * 8 + u
                out_ref[j, k] = rows_ref[order_ref[jnp.minimum(first + k, last)]]
            return c

        return lax.fori_loop(0, cap // 8, body, carry)

    lax.fori_loop(0, group_size, per_dst, 0)


def pick(order, table, rows, cap, group_size):
    return pl.pallas_call(
        functools.partial(pick_kernel, cap, group_size),
        out_shape=jax.ShapeDtypeStruct((group_size, cap, *rows.shape[1:]), rows.dtype),
        in_specs=[SMEM, SMEM, VMEM],
        out_specs=VMEM,
        name="pick_rows",
    )(order, table, rows)


def place_kernel(idx_ref, count_ref, held, keys_ref, out_ref, out_keys_ref, staged, blank, out_sem, blank_sem, keys_sem):
    slots, block, width = staged.shape
    parts = held.shape[1]
    keys_copy = pltpu.make_async_copy(keys_ref, out_keys_ref, keys_sem)
    keys_copy.start()
    blank[...] = jnp.zeros(blank.shape, blank.dtype)
    steps = out_ref.shape[0] // block
    count = count_ref[0]
    live = pl.cdiv(count, block)

    def clear(s):
        return pltpu.make_async_copy(blank, out_ref.at[pl.ds(s * block, block)], blank_sem)

    def store(s):
        slot = lax.rem(s, slots)
        return pltpu.make_async_copy(staged.at[slot], out_ref.at[pl.ds(s * block, block)], out_sem.at[slot])

    def start_clear(s, carry):
        clear(s).start()
        return carry

    def step(s, carry):
        @pl.when(s >= slots)
        def _():
            store(s - slots).wait()

        slot = lax.rem(s, slots)

        def body(g, c):
            for half in range(2):
                r = pl.multiple_of(g * 32 + half * 16, 16)
                rows = []
                for u in range(16):
                    k = idx_ref[s * block + r + u]
                    rows.append(jnp.concatenate([held[k, q] for q in range(parts)], 0))
                staged[slot, pl.ds(r, 16), :] = jnp.stack(rows, 0).reshape(16, width)
            return c

        lax.fori_loop(0, pl.cdiv(jnp.minimum(count - s * block, block), 32), body, 0)

        @pl.when((s + 1) * block > count)
        def _():
            row = lax.broadcasted_iota(jnp.int32, (block, width), 0) + s * block
            staged[slot] = jnp.where(row < count, staged[slot], jnp.zeros((block, width), staged.dtype))

        store(s).start()
        return carry

    lax.fori_loop(live, steps, start_clear, 0)
    lax.fori_loop(0, live, step, 0)

    def end_store(s, carry):
        store(s).wait()
        return carry

    lax.fori_loop(jnp.maximum(live - slots, 0), live, end_store, 0)

    def end_clear(s, carry):
        clear(s).wait()
        return carry

    lax.fori_loop(live, steps, end_clear, 0)
    keys_copy.wait()


def place(idx, count, rows, keys, width):
    n_out = idx.shape[0]
    block, slots = 128, 4
    return pl.pallas_call(
        place_kernel,
        out_shape=[jax.ShapeDtypeStruct((n_out, width), rows.dtype), jax.ShapeDtypeStruct(keys.shape, keys.dtype)],
        in_specs=[SMEM, SMEM, VMEM, VMEM],
        out_specs=[ANY, ANY],
        scratch_shapes=[
            pltpu.VMEM((slots, block, width), rows.dtype),
            pltpu.VMEM((block, width), rows.dtype),
            pltpu.SemaphoreType.DMA((slots,)),
            pltpu.SemaphoreType.DMA,
            pltpu.SemaphoreType.DMA,
        ],
        compiler_params=pltpu.CompilerParams(vmem_limit_bytes=24 * 1024 * 1024),
        name="place_rows",
    )(idx, count, rows, keys)


def solution(mesh):
    group_size = mesh.shape["g"]

    def local_part(keys_loc, rows_loc):
        n_dev = keys_loc.shape[0]
        width = rows_loc.shape[1]
        cap_rows = 2 * n_dev // group_size
        blocks, merged, idx, order, rows, starts, segs, own_count, short = sort_exchange(keys_loc.reshape(n_dev // LANES, LANES), rows_loc, BASE, RELAY, group_size)
        out_rows, out_keys = place(idx.reshape(-1), own_count, blocks, merged, width)

        def general(carry):
            wide = lax.all_to_all(pick(order.reshape(-1), starts, rows, cap_rows, group_size), "g", 0, 0, tiled=True)
            _, at = lax.sort((segs.reshape(-1), lax.iota(jnp.int32, segs.size)), num_keys=1)
            return jnp.int32(1), place(at, own_count, wide.reshape(-1, *wide.shape[2:]), merged, width)[0]

        _, out_rows = lax.while_loop(lambda carry: carry[0] == 0, general, (short[0], out_rows))
        return out_keys.reshape(-1), out_rows, own_count

    row_spec = P(("batch", "g"))
    mat_spec = P(("batch", "g"), None)
    return jax.shard_map(local_part, mesh=mesh, in_specs=(row_spec, mat_spec), out_specs=(row_spec, mat_spec, row_spec), check_vma=False)
```

```python
import functools

import jax
import jax.numpy as jnp
from jax import lax
from jax.experimental import pallas as pl
from jax.experimental.pallas import tpu as pltpu
from jax.sharding import PartitionSpec as P

PAD_KEY = 128.0
LANES = 128
SUB = 4
BASE = 65
RELAY = 4
FIRST, SECOND, THIRD = 6, 12, 22
SIDE = 4
CORES = 2
SLOTS = (((0, 2), (2, 0)), ((0, 1), (2, 3)), ((0, 3), (2, 1)), ((1, 0), (3, 2)), ((3, 0), (1, 2)), ((3, 1), (1, 3)), ((3, 3), (1, 1)), ((2, 2),))
STEPS = (*((dx, dy, dc) for slot in SLOTS for dc in (1, 0) for dx, dy in slot), (0, 0, 1))

VMEM = pl.BlockSpec(memory_space=pltpu.VMEM)
SMEM = pl.BlockSpec(memory_space=pltpu.SMEM)
ANY = pl.BlockSpec(memory_space=pl.ANY)
HBM = pl.BlockSpec(memory_space=pltpu.HBM)
MESH = pl.DeviceIdType.MESH
FROM_SRC, EXTRA, SHORT, OWN = range(4)


def bitonic_sort(keys, vals):
    rows, lanes = keys.shape
    pos = lax.broadcasted_iota(jnp.int32, keys.shape, 0) * lanes + lax.broadcasted_iota(jnp.int32, keys.shape, 1)

    def partner(x, j, low):
        axis, size, d = (1, lanes, j) if j < lanes else (0, rows, j // lanes)
        return jnp.where(low, pltpu.roll(x, size - d, axis), pltpu.roll(x, d, axis))

    k = 2
    while k <= rows * lanes:
        j = k // 2
        while j:
            low = (pos & j) == 0
            keep_min = jnp.logical_xor(low, (pos & k) != 0)
            other = partner(keys, j, low)
            swap = jnp.logical_or(jnp.logical_and(keep_min, keys > other), jnp.logical_and(jnp.logical_not(keep_min), keys < other))
            vals = jnp.where(swap, partner(vals, j, low), vals)
            keys = jnp.where(swap, other, keys)
            j //= 2
        k *= 2
    return keys, vals


def sample_row(keys, group_size):
    rows, lanes = keys.shape
    per = rows * lanes // group_size
    each = lanes // per
    lane = lax.broadcasted_iota(jnp.int32, keys.shape, 1)
    sub = lax.broadcasted_iota(jnp.int32, keys.shape, 0)
    acc = jnp.zeros(keys.shape, keys.dtype)
    for l in range(each):
        acc = jnp.where(lane == each * sub + l, keys[:, l * per : l * per + 1], acc)
    return jnp.sum(acc, axis=0, keepdims=True)


def pick_splitters(samples):
    group_size = samples.shape[0]
    lane = lax.broadcasted_iota(jnp.int32, samples.shape, 1)
    sub = lax.broadcasted_iota(jnp.int32, samples.shape, 0)
    fit = LANES // group_size
    merged = samples
    for f in range(1, fit):
        merged = jnp.where(lax.rem(sub, fit) == f, pltpu.roll(samples, f * group_size, 1), merged)
    packed = [jnp.sum(merged[c * fit : (c + 1) * fit], axis=0, keepdims=True) for c in range(group_size // fit)]
    less = [jnp.zeros(samples.shape, jnp.float32) for _ in packed]
    for q in range(group_size):
        a = jnp.broadcast_to(samples[:, q : q + 1], samples.shape)
        less = [n + (a < b).astype(jnp.float32) for n, b in zip(less, packed)]
    target = (sub * group_size + group_size // 2).astype(jnp.float32)
    found = jnp.zeros(samples.shape, jnp.float32)
    for n, b in zip(less, packed):
        found += jnp.where(jnp.sum(n, axis=0, keepdims=True) == target, b, 0.0)
    return jnp.where(sub == 0, -PAD_KEY, jnp.sum(found, axis=1, keepdims=True))


def count_below(keys, splitters):
    less = jnp.zeros(splitters.shape, jnp.float32)
    for r in range(keys.shape[0]):
        less += (keys[r : r + 1] < splitters).astype(jnp.float32)
    return jnp.sum(less, axis=1, keepdims=True)


def to_row(column, shape):
    lane = lax.broadcasted_iota(jnp.int32, shape, 1)
    sub = lax.broadcasted_iota(jnp.int32, shape, 0)
    return jnp.sum(jnp.where(lane == sub, column, 0.0), axis=0, keepdims=True)


def to_table(rows):
    rows = rows + [rows[-1]] * (8 - len(rows))
    return jnp.concatenate([jnp.broadcast_to(r, (1, LANES)) for r in rows], 0).astype(jnp.int32)


def make_plan(me, cap, relay, n_dev, edges):
    group_size = edges.shape[0]
    hubs = group_size // CORES
    lane = lax.broadcasted_iota(jnp.int32, edges.shape, 1)
    sub = lax.broadcasted_iota(jnp.int32, edges.shape, 0)
    after = jnp.where(lane == group_size - 1, float(n_dev), pltpu.roll(edges, LANES - 1, 1))
    counts = jnp.where(lane < group_size, after - edges, 0.0)
    over = jnp.maximum(counts - cap, 0.0)
    has = (over > 0).astype(jnp.float32)
    worst = jnp.maximum(jnp.max(jnp.sum(has, axis=0, keepdims=True), axis=1, keepdims=True), jnp.max(jnp.sum(has, axis=1, keepdims=True), axis=0, keepdims=True))
    most_over = jnp.max(jnp.max(over, axis=0, keepdims=True), axis=1, keepdims=True)
    short = ((worst <= 1) & (most_over <= relay * hubs)).astype(jnp.float32)
    my_counts = jnp.sum(jnp.where(lane == me, counts, 0.0), axis=1, keepdims=True)
    own = jnp.sum(my_counts, axis=0, keepdims=True)
    from_src = jnp.sum(has * sub.astype(jnp.float32), axis=0, keepdims=True)
    extra = jnp.sum(jnp.sum(jnp.where(sub == me, has * (edges + cap), 0.0), axis=0, keepdims=True), axis=1, keepdims=True)
    past = lane - cap
    slot = jnp.where(past < 0, sub * cap + lane, group_size * cap + lax.rem(past, hubs) * relay + past // hubs)
    slot = jnp.where(lane.astype(jnp.float32) < my_counts, slot, 0)
    return to_table([from_src, extra, short, own]), slot


def write_messages(start_ref, mine, msg_ref, edges):
    group_size = msg_ref.shape[0]
    tiles = mine.shape[0]
    n_dev = tiles * LANES
    lane = lax.broadcasted_iota(jnp.int32, (1, LANES), 1)

    def one(j):
        s = start_ref[0, j] & (2 * n_dev - 1)
        stop = jnp.where(j == group_size - 1, n_dev, start_ref[0, j + 1])
        t = s // LANES
        off = s & (LANES - 1)
        a = mine[pl.ds(jnp.minimum(t, tiles - 1), 1), :]
        b = mine[pl.ds(jnp.minimum(t + 1, tiles - 1), 1), :]
        shift = (LANES - off) & (LANES - 1)
        v = jnp.where(lane < LANES - off, pltpu.roll(a, shift, 1), pltpu.roll(b, shift, 1))
        msg_ref[j, 0:1] = jnp.where(lane < stop - s, v, PAD_KEY)
        msg_ref[j, 1:2] = edges

    def body(b, carry):
        for u in range(4):
            one(b * 4 + u)
        return carry

    lax.fori_loop(0, group_size // 4, body, 0)


def sort_exchange_kernel(
    group_size, cap, relay, block,
    keys_ref, rows_ref,
    out_ref, merged_ref, idx_ref, order_ref, split_ref, start_ref, seg_ref, own_ref, short_ref,
    fetched, held, outgoing, first, arrived, second, mine, my_samples, samples, msgs, inbox, edge_ref, edge_row, table_ref, order, starts, table,
    in_sem, own_sem, send_sem, recv_sem,
):
    me = lax.axis_index("g")
    core, x, y = lax.rem(me, CORES), lax.rem(me // CORES, SIDE), me // (CORES * SIDE)
    n, width = rows_ref.shape
    tiles = width // LANES

    def peer(d):
        return lax.rem(me + d, group_size)

    barrier = pltpu.get_barrier_semaphore()
    for d in range(1, group_size):
        pl.semaphore_signal(barrier, inc=1, device_id={"g": peer(d)}, device_id_type=MESH)

    def fetch(s):
        return pltpu.make_async_copy(rows_ref.at[pl.ds(s * block, block)], fetched.at[s], in_sem.at[s])

    def split(s):
        fetch(s).wait()

        def body(g, carry):
            r = pl.multiple_of(g * 16, 16)
            v = fetched[s, pl.ds(r, 16), :].reshape(16, tiles, LANES)
            for q in range(tiles // SUB):
                held[pl.ds(s * block + r, 16), q] = v[:, SUB * q : SUB * (q + 1)]
            return carry

        lax.fori_loop(0, block // 16, body, 0)

    for s in range(n // block):
        fetch(s).start()
    shape = keys_ref.shape
    places = lax.broadcasted_iota(jnp.int32, shape, 0) * LANES + lax.broadcasted_iota(jnp.int32, shape, 1)
    sorted_keys, sorted_places = bitonic_sort(keys_ref[...], places)
    mine[...] = sorted_keys
    order_ref[...] = sorted_places
    my_samples[...] = sample_row(sorted_keys, group_size)
    samples[pl.ds(me, 1)] = my_samples[...][None]
    pl.semaphore_wait(barrier, group_size - 1)

    def remote(d, dst, src_ref, dst_ref, kind):
        return pltpu.make_async_remote_copy(
            src_ref=src_ref, dst_ref=dst_ref, send_sem=send_sem.at[kind, d], recv_sem=recv_sem.at[kind, d], device_id={"g": dst}, device_id_type=MESH
        )

    def share(d):
        return remote(d, peer(d), msgs.at[peer(d)], inbox.at[me], 3)

    def share_samples(d):
        return remote(d, peer(d), my_samples, samples.at[me], 4)

    hubs = group_size // CORES
    chip = me // CORES
    forward = core == CORES - 1

    def near(d):
        return lax.rem(chip + d, hubs)

    def hop_one(d, c):
        return pltpu.make_async_remote_copy(
            src_ref=first.at[near(d)],
            dst_ref=arrived.at[me],
            send_sem=send_sem.at[1, d],
            recv_sem=recv_sem.at[1, c * hubs + d],
            device_id={"g": near(d) * CORES + CORES - 1},
            device_id_type=MESH,
        )

    def hop_two(d, hub):
        return pltpu.make_async_remote_copy(
            src_ref=second.at[peer(d)],
            dst_ref=out_ref.at[pl.ds(group_size * cap + chip * relay, relay)],
            send_sem=send_sem.at[2, d],
            recv_sem=recv_sem.at[2, hub],
            device_id={"g": peer(d)},
            device_id_type=MESH,
        )

    def far(s):
        dx, dy, dc = STEPS[s]
        return (lax.rem(y + dy, SIDE) * SIDE + lax.rem(x + dx, SIDE)) * CORES + lax.rem(core + dc, CORES)

    def base(s):
        return remote(s, far(s), outgoing.at[far(s)], out_ref.at[pl.ds(me * cap, cap)], 0)

    def each(act, begin=1, end=group_size):
        def body(d, carry):
            act(d)
            return carry

        lax.fori_loop(begin, end, body, 0)

    each(lambda d: share_samples(d).start())
    to_order = pltpu.make_async_copy(order_ref, order, own_sem.at[2])
    to_order.start()
    for s in range(n // block):
        split(s)
    each(lambda d: share_samples(d).wait())
    for i in range(group_size):
        edge_ref[i : i + 1] = samples[i]
    edges = to_row(count_below(mine[...], pick_splitters(edge_ref[...])), edge_ref.shape)
    edge_row[...] = edges
    start_ref[...] = to_table([edges])
    to_starts = pltpu.make_async_copy(start_ref, starts, own_sem.at[3])
    to_starts.start()
    to_order.wait()
    to_starts.wait()

    last = n - 1

    def row(k):
        k = k & last
        return held[order[k >> 7, k & (LANES - 1)] & last]

    def gather(dst):
        begin = starts[0, dst]

        def body(b, carry):
            for u in range(13):
                k = b * 13 + u
                outgoing[dst, k] = row(begin + k)
            return carry

        lax.fori_loop(0, cap // 13, body, 0)

    own_base = pltpu.make_async_copy(outgoing.at[me], out_ref.at[pl.ds(me * cap, cap)], own_sem.at[0])

    def send(begin, end):
        for s in range(begin, end):
            gather(far(s))
            if s > begin:
                base(s - 1).start()
        return end - 1

    waiting = send(0, FIRST)
    write_messages(starts, mine, msgs, edge_row[...])
    base(waiting).start()
    inbox[pl.ds(me, 1)] = msgs[pl.ds(me, 1)]
    gather(far(FIRST))
    each(lambda d: share(d).start())
    base(FIRST).start()
    waiting = send(FIRST + 1, SECOND)
    gather(me)
    base(waiting).start()
    each(lambda d: share(d).wait())
    for i in range(group_size):
        seg_ref[i : i + 1] = inbox[i, 0:1]
        edge_ref[i : i + 1] = inbox[i, 1:2]
    table_ref[...], slots = make_plan(me, cap, relay, n, edge_ref[...])
    to_smem = pltpu.make_async_copy(table_ref, table, own_sem.at[5])
    to_smem.start()
    own_base.start()
    to_smem.wait()
    extra = table[EXTRA, 0]

    def gather_extra(b, carry):
        for u in range(4):
            m = b * 4 + u
            for r in range(relay):
                first[m, r] = row(extra + r * hubs + m)
        return carry

    lax.fori_loop(0, hubs // 4, gather_extra, 0)
    gather(far(SECOND))
    each(lambda d: hop_one(d, core).start(), 1, hubs)

    @pl.when(jnp.logical_not(forward))
    def _():
        hop_one(0, 0).start()

    @pl.when(forward)
    def _():
        arrived[me] = first[chip]

    base(SECOND).start()
    waiting = send(SECOND + 1, THIRD)
    own_ref[0] = table[OWN, 0]
    short_ref[0] = table[SHORT, 0]
    base(waiting).start()
    merged_ref[...], idx_ref[...] = bitonic_sort(seg_ref[...], slots)
    gather(far(THIRD))
    each(lambda d: hop_one(d, core).wait_send(), 1, hubs)

    @pl.when(jnp.logical_not(forward))
    def _():
        hop_one(0, 0).wait_send()

    @pl.when(forward)
    def _():
        for c in range(CORES - 1):
            hop_one(0, c).wait_recv()
        for c in range(CORES):
            each(lambda d: hop_one(d, c).wait_recv(), 1, hubs)
        for j in range(group_size):
            second[j] = arrived[table[FROM_SRC, j] & (group_size - 1)]
        each(lambda d: hop_two(d, chip).start())
        out_ref[pl.ds(group_size * cap + chip * relay, relay)] = second[me]

    base(THIRD).start()
    waiting = send(THIRD + 1, group_size - 1)
    keep = pltpu.make_async_copy(held, split_ref, own_sem.at[4])
    keep.start()
    base(waiting).start()
    for s in range(group_size - 1):
        base(s).wait()
    each(lambda d: hop_two(0, near(d)).wait_recv(), 1, hubs)

    @pl.when(jnp.logical_not(forward))
    def _():
        hop_two(0, chip).wait_recv()

    @pl.when(forward)
    def _():
        each(lambda d: hop_two(d, chip).wait_send())

    own_base.wait()
    keep.wait()


def sort_exchange(keys, rows, cap, relay, group_size):
    n, width = rows.shape
    block = 512
    row = (width // (SUB * LANES), SUB, LANES)
    segs = (group_size, LANES)
    sems = pltpu.SemaphoreType.DMA
    return pl.pallas_call(
        functools.partial(sort_exchange_kernel, group_size, cap, relay, block),
        out_shape=[
            pltpu.VMEM((group_size * cap + group_size // CORES * relay, *row), rows.dtype),
            jax.ShapeDtypeStruct(segs, keys.dtype),
            pltpu.VMEM(segs, jnp.int32),
            jax.ShapeDtypeStruct(keys.shape, jnp.int32),
            jax.ShapeDtypeStruct((n, *row), rows.dtype),
            jax.ShapeDtypeStruct((8, LANES), jnp.int32),
            jax.ShapeDtypeStruct(segs, keys.dtype),
            jax.ShapeDtypeStruct((1,), jnp.int32),
            jax.ShapeDtypeStruct((1,), jnp.int32),
        ],
        in_specs=[VMEM, HBM],
        out_specs=[VMEM, VMEM, VMEM, VMEM, HBM, VMEM, VMEM, SMEM, SMEM],
        scratch_shapes=[
            pltpu.VMEM((n // block, block, width), rows.dtype),
            pltpu.VMEM((n, *row), rows.dtype),
            pltpu.VMEM((group_size, cap, *row), rows.dtype),
            pltpu.VMEM((group_size // CORES, relay, *row), rows.dtype),
            pltpu.VMEM((group_size, relay, *row), rows.dtype),
            pltpu.VMEM((group_size, relay, *row), rows.dtype),
            pltpu.VMEM(keys.shape, keys.dtype),
            pltpu.VMEM((1, LANES), keys.dtype),
            pltpu.VMEM((group_size, 1, LANES), keys.dtype),
            pltpu.VMEM((group_size, 2, LANES), keys.dtype),
            pltpu.VMEM((group_size, 2, LANES), keys.dtype),
            pltpu.VMEM(segs, jnp.float32),
            pltpu.VMEM((1, LANES), jnp.float32),
            pltpu.VMEM((8, LANES), jnp.int32),
            pltpu.SMEM(keys.shape, jnp.int32),
            pltpu.SMEM((8, LANES), jnp.int32),
            pltpu.SMEM((8, LANES), jnp.int32),
            sems((n // block,)),
            sems((6,)),
            sems((5, group_size)),
            sems((5, group_size)),
        ],
        compiler_params=pltpu.CompilerParams(collective_id=0, has_side_effects=True, vmem_limit_bytes=52 * 1024 * 1024),
        name="sort_exchange",
    )(keys, rows)


def pick_kernel(cap, group_size, order_ref, table_ref, rows_ref, out_ref):
    last = rows_ref.shape[0] - 1

    def per_dst(j, carry):
        first = table_ref[0, j]

        def body(b, c):
            for u in range(8):
                k = b * 8 + u
                out_ref[j, k] = rows_ref[order_ref[jnp.minimum(first + k, last)]]
            return c

        return lax.fori_loop(0, cap // 8, body, carry)

    lax.fori_loop(0, group_size, per_dst, 0)


def pick(order, table, rows, cap, group_size):
    return pl.pallas_call(
        functools.partial(pick_kernel, cap, group_size),
        out_shape=jax.ShapeDtypeStruct((group_size, cap, *rows.shape[1:]), rows.dtype),
        in_specs=[SMEM, SMEM, VMEM],
        out_specs=VMEM,
        name="pick_rows",
    )(order, table, rows)


def place_kernel(idx_ref, count_ref, held, keys_ref, out_ref, out_keys_ref, staged, blank, idx, out_sem, blank_sem, keys_sem, idx_sem):
    slots, block, width = staged.shape
    parts = held.shape[1]
    early = 8
    idx_copies = [
        pltpu.make_async_copy(idx_ref.at[pl.ds(a, b - a)], idx.at[pl.ds(a, b - a)], idx_sem.at[i])
        for i, (a, b) in enumerate(((0, early), (early, idx_ref.shape[0])))
    ]
    for c in idx_copies:
        c.start()
    keys_copy = pltpu.make_async_copy(keys_ref, out_keys_ref, keys_sem)
    keys_copy.start()
    blank[...] = jnp.zeros(blank.shape, blank.dtype)
    steps = out_ref.shape[0] // block
    count = count_ref[0]
    live = pl.cdiv(count, block)

    def clear(s):
        return pltpu.make_async_copy(blank, out_ref.at[pl.ds(s * block, block)], blank_sem)

    def store(s):
        slot = lax.rem(s, slots)
        return pltpu.make_async_copy(staged.at[slot], out_ref.at[pl.ds(s * block, block)], out_sem.at[slot])

    def start_clear(s, carry):
        clear(s).start()
        return carry

    def step(s, carry):
        @pl.when(s >= slots)
        def _():
            store(s - slots).wait()

        slot = lax.rem(s, slots)

        def body(g, c):
            for half in range(2):
                r = pl.multiple_of(g * 32 + half * 16, 16)
                rows = []
                for u in range(16):
                    k = idx[s, r + u]
                    rows.append(jnp.concatenate([held[k, q] for q in range(parts)], 0))
                staged[slot, pl.ds(r, 16), :] = jnp.stack(rows, 0).reshape(16, width)
            return c

        lax.fori_loop(0, pl.cdiv(jnp.minimum(count - s * block, block), 32), body, 0)

        @pl.when((s + 1) * block > count)
        def _():
            row = lax.broadcasted_iota(jnp.int32, (block, width), 0) + s * block
            staged[slot] = jnp.where(row < count, staged[slot], jnp.zeros((block, width), staged.dtype))

        store(s).start()
        return carry

    lax.fori_loop(live, steps, start_clear, 0)
    idx_copies[0].wait()
    lax.fori_loop(0, jnp.minimum(live, early), step, 0)
    idx_copies[1].wait()
    lax.fori_loop(early, live, step, 0)

    def end_store(s, carry):
        store(s).wait()
        return carry

    lax.fori_loop(jnp.maximum(live - slots, 0), live, end_store, 0)

    def end_clear(s, carry):
        clear(s).wait()
        return carry

    lax.fori_loop(live, steps, end_clear, 0)
    keys_copy.wait()


def place(idx, count, rows, keys, width):
    n_out, block = idx.size, idx.shape[1]
    slots = 4
    return pl.pallas_call(
        place_kernel,
        out_shape=[jax.ShapeDtypeStruct((n_out, width), rows.dtype), jax.ShapeDtypeStruct(keys.shape, keys.dtype)],
        in_specs=[VMEM, SMEM, VMEM, VMEM],
        out_specs=[ANY, ANY],
        scratch_shapes=[
            pltpu.VMEM((slots, block, width), rows.dtype),
            pltpu.VMEM((block, width), rows.dtype),
            pltpu.SMEM(idx.shape, jnp.int32),
            pltpu.SemaphoreType.DMA((slots,)),
            pltpu.SemaphoreType.DMA,
            pltpu.SemaphoreType.DMA,
            pltpu.SemaphoreType.DMA((2,)),
        ],
        compiler_params=pltpu.CompilerParams(vmem_limit_bytes=24 * 1024 * 1024),
        name="place_rows",
    )(idx, count, rows, keys)


def solution(mesh):
    group_size = mesh.shape["g"]

    def local_part(keys_loc, rows_loc):
        n_dev = keys_loc.shape[0]
        width = rows_loc.shape[1]
        cap_rows = 2 * n_dev // group_size
        blocks, merged, idx, order, rows, starts, segs, own_count, short = sort_exchange(keys_loc.reshape(n_dev // LANES, LANES), rows_loc, BASE, RELAY, group_size)
        out_rows, out_keys = place(idx, own_count, blocks, merged, width)

        def general(carry):
            wide = lax.all_to_all(pick(order.reshape(-1), starts, rows, cap_rows, group_size), "g", 0, 0, tiled=True)
            _, at = lax.sort((segs.reshape(-1), lax.iota(jnp.int32, segs.size)), num_keys=1)
            return jnp.int32(1), place(at.reshape(idx.shape), own_count, wide.reshape(-1, *wide.shape[2:]), merged, width)[0]

        _, out_rows = lax.while_loop(lambda carry: carry[0] == 0, general, (short[0], out_rows))
        return out_keys.reshape(-1), out_rows, own_count

    row_spec = P(("batch", "g"))
    mat_spec = P(("batch", "g"), None)
    return jax.shard_map(local_part, mesh=mesh, in_specs=(row_spec, mat_spec), out_specs=(row_spec, mat_spec, row_spec), check_vma=False)
```

```python
import functools

import jax
import jax.numpy as jnp
from jax import lax
from jax.experimental import pallas as pl
from jax.experimental.pallas import tpu as pltpu
from jax.sharding import PartitionSpec as P

PAD_KEY = 128.0
LANES = 128
SUB = 4
BASE = 65
RELAY = 4
FIRST, SECOND, THIRD = 6, 12, 22
SIDE = 4
CORES = 2
SLOTS = (((0, 2), (2, 0)), ((0, 1), (2, 3)), ((0, 3), (2, 1)), ((1, 0), (3, 2)), ((3, 0), (1, 2)), ((3, 1), (1, 3)), ((3, 3), (1, 1)), ((2, 2),))
STEPS = (*((dx, dy, dc) for slot in SLOTS for dc in (1, 0) for dx, dy in slot), (0, 0, 1))

VMEM = pl.BlockSpec(memory_space=pltpu.VMEM)
SMEM = pl.BlockSpec(memory_space=pltpu.SMEM)
ANY = pl.BlockSpec(memory_space=pl.ANY)
HBM = pl.BlockSpec(memory_space=pltpu.HBM)
MESH = pl.DeviceIdType.MESH
FROM_SRC, EXTRA, SHORT, OWN = range(4)


def bitonic_sort(keys, vals):
    rows, lanes = keys.shape
    pos = lax.broadcasted_iota(jnp.int32, keys.shape, 0) * lanes + lax.broadcasted_iota(jnp.int32, keys.shape, 1)

    def partner(x, j, low):
        axis, size, d = (1, lanes, j) if j < lanes else (0, rows, j // lanes)
        return jnp.where(low, pltpu.roll(x, size - d, axis), pltpu.roll(x, d, axis))

    k = 2
    while k <= rows * lanes:
        j = k // 2
        while j:
            low = (pos & j) == 0
            keep_min = jnp.logical_xor(low, (pos & k) != 0)
            other = partner(keys, j, low)
            swap = jnp.logical_or(jnp.logical_and(keep_min, keys > other), jnp.logical_and(jnp.logical_not(keep_min), keys < other))
            vals = jnp.where(swap, partner(vals, j, low), vals)
            keys = jnp.where(swap, other, keys)
            j //= 2
        k *= 2
    return keys, vals


def sample_row(keys, group_size):
    rows, lanes = keys.shape
    per = rows * lanes // group_size
    each = lanes // per
    lane = lax.broadcasted_iota(jnp.int32, keys.shape, 1)
    sub = lax.broadcasted_iota(jnp.int32, keys.shape, 0)
    acc = jnp.zeros(keys.shape, keys.dtype)
    for l in range(each):
        acc = jnp.where(lane == each * sub + l, keys[:, l * per : l * per + 1], acc)
    return jnp.sum(acc, axis=0, keepdims=True)


def pick_splitters(samples):
    group_size = samples.shape[0]
    lane = lax.broadcasted_iota(jnp.int32, samples.shape, 1)
    sub = lax.broadcasted_iota(jnp.int32, samples.shape, 0)
    fit = LANES // group_size
    merged = samples
    for f in range(1, fit):
        merged = jnp.where(lax.rem(sub, fit) == f, pltpu.roll(samples, f * group_size, 1), merged)
    packed = [jnp.sum(merged[c * fit : (c + 1) * fit], axis=0, keepdims=True) for c in range(group_size // fit)]
    less = [jnp.zeros(samples.shape, jnp.float32) for _ in packed]
    for q in range(group_size):
        a = jnp.broadcast_to(samples[:, q : q + 1], samples.shape)
        less = [n + (a < b).astype(jnp.float32) for n, b in zip(less, packed)]
    target = (sub * group_size + group_size // 2).astype(jnp.float32)
    found = jnp.zeros(samples.shape, jnp.float32)
    for n, b in zip(less, packed):
        found += jnp.where(jnp.sum(n, axis=0, keepdims=True) == target, b, 0.0)
    return jnp.where(sub == 0, -PAD_KEY, jnp.sum(found, axis=1, keepdims=True))


def count_below(keys, splitters):
    less = jnp.zeros(splitters.shape, jnp.float32)
    for r in range(keys.shape[0]):
        less += (keys[r : r + 1] < splitters).astype(jnp.float32)
    return jnp.sum(less, axis=1, keepdims=True)


def to_row(column, shape):
    lane = lax.broadcasted_iota(jnp.int32, shape, 1)
    sub = lax.broadcasted_iota(jnp.int32, shape, 0)
    return jnp.sum(jnp.where(lane == sub, column, 0.0), axis=0, keepdims=True)


def to_table(rows):
    rows = rows + [rows[-1]] * (8 - len(rows))
    return jnp.concatenate([jnp.broadcast_to(r, (1, LANES)) for r in rows], 0).astype(jnp.int32)


def make_plan(me, cap, relay, n_dev, edges):
    group_size = edges.shape[0]
    hubs = group_size // CORES
    lane = lax.broadcasted_iota(jnp.int32, edges.shape, 1)
    sub = lax.broadcasted_iota(jnp.int32, edges.shape, 0)
    after = jnp.where(lane == group_size - 1, float(n_dev), pltpu.roll(edges, LANES - 1, 1))
    counts = jnp.where(lane < group_size, after - edges, 0.0)
    over = jnp.maximum(counts - cap, 0.0)
    has = (over > 0).astype(jnp.float32)
    worst = jnp.maximum(jnp.max(jnp.sum(has, axis=0, keepdims=True), axis=1, keepdims=True), jnp.max(jnp.sum(has, axis=1, keepdims=True), axis=0, keepdims=True))
    most_over = jnp.max(jnp.max(over, axis=0, keepdims=True), axis=1, keepdims=True)
    short = ((worst <= 1) & (most_over <= relay * hubs)).astype(jnp.float32)
    my_counts = jnp.sum(jnp.where(lane == me, counts, 0.0), axis=1, keepdims=True)
    own = jnp.sum(my_counts, axis=0, keepdims=True)
    from_src = jnp.sum(has * sub.astype(jnp.float32), axis=0, keepdims=True)
    extra = jnp.sum(jnp.sum(jnp.where(sub == me, has * (edges + cap), 0.0), axis=0, keepdims=True), axis=1, keepdims=True)
    past = lane - cap
    slot = jnp.where(past < 0, sub * cap + lane, group_size * cap + lax.rem(past, hubs) * relay + past // hubs)
    slot = jnp.where(lane.astype(jnp.float32) < my_counts, slot, 0)
    return to_table([from_src, extra, short, own]), slot


def write_messages(start_ref, mine, msg_ref, edges):
    group_size = msg_ref.shape[0]
    tiles = mine.shape[0]
    n_dev = tiles * LANES
    lane = lax.broadcasted_iota(jnp.int32, (1, LANES), 1)

    def one(j):
        s = start_ref[0, j] & (2 * n_dev - 1)
        stop = jnp.where(j == group_size - 1, n_dev, start_ref[0, j + 1])
        t = s // LANES
        off = s & (LANES - 1)
        a = mine[pl.ds(jnp.minimum(t, tiles - 1), 1), :]
        b = mine[pl.ds(jnp.minimum(t + 1, tiles - 1), 1), :]
        shift = (LANES - off) & (LANES - 1)
        v = jnp.where(lane < LANES - off, pltpu.roll(a, shift, 1), pltpu.roll(b, shift, 1))
        msg_ref[j, 0:1] = jnp.where(lane < stop - s, v, PAD_KEY)
        msg_ref[j, 1:2] = edges

    def body(b, carry):
        for u in range(4):
            one(b * 4 + u)
        return carry

    lax.fori_loop(0, group_size // 4, body, 0)


def sort_exchange_kernel(
    group_size, cap, relay, block,
    keys_ref, rows_ref,
    out_ref, merged_ref, idx_ref, order_ref, split_ref, start_ref, seg_ref, own_ref, short_ref,
    fetched, held, outgoing, first, arrived, second, mine, my_samples, samples, msgs, inbox, edge_ref, edge_row, table_ref, order, starts, table,
    in_sem, own_sem, send_sem, recv_sem,
):
    me = lax.axis_index("g")
    core, x, y = lax.rem(me, CORES), lax.rem(me // CORES, SIDE), me // (CORES * SIDE)
    n, width = rows_ref.shape
    tiles = width // LANES

    def peer(d):
        return lax.rem(me + d, group_size)

    barrier = pltpu.get_barrier_semaphore()
    for d in range(1, group_size):
        pl.semaphore_signal(barrier, inc=1, device_id={"g": peer(d)}, device_id_type=MESH)

    def fetch(s):
        return pltpu.make_async_copy(rows_ref.at[pl.ds(s * block, block)], fetched.at[s], in_sem.at[s])

    def split(s):
        fetch(s).wait()

        def body(g, carry):
            r = pl.multiple_of(g * 16, 16)
            v = fetched[s, pl.ds(r, 16), :].reshape(16, tiles, LANES)
            for q in range(tiles // SUB):
                held[pl.ds(s * block + r, 16), q] = v[:, SUB * q : SUB * (q + 1)]
            return carry

        lax.fori_loop(0, block // 16, body, 0)

    for s in range(n // block):
        fetch(s).start()
    shape = keys_ref.shape
    places = lax.broadcasted_iota(jnp.int32, shape, 0) * LANES + lax.broadcasted_iota(jnp.int32, shape, 1)
    sorted_keys, sorted_places = bitonic_sort(keys_ref[...], places)
    mine[...] = sorted_keys
    order_ref[...] = sorted_places
    my_samples[...] = sample_row(sorted_keys, group_size)
    samples[pl.ds(me, 1)] = my_samples[...][None]
    pl.semaphore_wait(barrier, group_size - 1)

    def remote(d, dst, src_ref, dst_ref, kind):
        return pltpu.make_async_remote_copy(
            src_ref=src_ref, dst_ref=dst_ref, send_sem=send_sem.at[kind, d], recv_sem=recv_sem.at[kind, d], device_id={"g": dst}, device_id_type=MESH
        )

    def share(d):
        return remote(d, peer(d), msgs.at[peer(d)], inbox.at[me], 3)

    def share_samples(d):
        return remote(d, peer(d), my_samples, samples.at[me], 4)

    hubs = group_size // CORES
    chip = me // CORES
    forward = core == CORES - 1

    def near(d):
        return lax.rem(chip + d, hubs)

    def hop_one(d, c):
        return pltpu.make_async_remote_copy(
            src_ref=first.at[near(d)],
            dst_ref=arrived.at[me],
            send_sem=send_sem.at[1, d],
            recv_sem=recv_sem.at[1, c * hubs + d],
            device_id={"g": near(d) * CORES + CORES - 1},
            device_id_type=MESH,
        )

    def hop_two(d, hub):
        return pltpu.make_async_remote_copy(
            src_ref=second.at[peer(d)],
            dst_ref=out_ref.at[pl.ds(group_size * cap + chip * relay, relay)],
            send_sem=send_sem.at[2, d],
            recv_sem=recv_sem.at[2, hub],
            device_id={"g": peer(d)},
            device_id_type=MESH,
        )

    def far(s):
        dx, dy, dc = STEPS[s]
        return (lax.rem(y + dy, SIDE) * SIDE + lax.rem(x + dx, SIDE)) * CORES + lax.rem(core + dc, CORES)

    def base(s):
        return remote(s, far(s), outgoing.at[far(s)], out_ref.at[pl.ds(me * cap, cap)], 0)

    def each(act, begin=1, end=group_size):
        def body(d, carry):
            act(d)
            return carry

        lax.fori_loop(begin, end, body, 0)

    each(lambda d: share_samples(d).start())
    to_order = pltpu.make_async_copy(order_ref, order, own_sem.at[2])
    to_order.start()
    for s in range(n // block):
        split(s)
    each(lambda d: share_samples(d).wait())
    for i in range(group_size):
        edge_ref[i : i + 1] = samples[i]
    edges = to_row(count_below(mine[...], pick_splitters(edge_ref[...])), edge_ref.shape)
    edge_row[...] = edges
    start_ref[...] = to_table([edges])
    to_starts = pltpu.make_async_copy(start_ref, starts, own_sem.at[3])
    to_starts.start()
    to_order.wait()
    to_starts.wait()

    last = n - 1

    def row(k):
        k = k & last
        return held[order[k >> 7, k & (LANES - 1)] & last]

    def gather(dst):
        begin = starts[0, dst]

        def body(b, carry):
            for u in range(13):
                k = b * 13 + u
                outgoing[dst, k] = row(begin + k)
            return carry

        lax.fori_loop(0, cap // 13, body, 0)

    own_base = pltpu.make_async_copy(outgoing.at[me], out_ref.at[pl.ds(me * cap, cap)], own_sem.at[0])

    def send(begin, end):
        for s in range(begin, end):
            gather(far(s))
            if s > begin:
                base(s - 1).start()
        return end - 1

    waiting = send(0, FIRST)
    write_messages(starts, mine, msgs, edge_row[...])
    base(waiting).start()
    inbox[pl.ds(me, 1)] = msgs[pl.ds(me, 1)]
    gather(far(FIRST))
    each(lambda d: share(d).start())
    base(FIRST).start()
    waiting = send(FIRST + 1, SECOND)
    gather(me)
    base(waiting).start()
    each(lambda d: share(d).wait())
    for i in range(group_size):
        seg_ref[i : i + 1] = inbox[i, 0:1]
        edge_ref[i : i + 1] = inbox[i, 1:2]
    table_ref[...], slots = make_plan(me, cap, relay, n, edge_ref[...])
    to_smem = pltpu.make_async_copy(table_ref, table, own_sem.at[5])
    to_smem.start()
    own_base.start()
    to_smem.wait()
    extra = table[EXTRA, 0]

    def gather_extra(b, carry):
        for u in range(4):
            m = b * 4 + u
            for r in range(relay):
                first[m, r] = row(extra + r * hubs + m)
        return carry

    lax.fori_loop(0, hubs // 4, gather_extra, 0)
    gather(far(SECOND))
    each(lambda d: hop_one(d, core).start(), 1, hubs)

    @pl.when(jnp.logical_not(forward))
    def _():
        hop_one(0, 0).start()

    @pl.when(forward)
    def _():
        arrived[me] = first[chip]

    base(SECOND).start()
    waiting = send(SECOND + 1, THIRD)
    own_ref[0] = table[OWN, 0]
    short_ref[0] = table[SHORT, 0]
    base(waiting).start()
    merged_ref[...], idx_ref[...] = bitonic_sort(seg_ref[...], slots)
    gather(far(THIRD))
    each(lambda d: hop_one(d, core).wait_send(), 1, hubs)

    @pl.when(jnp.logical_not(forward))
    def _():
        hop_one(0, 0).wait_send()

    @pl.when(forward)
    def _():
        for c in range(CORES - 1):
            hop_one(0, c).wait_recv()
        for c in range(CORES):
            each(lambda d: hop_one(d, c).wait_recv(), 1, hubs)
        for j in range(group_size):
            second[j] = arrived[table[FROM_SRC, j] & (group_size - 1)]
        each(lambda d: hop_two(d, chip).start())
        out_ref[pl.ds(group_size * cap + chip * relay, relay)] = second[me]

    base(THIRD).start()
    waiting = send(THIRD + 1, group_size - 1)
    keep = pltpu.make_async_copy(held, split_ref, own_sem.at[4])
    keep.start()
    base(waiting).start()
    for s in range(group_size - 1):
        base(s).wait()
    each(lambda d: hop_two(0, near(d)).wait_recv(), 1, hubs)

    @pl.when(jnp.logical_not(forward))
    def _():
        hop_two(0, chip).wait_recv()

    @pl.when(forward)
    def _():
        each(lambda d: hop_two(d, chip).wait_send())

    own_base.wait()
    keep.wait()


def sort_exchange(keys, rows, cap, relay, group_size):
    n, width = rows.shape
    block = 512
    row = (width // (SUB * LANES), SUB, LANES)
    segs = (group_size, LANES)
    sems = pltpu.SemaphoreType.DMA
    return pl.pallas_call(
        functools.partial(sort_exchange_kernel, group_size, cap, relay, block),
        out_shape=[
            pltpu.VMEM((group_size * cap + group_size // CORES * relay, *row), rows.dtype),
            jax.ShapeDtypeStruct(segs, keys.dtype),
            pltpu.VMEM(segs, jnp.int32),
            jax.ShapeDtypeStruct(keys.shape, jnp.int32),
            jax.ShapeDtypeStruct((n, *row), rows.dtype),
            jax.ShapeDtypeStruct((8, LANES), jnp.int32),
            jax.ShapeDtypeStruct(segs, keys.dtype),
            jax.ShapeDtypeStruct((1,), jnp.int32),
            jax.ShapeDtypeStruct((1,), jnp.int32),
        ],
        in_specs=[VMEM, HBM],
        out_specs=[VMEM, VMEM, VMEM, VMEM, HBM, VMEM, VMEM, SMEM, SMEM],
        scratch_shapes=[
            pltpu.VMEM((n // block, block, width), rows.dtype),
            pltpu.VMEM((n, *row), rows.dtype),
            pltpu.VMEM((group_size, cap, *row), rows.dtype),
            pltpu.VMEM((group_size // CORES, relay, *row), rows.dtype),
            pltpu.VMEM((group_size, relay, *row), rows.dtype),
            pltpu.VMEM((group_size, relay, *row), rows.dtype),
            pltpu.VMEM(keys.shape, keys.dtype),
            pltpu.VMEM((1, LANES), keys.dtype),
            pltpu.VMEM((group_size, 1, LANES), keys.dtype),
            pltpu.VMEM((group_size, 2, LANES), keys.dtype),
            pltpu.VMEM((group_size, 2, LANES), keys.dtype),
            pltpu.VMEM(segs, jnp.float32),
            pltpu.VMEM((1, LANES), jnp.float32),
            pltpu.VMEM((8, LANES), jnp.int32),
            pltpu.SMEM(keys.shape, jnp.int32),
            pltpu.SMEM((8, LANES), jnp.int32),
            pltpu.SMEM((8, LANES), jnp.int32),
            sems((n // block,)),
            sems((6,)),
            sems((5, group_size)),
            sems((5, group_size)),
        ],
        compiler_params=pltpu.CompilerParams(collective_id=0, has_side_effects=True, vmem_limit_bytes=52 * 1024 * 1024),
        name="sort_exchange",
    )(keys, rows)


def pick_kernel(cap, group_size, order_ref, table_ref, rows_ref, out_ref):
    last = rows_ref.shape[0] - 1

    def per_dst(j, carry):
        first = table_ref[0, j]

        def body(b, c):
            for u in range(8):
                k = b * 8 + u
                out_ref[j, k] = rows_ref[order_ref[jnp.minimum(first + k, last)]]
            return c

        return lax.fori_loop(0, cap // 8, body, carry)

    lax.fori_loop(0, group_size, per_dst, 0)


def pick(order, table, rows, cap, group_size):
    return pl.pallas_call(
        functools.partial(pick_kernel, cap, group_size),
        out_shape=jax.ShapeDtypeStruct((group_size, cap, *rows.shape[1:]), rows.dtype),
        in_specs=[SMEM, SMEM, VMEM],
        out_specs=VMEM,
        name="pick_rows",
    )(order, table, rows)


def place_kernel(idx_ref, count_ref, held, keys_ref, out_ref, out_keys_ref, staged, blank, out_sem, blank_sem, keys_sem):
    slots, block, width = staged.shape
    parts = held.shape[1]
    keys_copy = pltpu.make_async_copy(keys_ref, out_keys_ref, keys_sem)
    keys_copy.start()
    blank[...] = jnp.zeros(blank.shape, blank.dtype)
    steps = out_ref.shape[0] // block
    count = count_ref[0]
    live = pl.cdiv(count, block)

    def clear(s):
        return pltpu.make_async_copy(blank, out_ref.at[pl.ds(s * block, block)], blank_sem)

    def store(s):
        slot = lax.rem(s, slots)
        return pltpu.make_async_copy(staged.at[slot], out_ref.at[pl.ds(s * block, block)], out_sem.at[slot])

    def start_clear(s, carry):
        clear(s).start()
        return carry

    def step(s, carry):
        @pl.when(s >= slots)
        def _():
            store(s - slots).wait()

        slot = lax.rem(s, slots)

        def body(g, c):
            for half in range(2):
                r = pl.multiple_of(g * 32 + half * 16, 16)
                rows = []
                for u in range(16):
                    k = idx_ref[s * block + r + u]
                    rows.append(jnp.concatenate([held[k, q] for q in range(parts)], 0))
                staged[slot, pl.ds(r, 16), :] = jnp.stack(rows, 0).reshape(16, width)
            return c

        lax.fori_loop(0, pl.cdiv(jnp.minimum(count - s * block, block), 32), body, 0)

        @pl.when((s + 1) * block > count)
        def _():
            row = lax.broadcasted_iota(jnp.int32, (block, width), 0) + s * block
            staged[slot] = jnp.where(row < count, staged[slot], jnp.zeros((block, width), staged.dtype))

        store(s).start()
        return carry

    lax.fori_loop(live, steps, start_clear, 0)
    lax.fori_loop(0, live, step, 0)

    def end_store(s, carry):
        store(s).wait()
        return carry

    lax.fori_loop(jnp.maximum(live - slots, 0), live, end_store, 0)

    def end_clear(s, carry):
        clear(s).wait()
        return carry

    lax.fori_loop(live, steps, end_clear, 0)
    keys_copy.wait()


def place(idx, count, rows, keys, width):
    n_out = idx.shape[0]
    block, slots = 128, 12
    return pl.pallas_call(
        place_kernel,
        out_shape=[jax.ShapeDtypeStruct((n_out, width), rows.dtype), jax.ShapeDtypeStruct(keys.shape, keys.dtype)],
        in_specs=[SMEM, SMEM, VMEM, VMEM],
        out_specs=[ANY, ANY],
        scratch_shapes=[
            pltpu.VMEM((slots, block, width), rows.dtype),
            pltpu.VMEM((block, width), rows.dtype),
            pltpu.SemaphoreType.DMA((slots,)),
            pltpu.SemaphoreType.DMA,
            pltpu.SemaphoreType.DMA,
        ],
        compiler_params=pltpu.CompilerParams(vmem_limit_bytes=24 * 1024 * 1024),
        name="place_rows",
    )(idx, count, rows, keys)


def solution(mesh):
    group_size = mesh.shape["g"]

    def local_part(keys_loc, rows_loc):
        n_dev = keys_loc.shape[0]
        width = rows_loc.shape[1]
        cap_rows = 2 * n_dev // group_size
        blocks, merged, idx, order, rows, starts, segs, own_count, short = sort_exchange(keys_loc.reshape(n_dev // LANES, LANES), rows_loc, BASE, RELAY, group_size)
        out_rows, out_keys = place(idx.reshape(-1), own_count, blocks, merged, width)

        def general(carry):
            wide = lax.all_to_all(pick(order.reshape(-1), starts, rows, cap_rows, group_size), "g", 0, 0, tiled=True)
            _, at = lax.sort((segs.reshape(-1), lax.iota(jnp.int32, segs.size)), num_keys=1)
            return jnp.int32(1), place(at, own_count, wide.reshape(-1, *wide.shape[2:]), merged, width)[0]

        _, out_rows = lax.while_loop(lambda carry: carry[0] == 0, general, (short[0], out_rows))
        return out_keys.reshape(-1), out_rows, own_count

    row_spec = P(("batch", "g"))
    mat_spec = P(("batch", "g"), None)
    return jax.shard_map(local_part, mesh=mesh, in_specs=(row_spec, mat_spec), out_specs=(row_spec, mat_spec, row_spec), check_vma=False)
```
